128 devices in a mesh: dp: 4 (over z_lo, core), seq: 8 (over x, z_hi), tensor: 4 (over y).
Axes of the slice: x: 4, y: 4, z: 4 (z_hi: 2, z_lo: 2; z = z_hi * 2 + z_lo), core: 2. Of those that a mesh axis runs over, the one named last changes fastest.
Arguments:
- latents: bfloat16 [4, 16, 256, 1152], P('dp', 'seq', 'tensor'), may hold values from -6 to 6
- modulation: float32 [4, 6, 1152], P('dp'), may hold values from -3 to 3
- in_weight: bfloat16 [1152, 3, 1152], P(None, None, 'tensor'), may hold values from -0.5 to 0.5
- out_weight: bfloat16 [1152, 1152], P('tensor'), may hold values from -0.1875 to 0.1875
- up_weight: bfloat16 [1152, 4608], P(None, 'tensor'), may hold values from -0.1875 to 0.1875
- down_weight: bfloat16 [4608, 1152], P('tensor'), may hold values from -0.09375 to 0.09375
- cotangent: bfloat16 [4, 16, 256, 1152], P('dp', 'seq', 'tensor'), may hold values from -6 to 6
Outputs:
- result: bfloat16 [4, 16, 256, 1152], P('dp', 'seq', 'tensor')
- latents_grad: bfloat16 [4, 16, 256, 1152], P('dp', 'seq', 'tensor')
- in_grad: bfloat16 [1152, 3, 1152], P(('dp', 'seq'), None, 'tensor')
- out_grad: bfloat16 [1152, 1152], P('tensor', ('dp', 'seq'))
- up_grad: bfloat16 [1152, 4608], P(('dp', 'seq'), 'tensor')
- down_grad: bfloat16 [4608, 1152], P('tensor', ('dp', 'seq'))
The draws below stay inside these ranges and needn't reach their ends.
All inputs are finite; a program needn't handle non-finite values.
Results may differ from the reference program's by a relative error of at most 0.02.
The reference program's roundings to bfloat16 on the way count: a program that leaves them out, or rounds other values in their place, can miss the bound.
Values may be sent and summed in bfloat16 or wider, within the bound.
A program may use at most 128 MiB of HBM per device.

```python
import math
import jax
import jax.numpy as jnp
from jax import lax

D = 1152
HEADS = 16
FF = 4608
PIX = 256
FRAMES = 16
BATCH = 4


def draw_latents(key, part):
    shape = (BATCH, FRAMES, PIX, D)
    values = jax.random.normal(key, shape, jnp.float32)
    return jnp.clip(values, -6.0, 6.0).astype(jnp.bfloat16)


def draw_in_weight(key, part):
    first_key = jax.random.fold_in(key, 0)
    basis = jax.random.normal(first_key, (D, 3, D), jnp.float32) * D ** (-0.5)
    values = basis
    return jnp.clip(values, -0.5, 0.5).astype(jnp.bfloat16)


def with_spikes(values, rng, source, target, shards_of, factor):
    def block_of(position):
        return (jnp.arange(values.shape[position]) // (values.shape[position] // shards_of)).reshape((-1,) + (1,) * (values.ndim - 1 - position))

    one_side = jax.random.permutation(rng, shards_of)[block_of(target)]
    far = (block_of(target) + shards_of // 2) % shards_of
    return jnp.where((block_of(source) == one_side) | (block_of(source) == far), factor * values, values)


def level_of(stream_key, shape, cuts, least, largest):
    gain = 1.0
    for axis_at, blocks in cuts:
        draws = jax.random.uniform(jax.random.fold_in(jax.random.fold_in(stream_key, 6), axis_at), (blocks,), jnp.float32, least / len(cuts), largest / len(cuts))
        gain = gain * jnp.repeat(jnp.exp(draws), shape[axis_at] // blocks).reshape((-1,) + (1,) * (len(shape) - 1 - axis_at))
    return gain


def gaussian(own_key, extent, scale, reach, cuts=(), kind=jnp.bfloat16):
    values = scale * jax.random.normal(own_key, extent, jnp.float32)
    if cuts:
        values = values * level_of(own_key, extent, cuts, -0.22, 0.18)
    return jnp.clip(values, -reach, reach).astype(kind)


def gaussian_with(rng, extent, scale, limit, cuts, heavy, dtype=jnp.bfloat16):
    entries = scale * jax.random.normal(rng, extent, jnp.float32)
    if cuts:
        entries = entries * level_of(rng, extent, cuts, -0.22, 0.18)
    return jnp.clip(with_spikes(entries, jax.random.fold_in(rng, 3), *heavy), -limit, limit).astype(dtype)


def setup_inputs(seed: int = 0) -> dict:
    keys = jax.random.split(jax.random.key(seed), 8)
    latents = draw_latents(jax.random.fold_in(keys[7], 71), 0)
    modulation = gaussian(keys[1], (BATCH, 6, D), 0.5, 3.0, ((0, 4),), jnp.float32)
    in_weight = draw_in_weight(jax.random.fold_in(keys[7], 71), 0)
    out_weight = gaussian(keys[3], (D, D), D ** -0.5, 0.1875, ((0, 4),))
    up_weight = gaussian(keys[4], (D, FF), D ** -0.5, 0.1875, ((1, 4),))
    down_weight = gaussian(keys[5], (FF, D), FF ** -0.5, 0.09375, ((0, 4),))
    cotangent = gaussian_with(keys[6], (BATCH, FRAMES, PIX, D), 1.0, 6.0, ((0, 4), (1, 8), (2, 4)), (1, 3, 8, 2.0))
    return {"latents": latents, "modulation": modulation, "in_weight": in_weight, "out_weight": out_weight, "up_weight": up_weight, "down_weight": down_weight, "cotangent": cotangent}


epsilon = 1e-06

def normalize(rows):
    center = lax.optimization_barrier(jnp.mean(rows, axis=-1, keepdims=True))
    centred = rows - center
    spread = lax.optimization_barrier(jnp.mean(centred * centred, axis=-1, keepdims=True))
    inverse = lax.rsqrt(spread + epsilon)
    return (centred * inverse, inverse)

def norm_back(normed, inverse, upstream):
    mean_grad = lax.optimization_barrier(jnp.mean(upstream, axis=-1, keepdims=True))
    mean_cross = lax.optimization_barrier(jnp.mean(upstream * normed, axis=-1, keepdims=True))
    return (upstream - mean_grad - normed * mean_cross) * inverse

def gelu_tanh(values):
    return jax.nn.gelu(values, approximate=True)

def flat_dot(left, right):
    leading = left.shape[:-1]
    out_rows = jnp.dot(left.reshape(-1, left.shape[-1]), right, preferred_element_type=jnp.float32)
    return out_rows.reshape(leading + (right.shape[-1],))

def flat_dot_t(left, right):
    leading = left.shape[:-1]
    out_rows = lax.dot_general(left.reshape(-1, left.shape[-1]), right, (((1,), (1,)), ((), ())), preferred_element_type=jnp.float32)
    return out_rows.reshape(leading + (right.shape[0],))

def weight_grad(left, right):
    return lax.dot_general(left.reshape(-1, left.shape[-1]), right.reshape(-1, right.shape[-1]), (((0,), (0,)), ((), ())), preferred_element_type=jnp.float32)

def attend(queries, key_rows, value_rows):
    scaling = 1.0 / math.sqrt(queries.shape[-1])
    scores = jnp.einsum('bfphe,bgphe->bphfg', queries.astype(jnp.float32), key_rows.astype(jnp.float32)) * scaling
    highest = lax.optimization_barrier(jnp.max(scores, axis=-1, keepdims=True))
    raised = jnp.exp(scores - highest)
    probs = raised / lax.optimization_barrier(jnp.sum(raised, axis=-1, keepdims=True))
    probs_low = probs.astype(jnp.bfloat16)
    attended = jnp.einsum('bphfg,bgphe->bfphe', probs_low.astype(jnp.float32), value_rows.astype(jnp.float32)).astype(jnp.bfloat16)
    return (attended, probs, probs_low)

def attend_back(queries, key_rows, value_rows, probs, probs_low, attended_grad):
    scaling = 1.0 / math.sqrt(queries.shape[-1])
    grad_wide = attended_grad.astype(jnp.float32)
    value_grad = jnp.einsum('bphfg,bfphe->bgphe', probs_low.astype(jnp.float32), grad_wide).astype(jnp.bfloat16)
    prob_grad = jnp.einsum('bfphe,bgphe->bphfg', grad_wide, value_rows.astype(jnp.float32))
    score_grad = probs * (prob_grad - lax.optimization_barrier(jnp.sum(probs * prob_grad, axis=-1, keepdims=True))) * scaling
    score_low = score_grad.astype(jnp.bfloat16).astype(jnp.float32)
    query_grad = jnp.einsum('bphfg,bgphe->bfphe', score_low, key_rows.astype(jnp.float32)).astype(jnp.bfloat16)
    key_grad = jnp.einsum('bphfg,bfphe->bgphe', score_low, queries.astype(jnp.float32)).astype(jnp.bfloat16)
    return (query_grad, key_grad, value_grad)

def reference(latents, modulation, in_weight, out_weight, up_weight, down_weight, cotangent):
    samples, frames_all, patches, width = latents.shape
    modulate = modulation[:, :, None, None, :]
    shift_first, scale_first, gate_first = (modulate[:, 0], modulate[:, 1], modulate[:, 2])
    shift_second, scale_second, gate_second = (modulate[:, 3], modulate[:, 4], modulate[:, 5])
    inputs = latents.astype(jnp.float32)
    first_normed, first_inverse = normalize(inputs)
    first_input = (first_normed * (1.0 + scale_first) + shift_first).astype(jnp.bfloat16)
    in_flat = in_weight.reshape(width, 3 * width)
    projected = flat_dot(first_input, in_flat).astype(jnp.bfloat16)
    split_parts = projected.reshape(samples, frames_all, patches, 3, HEADS, width // HEADS)
    queries, key_rows, value_rows = (split_parts[:, :, :, 0], split_parts[:, :, :, 1], split_parts[:, :, :, 2])
    attended, probs, probs_low = attend(queries, key_rows, value_rows)
    attended_flat = attended.reshape(samples, frames_all, patches, width)
    midway = inputs + gate_first * flat_dot(attended_flat, out_weight)
    second_normed, second_inverse = normalize(midway)
    second_input = (second_normed * (1.0 + scale_second) + shift_second).astype(jnp.bfloat16)
    hidden = flat_dot(second_input, up_weight)
    activated = gelu_tanh(hidden).astype(jnp.bfloat16)
    result = (midway + gate_second * flat_dot(activated, down_weight)).astype(jnp.bfloat16)
    upstream = cotangent.astype(jnp.float32)
    branch_grad = (gate_second * upstream).astype(jnp.bfloat16)
    down_grad = weight_grad(activated, branch_grad)
    activated_grad = flat_dot_t(branch_grad, down_weight)
    hidden_grad = jax.vjp(gelu_tanh, hidden)[1](activated_grad)[0].astype(jnp.bfloat16)
    up_grad = weight_grad(second_input, hidden_grad)
    second_grad = flat_dot_t(hidden_grad, up_weight)
    midway_grad = upstream + norm_back(second_normed, second_inverse, second_grad * (1.0 + scale_second))
    attention_grad = (gate_first * midway_grad).astype(jnp.bfloat16)
    out_grad = weight_grad(attended_flat, attention_grad)
    attended_grad = flat_dot_t(attention_grad, out_weight).astype(jnp.bfloat16)
    attended_grad = attended_grad.reshape(samples, frames_all, patches, HEADS, width // HEADS)
    query_grad, key_grad, value_grad = attend_back(queries, key_rows, value_rows, probs, probs_low, attended_grad)
    projected_grad = jnp.stack([query_grad, key_grad, value_grad], axis=3).reshape(samples, frames_all, patches, 3 * width)
    in_grad = weight_grad(first_input, projected_grad).reshape(width, 3, width)
    first_grad = flat_dot_t(projected_grad, in_flat)
    latents_grad = (midway_grad + norm_back(first_normed, first_inverse, first_grad * (1.0 + scale_first))).astype(jnp.bfloat16)
    return (result, latents_grad, in_grad.astype(jnp.bfloat16), out_grad.astype(jnp.bfloat16), up_grad.astype(jnp.bfloat16), down_grad.astype(jnp.bfloat16))
```

```python
import math

import jax
import jax.numpy as jnp
from jax import lax
from jax.experimental import pallas as pl
from jax.experimental.pallas import tpu as pltpu
from jax.sharding import PartitionSpec as P

HEAD_DIM = 72
HEADS = 4
D = 1152
W = 288
WP = 384
SCALE = 1.0 / math.sqrt(HEAD_DIM)
EPS = 1e-6
MESH = pl.DeviceIdType.MESH
F32 = jnp.float32
BF16 = jnp.bfloat16
GELU_C = math.sqrt(2.0 / math.pi)

NN = (((1,), (0,)), ((), ()))
NT = (((1,), (1,)), ((), ()))
TN = (((0,), (0,)), ((), ()))


def rem(a, b):
    return lax.rem(a, b)


def div(a, b):
    return lax.div(a, b)


def dot(a, b, dims):
    return lax.dot_general(a, b, dims, preferred_element_type=F32)


def norm(rows):
    center = jnp.mean(rows, axis=-1, keepdims=True)
    centred = rows - center
    spread = jnp.mean(centred * centred, axis=-1, keepdims=True)
    inverse = lax.rsqrt(spread + EPS)
    return centred * inverse, inverse


def norm_back(normed, inverse, up):
    mean_grad = jnp.mean(up, axis=-1, keepdims=True)
    mean_cross = jnp.mean(up * normed, axis=-1, keepdims=True)
    return (up - mean_grad - normed * mean_cross) * inverse


JOBS = (("u", 1152, True), ("d", 1152, False), ("i", 768, True), ("v", 768, False))


def scratch_spec():
    vm = lambda *s, t=BF16: pltpu.VMEM(s, t)
    dma = lambda *s: pltpu.SemaphoreType.DMA(s)
    spec = {
        "xs": vm(8, 2, 8, D), "cs": vm(8, 2, 8, D),
        "win": vm(3, WP, D), "wout": vm(WP, D), "wup": vm(D, D), "wdown": vm(D, D),
        "f": vm(4, 128, D), "s": vm(4, 128, D), "g": vm(4, 128, D), "a": vm(4, 128, D),
        "p2": vm(4, 128, D), "p5": vm(4, 128, D), "p7": vm(4, 128, D), "p8": vm(4, 128, D),
        "r2": vm(4, 128, D), "r5": vm(4, 128, D), "r7": vm(4, 128, D), "r8": vm(4, 128, D),
        "qkv": vm(4, 128, 3 * WP), "probs": vm(4, 512, 128, t=F32), "att": vm(4, 128, WP),
        "act": vm(4, 128, D), "hg": vm(4, 128, D), "dqkv": vm(4, 128, 3 * WP),
        "mid": vm(128, D, t=F32), "mg": vm(128, D, t=F32),
        "ro": vm(8, 2, 8, D), "lo": vm(8, 2, 8, D), "rl": vm(2, 8, 8, D), "ll": vm(2, 8, 8, D),
        "wsem": dma(6),
        "ys": dma(8, 4), "yr": dma(8, 4),
        "ss": dma(4, 8), "sr": dma(4, 8),
        "osem": dma(2),
        "js": dma(4, 7), "jr": dma(4, 7),
    }
    for name, n, x_first in JOBS:
        spec["G" + name] = vm(2, 2, 4, 9, 8, n)
        spec["A" + name] = vm(2, 4, 9, 8, n)
        if x_first:
            spec["B" + name] = vm(4, 2, 9, 8, n)
            spec["H" + name] = vm(2, 9, 8, n)
        else:
            spec["B" + name] = vm(4, 4, 5, 8, n)
            spec["H" + name] = vm(4, 5, 8, n)
        spec["C" + name] = vm(4, 5, 8, n)
    return spec


SPEC = scratch_spec()


def kernel(lat, cot, mod, in_w, out_w, up_w, down_w, res, lgr, gu, gd, gi, gv, *scratch):
    r = dict(zip(SPEC, scratch))
    dp, seq, me = lax.axis_index("dp"), lax.axis_index("seq"), lax.axis_index("tensor")
    core, z_lo = rem(dp, 2), div(dp, 2)
    x, z_hi = div(seq, 2), rem(seq, 2)
    z = z_hi * 2 + z_lo

    def remote(src, dst, send, recv, where):
        return pltpu.make_async_remote_copy(src_ref=src, dst_ref=dst, send_sem=send, recv_sem=recv, device_id=where, device_id_type=MESH)

    def local(src, dst, sem):
        return pltpu.make_async_copy(src, dst, sem)

    def seq_peer(k):
        return (dp, rem(seq + k, 8), me)

    def y_peer(k):
        return (dp, seq, rem(me + k, 4))

    def core_peer():
        return (dp + 1 - 2 * core, seq, me)

    def x_peer(k):
        return (dp, rem(x + k, 4) * 2 + z_hi, me)

    def z_peer(k):
        other = rem(z + k, 4)
        return (rem(other, 2) * 2 + core, x * 2 + div(other, 2), me)

    weights = [local(in_w.at[j], r["win"].at[j, pl.ds(0, W)], r["wsem"].at[j]) for j in range(3)]
    weights += [
        local(out_w, r["wout"].at[pl.ds(0, W)], r["wsem"].at[3]),
        local(up_w, r["wup"], r["wsem"].at[4]),
        local(down_w, r["wdown"], r["wsem"].at[5]),
    ]

    barrier = pltpu.get_barrier_semaphore()
    peers = [seq_peer(k) for k in range(1, 8)] + [y_peer(k) for k in range(1, 4)] + [core_peer()]
    peers += [z_peer(1), z_peer(3)]
    for where in peers:
        pl.semaphore_signal(barrier, inc=1, device_id=where, device_id_type=MESH)
    pl.semaphore_wait(barrier, len(peers))

    sends = []

    def exchange_in(row, src, dst):
        for k in range(1, 8):
            to = rem(seq + k, 8)
            c = remote(src.at[:, to], dst.at[seq], r["ss"].at[row, k], r["sr"].at[row, k], seq_peer(k))
            c.start()
            sends.append(c)
        c = local(src.at[:, seq], dst.at[seq], r["sr"].at[row, 0])
        c.start()

    def exchange_in_wait(row, src, dst):
        local(src.at[:, seq], dst.at[seq], r["sr"].at[row, 0]).wait()
        for k in range(1, 8):
            frm = rem(seq + 8 - k, 8)
            remote(src.at[:, frm], dst.at[frm], r["ss"].at[row, k], r["sr"].at[row, k], seq_peer(k)).wait_recv()

    exchange_in(0, lat, r["xs"])
    exchange_in(1, cot, r["cs"])
    for c in weights:
        c.start()
    for j in range(3):
        r["win"][j, W:] = jnp.zeros((WP - W, D), BF16)
    r["wout"][W:] = jnp.zeros((WP - W, D), BF16)

    def row(i):
        return mod[i : i + 1, :]

    def halves(ref, h):
        return ref[4 * h : 4 * h + 4].astype(F32).reshape(64, D)

    def gather_start(ph, buf):
        for k in (2, 1, 3):
            c = remote(buf.at[me], buf.at[me], r["ys"].at[ph, k], r["yr"].at[ph, k], y_peer(k))
            c.start()
            sends.append(c)

    def gather_wait(ph, buf, k):
        frm = rem(me + 4 - k, 4)
        remote(buf.at[frm], buf.at[frm], r["ys"].at[ph, k], r["yr"].at[ph, k], y_peer(k)).wait_recv()

    def part_send(ph, src, dst, k):
        to = rem(me + k, 4)
        c = remote(src.at[to], dst.at[me], r["ys"].at[ph, k], r["yr"].at[ph, k], y_peer(k))
        c.start()

    def part_send_wait(ph, src, dst):
        for k in range(1, 4):
            remote(src.at[0], dst.at[me], r["ys"].at[ph, k], r["yr"].at[ph, k], y_peer(k)).wait_send()

    def part_wait(ph, src, dst):
        for k in range(1, 4):
            frm = rem(me + 4 - k, 4)
            remote(src.at[frm], dst.at[frm], r["ys"].at[ph, k], r["yr"].at[ph, k], y_peer(k)).wait_recv()

    def part_sum(src, dst, h):
        rows = pl.ds(64 * h, 64)
        total = src[me, rows, :].astype(F32)
        for k in (1, 2, 3):
            total = total + dst[rem(me + k, 4), rows, :].astype(F32)
        return total

    def block_of(i):
        k = jnp.where(i < 2, i, 5 - i)
        return k, rem(me + k, 4)

    def arrival(ph, buf, i):
        for j, k in ((1, 1), (2, 3), (3, 2)):
            @pl.when(i == j)
            def _():
                gather_wait(ph, buf, 4 - k)

    def part_out(ph, src, dst, i):
        for j, k in ((1, 1), (2, 3), (3, 2)):
            @pl.when(i == j)
            def _():
                part_send(ph, src, dst, k)

    lane = lax.broadcasted_iota(jnp.int32, (128, WP), 1)
    head_masks = [(lane >= HEAD_DIM * h) & (lane < HEAD_DIM * (h + 1)) for h in range(HEADS)]
    same_pixel = rem(lax.broadcasted_iota(jnp.int32, (512, 128), 0), 8) == rem(lax.broadcasted_iota(jnp.int32, (512, 128), 1), 8)

    def stacked(v):
        zero = jnp.zeros_like(v)
        return jnp.concatenate([jnp.where(m, v, zero) for m in head_masks], axis=0)

    def side_by_side(v):
        return jnp.concatenate([v[128 * h : 128 * h + 128] for h in range(HEADS)], axis=1)

    exchange_in_wait(0, lat, r["xs"])
    for h in range(2):
        normed, _ = norm(halves(r["xs"], h))
        r["f"][me, 64 * h : 64 * h + 64, :] = (normed * (1.0 + row(1)) + row(0)).astype(BF16)
    gather_start(0, r["f"])
    exchange_in_wait(1, cot, r["cs"])
    for h in range(2):
        r["g"][me, 64 * h : 64 * h + 64, :] = (row(5) * halves(r["cs"], h)).astype(BF16)

    gather_start(1, r["g"])
    for c in weights[:4]:
        c.wait()

    def attend_block(i, carry):
        k, t = block_of(i)
        arrival(0, r["f"], i)

        block = r["f"][t]
        for j in range(3):
            r["qkv"][t, :, j * WP : (j + 1) * WP] = dot(block, r["win"][j], NT).astype(BF16)
        q, kk, v = (r["qkv"][t, :, j * WP : (j + 1) * WP] for j in range(3))
        scores = dot(stacked(q), kk, NT) * SCALE
        scores = jnp.where(same_pixel, scores, -1e30)
        raised = jnp.exp(scores - jnp.max(scores, axis=-1, keepdims=True))
        probs = raised / jnp.sum(raised, axis=-1, keepdims=True)
        r["probs"][t] = probs
        att = dot(side_by_side(probs.astype(BF16)), stacked(v), NN).astype(BF16)
        r["att"][t] = att
        for n in range(3):
            cols = slice(n * 384, n * 384 + 384)
            r["p2"][t, :, cols] = dot(att, r["wout"][:, cols], NN).astype(BF16)
        part_out(2, r["p2"], r["r2"], i)
        return carry

    lax.fori_loop(0, 4, attend_block, 0)
    part_wait(2, r["p2"], r["r2"])

    for h in range(2):
        rows = slice(64 * h, 64 * h + 64)
        midway = halves(r["xs"], h) + row(2) * part_sum(r["p2"], r["r2"], h)
        r["mid"][rows, :] = midway
        normed, _ = norm(midway)
        r["s"][me, rows, :] = (normed * (1.0 + row(4)) + row(3)).astype(BF16)
    gather_start(3, r["s"])

    weights[4].wait()
    weights[5].wait()

    def mlp_block(i, carry):
        k, t = block_of(i)
        arrival(3, r["s"], i)
        arrival(1, r["g"], i)

        def hidden_cols(n, c):
            cols = pl.ds(pl.multiple_of(n * 384, 384), 384)
            v = dot(r["s"][t], r["wup"][:, cols], NN)
            ag = dot(r["g"][t], r["wdown"][cols, :], NT)
            th = jnp.tanh(GELU_C * (v + 0.044715 * (v * v * v)))
            r["act"][t, :, cols] = (0.5 * v * (1.0 + th)).astype(BF16)
            slope = 0.5 * (1.0 + th) + (0.5 * v) * ((1.0 - th * th) * (GELU_C * (1.0 + (3.0 * 0.044715) * (v * v))))
            r["hg"][t, :, cols] = (ag * slope).astype(BF16)
            return c

        lax.fori_loop(0, 3, hidden_cols, 0)

        def grad_cols(n, c):
            cols = pl.ds(pl.multiple_of(n * 384, 384), 384)
            r["p5"][t, :, cols] = dot(r["hg"][t], r["wup"][cols, :], NT).astype(BF16)
            return c

        lax.fori_loop(0, 3, grad_cols, 0)
        part_out(4, r["p5"], r["r5"], i)

        def result_cols(n, c):
            cols = pl.ds(pl.multiple_of(n * 384, 384), 384)
            r["p8"][t, :, cols] = dot(r["act"][t], r["wdown"][:, cols], NN).astype(BF16)
            return c

        lax.fori_loop(0, 3, result_cols, 0)
        return carry

    lax.fori_loop(0, 4, mlp_block, 0)

    def weight_grad(lhs, rhs, width, name, at):
        def rows_step(m, c):
            cols = pl.ds(pl.multiple_of(m * 384, 384), 384)
            left = lhs[:, :, cols].reshape(512, 384)
            right = rhs().reshape(512, width)
            out = dot(left, right, TN).astype(BF16).reshape(48, 8, width)
            for q in range(48 // 3):
                grp = m * 16 + q
                outer = div(grp, 3)
                r["G" + name][div(outer, 8), rem(div(outer, 4), 2), rem(outer, 4), pl.ds(rem(grp, 3) * 3, 3), :, at : at + width] = out[3 * q : 3 * q + 3]
            return c

        lax.fori_loop(0, 3, rows_step, 0)

    def job(index):
        name, n, x_first = JOBS[index]
        return name, n, x_first

    def job_core(index, start):
        name, n, _ = JOBS[index]
        to = 1 - core if start else core
        c = remote(r["G" + name].at[:, 1 - core], r["A" + name], r["js"].at[index, 0], r["jr"].at[index, 0], core_peer())
        if start:
            c.start()
        else:
            c.wait()

    def job_core_sum(index):
        name, n, _ = JOBS[index]

        def step(i, c):
            a, b = div(i, 4), rem(i, 4)
            total = r["A" + name][a, b].astype(F32) + r["G" + name][a, core, b].astype(F32)
            r["A" + name][a, b] = total.astype(BF16)
            return c

        lax.fori_loop(0, 8, step, 0)

    def job_first(index, start):
        name, n, x_first = JOBS[index]
        for k in (2, 1, 3):
            if x_first:
                src = r["A" + name].at[:, rem(x + k, 4)]
                mine, frm, where = x, rem(x + 4 - k, 4), x_peer(k)
            else:
                other = rem(z + k, 4)
                src = r["A" + name].at[rem(other, 2), :, pl.ds(4 * div(other, 2), 5)]
                mine, frm, where = z, rem(z + 4 - k, 4), z_peer(k)
            if start:
                remote(src, r["B" + name].at[mine], r["js"].at[index, k], r["jr"].at[index, k], where).start()
            else:
                remote(src, r["B" + name].at[frm], r["js"].at[index, k], r["jr"].at[index, k], where).wait()

    def job_first_sum(index):
        name, n, x_first = JOBS[index]
        if x_first:
            for a in range(2):
                total = r["A" + name][a, x].astype(F32)
                for k in (1, 2, 3):
                    total = total + r["B" + name][rem(x + k, 4), a].astype(F32)
                r["H" + name][a] = total.astype(BF16)
        else:
            for b in range(4):
                total = r["A" + name][z_lo, b, pl.ds(4 * z_hi, 5)].astype(F32)
                for k in (1, 2, 3):
                    total = total + r["B" + name][rem(z + k, 4), b].astype(F32)
                r["H" + name][b] = total.astype(BF16)

    def job_second(index, start):
        name, n, x_first = JOBS[index]
        for k in (2, 1, 3):
            if x_first:
                other = rem(z + k, 4)
                src = r["H" + name].at[rem(other, 2), pl.ds(4 * div(other, 2), 5)]
                mine, frm, where = z, rem(z + 4 - k, 4), z_peer(k)
            else:
                src = r["H" + name].at[rem(x + k, 4)]
                mine, frm, where = x, rem(x + 4 - k, 4), x_peer(k)
            if start:
                remote(src, r["C" + name].at[mine], r["js"].at[index, 3 + k], r["jr"].at[index, 3 + k], where).start()
            else:
                remote(src, r["C" + name].at[frm], r["js"].at[index, 3 + k], r["jr"].at[index, 3 + k], where).wait()

    def job_second_sum(index, out):
        name, n, x_first = JOBS[index]
        if x_first:
            total = r["H" + name][z_lo, pl.ds(4 * z_hi, 5)].astype(F32)
            at = z
        else:
            total = r["H" + name][x].astype(F32)
            at = x
        for k in (1, 2, 3):
            total = total + r["C" + name][rem(at + k, 4)].astype(F32)
        out[...] = total.astype(BF16)

    weight_grad(r["s"], lambda: r["hg"][...], D, "u", 0)
    job_core(0, True)

    part_wait(4, r["p5"], r["r5"])
    for h in range(2):
        rows = slice(64 * h, 64 * h + 64)
        normed, inverse = norm(r["mid"][rows, :])
        back = norm_back(normed, inverse, part_sum(r["p5"], r["r5"], h) * (1.0 + row(4)))
        mg = halves(r["cs"], h) + back
        r["mg"][rows, :] = mg
        r["a"][me, rows, :] = (row(2) * mg).astype(BF16)
    gather_start(5, r["a"])
    for k in (1, 3, 2):
        part_send(7, r["p8"], r["r8"], k)

    weight_grad(r["g"], lambda: r["act"][...], D, "d", 0)
    job_core(1, True)
    job_core(0, False)
    job_core_sum(0)
    job_first(0, True)

    def attend_back_block(i, carry):
        k, t = block_of(i)
        arrival(5, r["a"], i)
        grad = dot(r["a"][t], r["wout"][...], NT).astype(BF16)
        q, kk, v = (r["qkv"][t, :, j * WP : (j + 1) * WP] for j in range(3))
        qs, gs = stacked(q), stacked(grad)
        probs = r["probs"][t]
        dv = dot(probs.astype(BF16), gs, TN)
        dp_ = dot(gs, v, NT)
        ds = (probs * (dp_ - jnp.sum(probs * dp_, axis=-1, keepdims=True)) * SCALE).astype(BF16)
        dq = dot(side_by_side(ds), stacked(kk), NN)
        dk = dot(ds, qs, TN)
        for j, part in enumerate((dq, dk, dv)):
            r["dqkv"][t, :, j * WP : (j + 1) * WP] = part.astype(BF16)
        for n in range(3):
            cols = slice(n * 384, n * 384 + 384)
            total = dot(r["dqkv"][t, :, 0:WP], r["win"][0, :, cols], NN)
            for j in (1, 2):
                total = total + dot(r["dqkv"][t, :, j * WP : (j + 1) * WP], r["win"][j, :, cols], NN)
            r["p7"][t, :, cols] = total.astype(BF16)
        part_out(6, r["p7"], r["r7"], i)
        return carry

    lax.fori_loop(0, 2, attend_back_block, 0)
    job_core(1, False)
    job_core_sum(1)
    job_first(1, True)
    lax.fori_loop(2, 4, attend_back_block, 0)

    weight_grad(r["f"], lambda: r["dqkv"][:, :, 0:768], 768, "i", 0)
    job_core(2, True)
    weight_grad(r["f"], lambda: r["dqkv"][:, :, 768:1152], 384, "v", 0)
    weight_grad(r["a"], lambda: r["att"][...], 384, "v", 384)
    job_core(3, True)

    def exchange_out(row_, src, dst):
        for k in range(1, 8):
            to = rem(seq + k, 8)
            remote(src.at[to], dst.at[:, seq], r["ss"].at[row_, k], r["sr"].at[row_, k], seq_peer(k)).start()
        local(src.at[seq], dst.at[:, seq], r["sr"].at[row_, 0]).start()

    def exchange_out_wait(row_, src, dst):
        local(src.at[seq], dst.at[:, seq], r["sr"].at[row_, 0]).wait()
        for k in range(1, 8):
            frm = rem(seq + 8 - k, 8)
            remote(src.at[frm], dst.at[:, frm], r["ss"].at[row_, k], r["sr"].at[row_, k], seq_peer(k)).wait()

    part_wait(7, r["p8"], r["r8"])
    for h in range(2):
        rows = slice(64 * h, 64 * h + 64)
        out = r["mid"][rows, :] + row(5) * part_sum(r["p8"], r["r8"], h)
        r["ro"][4 * h : 4 * h + 4] = out.astype(BF16).reshape(4, 2, 8, D)
    exchange_out(2, r["ro"], r["rl"])

    job_first(0, False)
    job_first_sum(0)
    job_second(0, True)

    part_wait(6, r["p7"], r["r7"])
    for h in range(2):
        rows = slice(64 * h, 64 * h + 64)
        normed, inverse = norm(halves(r["xs"], h))
        back = norm_back(normed, inverse, part_sum(r["p7"], r["r7"], h) * (1.0 + row(1)))
        out = r["mg"][rows, :] + back
        r["lo"][4 * h : 4 * h + 4] = out.astype(BF16).reshape(4, 2, 8, D)
    exchange_out(3, r["lo"], r["ll"])

    job_first(1, False)
    job_first_sum(1)
    job_second(1, True)
    for index in (2, 3):
        job_core(index, False)
        job_core_sum(index)
        job_first(index, True)
    job_second(0, False)
    job_second_sum(0, gu)
    job_second(1, False)
    job_second_sum(1, gd)
    exchange_out_wait(2, r["ro"], r["rl"])
    done = [local(r["rl"], res, r["osem"].at[0])]
    done[0].start()
    for index in (2, 3):
        job_first(index, False)
        job_first_sum(index)
        job_second(index, True)
    exchange_out_wait(3, r["lo"], r["ll"])
    done.append(local(r["ll"], lgr, r["osem"].at[1]))
    done[1].start()
    for index, out in ((2, gi), (3, gv)):
        job_second(index, False)
        job_second_sum(index, out)
    for c in sends:
        c.wait_send()
    for ph, src, dst in ((2, "p2", "r2"), (4, "p5", "r5"), (6, "p7", "r7"), (7, "p8", "r8")):
        part_send_wait(ph, r[src], r[dst])
    for c in done:
        c.wait()


def body(latents, modulation, in_weight, out_weight, up_weight, down_weight, cotangent):
    vmem = pl.BlockSpec(memory_space=pltpu.VMEM)
    anywhere = pl.BlockSpec(memory_space=pl.ANY)
    out = lambda *s: jax.ShapeDtypeStruct(s, BF16)
    res, lgr, gu, gd, gi, gv = pl.pallas_call(
        kernel,
        out_shape=(out(2, 8, 8, D), out(2, 8, 8, D), out(5, 8, D), out(5, 8, D), out(5, 8, 768), out(5, 8, 768)),
        in_specs=[anywhere, anywhere, vmem, anywhere, anywhere, anywhere, anywhere],
        out_specs=(anywhere, anywhere, vmem, vmem, vmem, vmem),
        scratch_shapes=list(SPEC.values()),
        compiler_params=pltpu.CompilerParams(collective_id=0, has_side_effects=True, vmem_limit_bytes=67043328),
        name="block",
    )(
        latents.reshape(2, 8, 8, D),
        cotangent.reshape(2, 8, 8, D),
        modulation[0],
        jnp.transpose(in_weight, (1, 2, 0)),
        out_weight,
        up_weight,
        down_weight,
    )
    at = 4 * rem(lax.axis_index("seq"), 2)

    def own(g):
        rows = g.reshape(40, g.shape[-1])
        return jnp.where(at == 0, rows[:36], rows[4:])

    gi, gv = own(gi), own(gv)
    in_grad = jnp.concatenate([gi, gv[:, :WP]], axis=1).reshape(36, 3, WP)[:, :, :W]
    return (
        res.reshape(latents.shape),
        lgr.reshape(latents.shape),
        in_grad,
        gv[:, WP : WP + W].T,
        own(gu),
        own(gd).T,
    )


def solution(mesh):
    placed = (
        P("dp", "seq", "tensor", None),
        P("dp", None, None),
        P(None, None, "tensor"),
        P("tensor", None),
        P(None, "tensor"),
        P("tensor", None),
        P("dp", "seq", "tensor", None),
    )
    return jax.shard_map(
        body,
        mesh=mesh,
        in_specs=placed,
        out_specs=(
            P("dp", "seq", "tensor", None),
            P("dp", "seq", "tensor", None),
            P(("dp", "seq"), None, "tensor"),
            P("tensor", ("dp", "seq")),
            P(("dp", "seq"), "tensor"),
            P("tensor", ("dp", "seq")),
        ),
        check_vma=False,
    )
```

```python
import math

import jax
import jax.numpy as jnp
from jax import lax
from jax.experimental import pallas as pl
from jax.experimental.pallas import tpu as pltpu
from jax.sharding import PartitionSpec as P

HEAD_DIM = 72
HEADS = 4
D = 1152
W = 288
WP = 384
SCALE = 1.0 / math.sqrt(HEAD_DIM)
EPS = 1e-6
MESH = pl.DeviceIdType.MESH
F32 = jnp.float32
BF16 = jnp.bfloat16
GELU_C = math.sqrt(2.0 / math.pi)

NN = (((1,), (0,)), ((), ()))
NT = (((1,), (1,)), ((), ()))
TN = (((0,), (0,)), ((), ()))


def rem(a, b):
    return lax.rem(a, b)


def div(a, b):
    return lax.div(a, b)


def dot(a, b, dims):
    return lax.dot_general(a, b, dims, preferred_element_type=F32)


def norm(rows):
    center = jnp.mean(rows, axis=-1, keepdims=True)
    centred = rows - center
    spread = jnp.mean(centred * centred, axis=-1, keepdims=True)
    inverse = lax.rsqrt(spread + EPS)
    return centred * inverse, inverse


def norm_back(normed, inverse, up):
    mean_grad = jnp.mean(up, axis=-1, keepdims=True)
    mean_cross = jnp.mean(up * normed, axis=-1, keepdims=True)
    return (up - mean_grad - normed * mean_cross) * inverse


JOBS = (("u", 1152, True), ("d", 1152, False), ("i", 768, True), ("v", 768, False))


def scratch_spec():
    vm = lambda *s, t=BF16: pltpu.VMEM(s, t)
    dma = lambda *s: pltpu.SemaphoreType.DMA(s)
    spec = {
        "xs": vm(8, 2, 8, D), "cy": vm(4, 2, 8, 8, D), "cg": vm(4, 8, 2, 8, D),
        "win": vm(3, WP, D), "wout": vm(WP, D), "wup": vm(D, D), "wdown": vm(D, D),
        "f": vm(4, 128, D), "s": vm(4, 128, D), "g": vm(4, 128, D), "a": vm(4, 128, D),
        "p2": vm(4, 128, D), "p5": vm(4, 128, D), "p8": vm(4, 128, D), "ag": vm(4, 128, D, t=F32),
        "r2": vm(4, 128, D), "r5": vm(4, 128, D), "r8": vm(4, 128, D),
        "qkv": vm(4, 128, 3 * WP), "probs": vm(4, 512, 128, t=F32), "att": vm(4, 128, WP),
        "act": vm(4, 128, D), "hg": vm(4, 128, D), "dqkv": vm(4, 128, 3 * WP),
        "mid": vm(128, D, t=F32), "mg": vm(128, D, t=F32),
        "ro": vm(8, 2, 8, D), "lo": vm(8, 2, 8, D), "rl": vm(2, 8, 8, D), "ll": vm(2, 8, 8, D),
        "wsem": dma(6),
        "ys": dma(8, 6), "yr": dma(8, 6),
        "ss": dma(7, 8), "sr": dma(7, 8),
        "osem": dma(2),
        "js": dma(4, 7), "jr": dma(4, 7),
    }
    for name, n, x_first in JOBS:
        spec["G" + name] = vm(2, 2, 4, 9, 8, n)
        spec["A" + name] = vm(2, 4, 9, 8, n)
        if x_first:
            spec["B" + name] = vm(4, 2, 9, 8, n)
            spec["H" + name] = vm(2, 9, 8, n)
        else:
            spec["B" + name] = vm(4, 4, 5, 8, n)
            spec["H" + name] = vm(4, 5, 8, n)
        spec["C" + name] = vm(4, 5, 8, n)
    return spec


SPEC = scratch_spec()


def kernel(lat, cot, mod, in_w, out_w, up_w, down_w, res, lgr, gu, gd, gi, go, *scratch):
    r = dict(zip(SPEC, scratch))
    dp, seq, me = lax.axis_index("dp"), lax.axis_index("seq"), lax.axis_index("tensor")
    core, z_lo = rem(dp, 2), div(dp, 2)
    x, z_hi = div(seq, 2), rem(seq, 2)
    z = z_hi * 2 + z_lo

    def remote(src, dst, send, recv, where):
        return pltpu.make_async_remote_copy(src_ref=src, dst_ref=dst, send_sem=send, recv_sem=recv, device_id=where, device_id_type=MESH)

    def local(src, dst, sem):
        return pltpu.make_async_copy(src, dst, sem)

    def seq_peer(k):
        return (dp, rem(seq + k, 8), me)

    def y_peer(k):
        return (dp, seq, rem(me + k, 4))

    def core_peer():
        return (dp + 1 - 2 * core, seq, me)

    def x_peer(k):
        return (dp, rem(x + k, 4) * 2 + z_hi, me)

    def z_peer(k):
        other = rem(z + k, 4)
        return (rem(other, 2) * 2 + core, x * 2 + div(other, 2), me)

    weights = [local(in_w.at[j], r["win"].at[j, pl.ds(0, W)], r["wsem"].at[j]) for j in range(3)]
    weights += [
        local(out_w, r["wout"].at[pl.ds(0, W)], r["wsem"].at[3]),
        local(up_w, r["wup"], r["wsem"].at[4]),
        local(down_w, r["wdown"], r["wsem"].at[5]),
    ]

    barrier = pltpu.get_barrier_semaphore()
    peers = [seq_peer(k) for k in range(1, 8)] + [y_peer(k) for k in range(1, 4)] + [core_peer()]
    peers += [z_peer(1), z_peer(3)]
    for where in peers:
        pl.semaphore_signal(barrier, inc=1, device_id=where, device_id_type=MESH)
    pl.semaphore_wait(barrier, len(peers))

    PARTS_C = (lambda v: v.at[0], lambda v: v.at[1])
    PARTS_T = (lambda v: v.at[pl.ds(0, 64)], lambda v: v.at[pl.ds(64, 64)])

    def hop(ph, buf, parts, src, k, half, n, to):
        t = rem(me + k, 4)
        piece = parts[half](buf.at[t])
        return remote(piece if src is None else parts[half](src), piece, r["ys"].at[ph, n], r["yr"].at[ph, n], y_peer(to))

    HOPS = ((0, 0, 0, 1), (0, 1, 2, 3), (0, 1, 1, 1), (0, 0, 3, 3))
    PASS = ((3, 0, 4, 1), (1, 1, 5, 3))

    def gather_start(ph, src, buf, parts):
        for k, half, n, to in HOPS:
            hop(ph, buf, parts, src, k, half, n, to).start()

    def gather_pass(ph, buf, parts):
        for n, half, frm, (k, _, m, to) in ((0, 0, 3, PASS[0]), (2, 1, 1, PASS[1])):
            hop(ph, buf, parts, None, frm, half, n, 1).wait_recv()
            hop(ph, buf, parts, None, k, half, m, to).start()

    def gather_left(ph, buf, parts):
        hop(ph, buf, parts, None, 3, 1, 1, 1).wait_recv()

    def gather_right(ph, buf, parts):
        hop(ph, buf, parts, None, 1, 0, 3, 1).wait_recv()

    def gather_far(ph, buf, parts):
        hop(ph, buf, parts, None, 2, 0, 4, 1).wait_recv()
        hop(ph, buf, parts, None, 2, 1, 5, 1).wait_recv()

    def gather_sent(ph, src, buf, parts):
        for k, half, n, to in HOPS:
            hop(ph, buf, parts, src, k, half, n, to).wait_send()
        for k, half, n, to in PASS:
            hop(ph, buf, parts, None, k, half, n, to).wait_send()

    def exchange_in(row, src, dst):
        for k in range(1, 8):
            to = rem(seq + k, 8)
            c = remote(src.at[:, to], dst.at[seq], r["ss"].at[row, k], r["sr"].at[row, k], seq_peer(k))
            c.start()
        c = local(src.at[:, seq], dst.at[seq], r["sr"].at[row, 0])
        c.start()

    def exchange_in_sent(row, src, dst):
        for k in range(1, 8):
            to = rem(seq + k, 8)
            remote(src.at[:, to], dst.at[seq], r["ss"].at[row, k], r["sr"].at[row, k], seq_peer(k)).wait_send()

    def exchange_in_wait(row, src, dst):
        local(src.at[:, seq], dst.at[seq], r["sr"].at[row, 0]).wait()
        for k in range(1, 8):
            frm = rem(seq + 8 - k, 8)
            remote(src.at[:, frm], dst.at[frm], r["ss"].at[row, k], r["sr"].at[row, k], seq_peer(k)).wait_recv()

    exchange_in(0, lat, r["xs"])
    gather_start(1, cot, r["cy"], PARTS_C)
    exchange_in(3, cot, r["cg"].at[me])
    for c in weights:
        c.start()
    for j in range(3):
        r["win"][j, W:] = jnp.zeros((WP - W, D), BF16)
    r["wout"][W:] = jnp.zeros((WP - W, D), BF16)

    def row(i):
        return mod[i]

    def halves(ref, h):
        return ref[4 * h : 4 * h + 4].astype(F32).reshape(64, D)

    def part_send(ph, src, dst, k):
        to = rem(me + k, 4)
        c = remote(src.at[to], dst.at[me], r["ys"].at[ph, k], r["yr"].at[ph, k], y_peer(k))
        c.start()

    def part_send_wait(ph, src, dst):
        for k in range(1, 4):
            remote(src.at[0], dst.at[me], r["ys"].at[ph, k], r["yr"].at[ph, k], y_peer(k)).wait_send()

    def part_wait(ph, src, dst):
        for k in range(1, 4):
            frm = rem(me + 4 - k, 4)
            remote(src.at[frm], dst.at[frm], r["ys"].at[ph, k], r["yr"].at[ph, k], y_peer(k)).wait_recv()

    def part_sum(src, dst, h):
        rows = pl.ds(64 * h, 64)
        total = src[me, rows, :].astype(F32)
        for k in (1, 2, 3):
            total = total + dst[rem(me + k, 4), rows, :].astype(F32)
        return total

    ORDER = (0, 3, 1, 2)

    def block_of(i):
        k = jnp.where(i == 1, 3, jnp.maximum(i - 1, 0))
        return k, rem(me + k, 4)

    def arrival(ph, buf, i):
        @pl.when(i == 1)
        def _():
            gather_pass(ph, buf, PARTS_T)
            gather_left(ph, buf, PARTS_T)

        @pl.when(i == 2)
        def _():
            gather_right(ph, buf, PARTS_T)

        @pl.when(i == 3)
        def _():
            gather_far(ph, buf, PARTS_T)

    def part_out(ph, src, dst, i):
        for j in (1, 2, 3):
            @pl.when(i == j)
            def _():
                part_send(ph, src, dst, ORDER[j])

    lane = lax.broadcasted_iota(jnp.int32, (128, WP), 1)
    head_masks = [(lane >= HEAD_DIM * h) & (lane < HEAD_DIM * (h + 1)) for h in range(HEADS)]
    same_pixel = rem(lax.broadcasted_iota(jnp.int32, (512, 128), 0), 8) == rem(lax.broadcasted_iota(jnp.int32, (512, 128), 1), 8)

    def stacked(v):
        zero = jnp.zeros_like(v)
        return jnp.concatenate([jnp.where(m, v, zero) for m in head_masks], axis=0)

    def side_by_side(v):
        return jnp.concatenate([v[128 * h : 128 * h + 128] for h in range(HEADS)], axis=1)

    gather_pass(1, r["cy"], PARTS_C)
    exchange_in_wait(0, lat, r["xs"])
    for h in range(2):
        normed, _ = norm(halves(r["xs"], h))
        r["f"][me, 64 * h : 64 * h + 64, :] = (normed * (1.0 + row(1)) + row(0)).astype(BF16)
    gather_start(0, None, r["f"], PARTS_T)
    for c in weights[:4]:
        c.wait()

    def attend_block(i, carry):
        k, t = block_of(i)
        arrival(0, r["f"], i)

        block = r["f"][t]
        for j in range(3):
            r["qkv"][t, :, j * WP : (j + 1) * WP] = dot(block, r["win"][j], NT).astype(BF16)
        q, kk, v = (r["qkv"][t, :, j * WP : (j + 1) * WP] for j in range(3))
        scores = dot(stacked(q), kk, NT) * SCALE
        scores = jnp.where(same_pixel, scores, -1e30)
        raised = jnp.exp(scores - jnp.max(scores, axis=-1, keepdims=True))
        probs = raised / jnp.sum(raised, axis=-1, keepdims=True)
        r["probs"][t] = probs
        att = dot(side_by_side(probs.astype(BF16)), stacked(v), NN).astype(BF16)
        r["att"][t] = att
        for n in range(3):
            cols = slice(n * 384, n * 384 + 384)
            r["p2"][t, :, cols] = dot(att, r["wout"][:, cols], NN).astype(BF16)
        part_out(2, r["p2"], r["r2"], i)
        return carry

    lax.fori_loop(0, 1, attend_block, 0)

    gather_left(1, r["cy"], PARTS_C)
    exchange_in(1 + 1, r["cy"].at[rem(me + 3, 4)], r["cg"].at[rem(me + 3, 4)])
    gather_right(1, r["cy"], PARTS_C)
    exchange_in(1 + 3, r["cy"].at[rem(me + 1, 4)], r["cg"].at[rem(me + 1, 4)])
    lax.fori_loop(1, 3, attend_block, 0)
    gather_far(1, r["cy"], PARTS_C)
    exchange_in(1 + 0, r["cy"].at[rem(me + 2, 4)], r["cg"].at[rem(me + 2, 4)])
    lax.fori_loop(3, 4, attend_block, 0)

    def branch_block(k, row_, src):
        t = rem(me + k, 4)
        exchange_in_wait(row_, src, r["cg"].at[t])
        for h in range(2):
            r["g"][t, 64 * h : 64 * h + 64, :] = (row(5) * r["cg"][t, 4 * h : 4 * h + 4].astype(F32).reshape(64, D)).astype(BF16)

    branch_block(0, 3, cot)
    branch_block(3, 2, r["cy"].at[rem(me + 3, 4)])
    branch_block(1, 4, r["cy"].at[rem(me + 1, 4)])
    branch_block(2, 1, r["cy"].at[rem(me + 2, 4)])
    weights[4].wait()
    weights[5].wait()

    def branch_back(n, c):
        cols = pl.ds(pl.multiple_of(n * 384, 384), 384)
        r["ag"][:, :, cols] = dot(r["g"][...].reshape(512, D), r["wdown"][cols, :], NT).reshape(4, 128, 384)
        return c

    lax.fori_loop(0, 3, branch_back, 0)
    part_wait(2, r["p2"], r["r2"])
    part_send_wait(2, r["p2"], r["r2"])

    for h in range(2):
        rows = slice(64 * h, 64 * h + 64)
        midway = halves(r["xs"], h) + row(2) * part_sum(r["p2"], r["r2"], h)
        r["mid"][rows, :] = midway
        normed, _ = norm(midway)
        r["s"][me, rows, :] = (normed * (1.0 + row(4)) + row(3)).astype(BF16)
    gather_start(3, None, r["s"], PARTS_T)

    def mlp_block(i, carry):
        k, t = block_of(i)
        arrival(3, r["s"], i)

        def hidden_cols(n, c):
            cols = pl.ds(pl.multiple_of(n * 384, 384), 384)
            v = dot(r["s"][t], r["wup"][:, cols], NN)
            ag = r["ag"][t, :, cols]
            th = jnp.tanh(GELU_C * (v + 0.044715 * (v * v * v)))
            r["act"][t, :, cols] = (0.5 * v * (1.0 + th)).astype(BF16)
            slope = 0.5 * (1.0 + th) + (0.5 * v) * ((1.0 - th * th) * (GELU_C * (1.0 + (3.0 * 0.044715) * (v * v))))
            r["hg"][t, :, cols] = (ag * slope).astype(BF16)
            return c

        lax.fori_loop(0, 3, hidden_cols, 0)

        def grad_cols(n, c):
            cols = pl.ds(pl.multiple_of(n * 384, 384), 384)
            r["p5"][t, :, cols] = dot(r["hg"][t], r["wup"][cols, :], NT).astype(BF16)
            return c

        lax.fori_loop(0, 3, grad_cols, 0)
        part_out(4, r["p5"], r["r5"], i)
        return carry

    lax.fori_loop(0, 4, mlp_block, 0)

    def weight_grad(lhs, rhs, width, name, at):
        def rows_step(m, c):
            cols = pl.ds(pl.multiple_of(m * 384, 384), 384)
            left = lhs[:, :, cols].reshape(512, 384)
            right = rhs().reshape(512, width)
            out = dot(left, right, TN).astype(BF16).reshape(48, 8, width)
            for q in range(48 // 3):
                grp = m * 16 + q
                outer = div(grp, 3)
                r["G" + name][div(outer, 8), rem(div(outer, 4), 2), rem(outer, 4), pl.ds(rem(grp, 3) * 3, 3), :, at : at + width] = out[3 * q : 3 * q + 3]
            return c

        lax.fori_loop(0, 3, rows_step, 0)

    def job(index):
        name, n, x_first = JOBS[index]
        return name, n, x_first

    def job_core(index, start):
        name, n, _ = JOBS[index]
        to = 1 - core if start else core
        c = remote(r["G" + name].at[:, 1 - core], r["A" + name], r["js"].at[index, 0], r["jr"].at[index, 0], core_peer())
        if start:
            c.start()
        else:
            c.wait()

    def job_core_sum(index):
        name, n, _ = JOBS[index]

        def step(i, c):
            a, b = div(i, 4), rem(i, 4)
            total = r["A" + name][a, b].astype(F32) + r["G" + name][a, core, b].astype(F32)
            r["A" + name][a, b] = total.astype(BF16)
            return c

        lax.fori_loop(0, 8, step, 0)

    def job_first(index, start):
        name, n, x_first = JOBS[index]
        for k in (2, 1, 3):
            if x_first:
                src = r["A" + name].at[:, rem(x + k, 4)]
                mine, frm, where = x, rem(x + 4 - k, 4), x_peer(k)
            else:
                other = rem(z + k, 4)
                src = r["A" + name].at[rem(other, 2), :, pl.ds(4 * div(other, 2), 5)]
                mine, frm, where = z, rem(z + 4 - k, 4), z_peer(k)
            if start:
                remote(src, r["B" + name].at[mine], r["js"].at[index, k], r["jr"].at[index, k], where).start()
            else:
                remote(src, r["B" + name].at[frm], r["js"].at[index, k], r["jr"].at[index, k], where).wait()

    def job_first_sum(index):
        name, n, x_first = JOBS[index]
        if x_first:
            for a in range(2):
                total = r["A" + name][a, x].astype(F32)
                for k in (1, 2, 3):
                    total = total + r["B" + name][rem(x + k, 4), a].astype(F32)
                r["H" + name][a] = total.astype(BF16)
        else:
            for b in range(4):
                total = r["A" + name][z_lo, b, pl.ds(4 * z_hi, 5)].astype(F32)
                for k in (1, 2, 3):
                    total = total + r["B" + name][rem(z + k, 4), b].astype(F32)
                r["H" + name][b] = total.astype(BF16)

    def job_second(index, start):
        name, n, x_first = JOBS[index]
        for k in (2, 1, 3):
            if x_first:
                other = rem(z + k, 4)
                src = r["H" + name].at[rem(other, 2), pl.ds(4 * div(other, 2), 5)]
                mine, frm, where = z, rem(z + 4 - k, 4), z_peer(k)
            else:
                src = r["H" + name].at[rem(x + k, 4)]
                mine, frm, where = x, rem(x + 4 - k, 4), x_peer(k)
            if start:
                remote(src, r["C" + name].at[mine], r["js"].at[index, 3 + k], r["jr"].at[index, 3 + k], where).start()
            else:
                remote(src, r["C" + name].at[frm], r["js"].at[index, 3 + k], r["jr"].at[index, 3 + k], where).wait()

    def job_second_sum(index):
        name, n, x_first = JOBS[index]
        if x_first:
            total = r["H" + name][z_lo, pl.ds(4 * z_hi, 5)].astype(F32)
            at = z
        else:
            total = r["H" + name][x].astype(F32)
            at = x
        for k in (1, 2, 3):
            total = total + r["C" + name][rem(at + k, 4)].astype(F32)
        total = total.reshape(40, n)
        return jnp.where(z_hi == 0, total[:36], total[4:]).astype(BF16)

    weight_grad(r["s"], lambda: r["hg"][...], D, "u", 0)
    job_core(0, True)
    weight_grad(r["g"], lambda: r["act"][...], D, "d", 0)
    job_core(1, True)
    job_core(0, False)
    job_core_sum(0)
    job_first(0, True)

    def result_block(i, carry):
        t = rem(me + i, 4)

        def result_cols(n, c):
            cols = pl.ds(pl.multiple_of(n * 384, 384), 384)
            r["p8"][t, :, cols] = dot(r["act"][t], r["wdown"][:, cols], NN).astype(BF16)
            return c

        lax.fori_loop(0, 3, result_cols, 0)
        return carry

    part_wait(4, r["p5"], r["r5"])
    for h in range(2):
        rows = slice(64 * h, 64 * h + 64)
        normed, inverse = norm(r["mid"][rows, :])
        back = norm_back(normed, inverse, part_sum(r["p5"], r["r5"], h) * (1.0 + row(4)))
        mg = r["cg"][me, 4 * h : 4 * h + 4].astype(F32).reshape(64, D) + back
        r["mg"][rows, :] = mg
        r["a"][me, rows, :] = (row(2) * mg).astype(BF16)
    gather_start(5, None, r["a"], PARTS_T)
    job_core(1, False)
    job_core_sum(1)
    job_first(1, True)
    lax.fori_loop(0, 2, result_block, 0)

    def attend_back_block(i, carry):
        k, t = block_of(i)
        arrival(5, r["a"], i)

        grad = dot(r["a"][t], r["wout"][...], NT).astype(BF16)
        q, kk, v = (r["qkv"][t, :, j * WP : (j + 1) * WP] for j in range(3))
        qs, gs = stacked(q), stacked(grad)
        probs = r["probs"][t]
        dv = dot(probs.astype(BF16), gs, TN)
        dp_ = dot(gs, v, NT)
        ds = (probs * (dp_ - jnp.sum(probs * dp_, axis=-1, keepdims=True)) * SCALE).astype(BF16)
        dq = dot(side_by_side(ds), stacked(kk), NN)
        dk = dot(ds, qs, TN)
        for j, part in enumerate((dq, dk, dv)):
            r["dqkv"][t, :, j * WP : (j + 1) * WP] = part.astype(BF16)
        for n in range(3):
            cols = slice(n * 384, n * 384 + 384)
            total = dot(r["dqkv"][t, :, 0:WP], r["win"][0, :, cols], NN)
            for j in (1, 2):
                total = total + dot(r["dqkv"][t, :, j * WP : (j + 1) * WP], r["win"][j, :, cols], NN)
            r["p2"][t, :, cols] = total.astype(BF16)
        part_out(6, r["p2"], r["r2"], i)
        return carry

    lax.fori_loop(0, 1, attend_back_block, 0)
    lax.fori_loop(1, 4, attend_back_block, 0)

    weight_grad(r["f"], lambda: r["dqkv"][:, :, 0:768], 768, "i", 0)
    job_core(2, True)
    weight_grad(r["f"], lambda: r["dqkv"][:, :, 768:1152], 384, "v", 0)
    weight_grad(r["a"], lambda: r["att"][...], 384, "v", 384)
    job_core(3, True)
    for index in (0, 1):
        job_first(index, False)
        job_first_sum(index)
        job_second(index, True)
    lax.fori_loop(2, 4, result_block, 0)
    for k in (1, 3, 2):
        part_send(7, r["p8"], r["r8"], k)
    for index in (2, 3):
        job_core(index, False)
        job_core_sum(index)
        job_first(index, True)

    def exchange_out(row_, src, dst):
        for k in range(1, 8):
            to = rem(seq + k, 8)
            remote(src.at[to], dst.at[:, seq], r["ss"].at[row_, k], r["sr"].at[row_, k], seq_peer(k)).start()
        local(src.at[seq], dst.at[:, seq], r["sr"].at[row_, 0]).start()

    def exchange_out_wait(row_, src, dst):
        local(src.at[seq], dst.at[:, seq], r["sr"].at[row_, 0]).wait()
        for k in range(1, 8):
            frm = rem(seq + 8 - k, 8)
            remote(src.at[frm], dst.at[:, frm], r["ss"].at[row_, k], r["sr"].at[row_, k], seq_peer(k)).wait()

    part_wait(6, r["p2"], r["r2"])
    for h in range(2):
        rows = slice(64 * h, 64 * h + 64)
        normed, inverse = norm(halves(r["xs"], h))
        back = norm_back(normed, inverse, part_sum(r["p2"], r["r2"], h) * (1.0 + row(1)))
        out = r["mg"][rows, :] + back
        r["lo"][4 * h : 4 * h + 4] = out.astype(BF16).reshape(4, 2, 8, D)
    exchange_out(6, r["lo"], r["ll"])

    for index, out in ((0, gu), (1, gd)):
        job_second(index, False)
        out[...] = job_second_sum(index)
    job_first(2, False)
    job_first_sum(2)
    job_second(2, True)

    part_wait(7, r["p8"], r["r8"])
    for h in range(2):
        rows = slice(64 * h, 64 * h + 64)
        out = r["mid"][rows, :] + row(5) * part_sum(r["p8"], r["r8"], h)
        r["ro"][4 * h : 4 * h + 4] = out.astype(BF16).reshape(4, 2, 8, D)
    exchange_out(5, r["ro"], r["rl"])

    job_first(3, False)
    job_first_sum(3)
    job_second(3, True)
    exchange_out_wait(6, r["lo"], r["ll"])
    exchange_out_wait(5, r["ro"], r["rl"])
    done = [local(r["rl"], res, r["osem"].at[0]), local(r["ll"], lgr, r["osem"].at[1])]
    for c in done:
        c.start()
    job_second(2, False)
    part = job_second_sum(2)
    gi[0] = part[:, :W]
    gi[1] = part[:, WP : WP + W]
    job_second(3, False)
    part = job_second_sum(3)
    gi[2] = part[:, :W]
    go[...] = part[:, WP : WP + W]
    for row_, src, dst in (
        (0, lat, r["xs"]),
        (3, cot, r["cg"].at[me]),
        (2, r["cy"].at[rem(me + 3, 4)], r["cg"].at[rem(me + 3, 4)]),
        (4, r["cy"].at[rem(me + 1, 4)], r["cg"].at[rem(me + 1, 4)]),
        (1, r["cy"].at[rem(me + 2, 4)], r["cg"].at[rem(me + 2, 4)]),
    ):
        exchange_in_sent(row_, src, dst)
    gather_sent(1, cot, r["cy"], PARTS_C)
    for ph, buf in ((0, "f"), (3, "s"), (5, "a")):
        gather_sent(ph, None, r[buf], PARTS_T)
    for ph, src, dst in ((4, "p5", "r5"), (6, "p2", "r2"), (7, "p8", "r8")):
        part_send_wait(ph, r[src], r[dst])
    for c in done:
        c.wait()


def body(latents, modulation, in_weight, out_weight, up_weight, down_weight, cotangent):
    vmem = pl.BlockSpec(memory_space=pltpu.VMEM)
    anywhere = pl.BlockSpec(memory_space=pl.ANY)
    out = lambda *s: jax.ShapeDtypeStruct(s, BF16)
    shapes = (out(2, 8, 8, D), out(2, 8, 8, D), out(36, D), out(36, D), out(3, 36, W), out(36, W))
    found = pl.pallas_call(
        kernel,
        out_shape=shapes,
        in_specs=[anywhere, anywhere, vmem, anywhere, anywhere, anywhere, anywhere],
        out_specs=(anywhere, anywhere, vmem, vmem, vmem, vmem),
        scratch_shapes=list(SPEC.values()),
        compiler_params=pltpu.CompilerParams(collective_id=0, has_side_effects=True, vmem_limit_bytes=67043328),
        name="block",
    )(
        latents.reshape(2, 8, 8, D),
        cotangent.reshape(2, 8, 8, D),
        jnp.transpose(modulation, (1, 0, 2)),
        jnp.transpose(in_weight, (1, 2, 0)),
        out_weight,
        up_weight,
        down_weight,
    )
    res, lgr, gu, gd, gi, go = pl.pallas_call(
        hand_over,
        out_shape=shapes,
        in_specs=[anywhere] * 6,
        out_specs=(anywhere,) * 6,
        scratch_shapes=[pltpu.VMEM(v.shape, BF16) for v in shapes] + [pltpu.SemaphoreType.DMA((2, 6))],
        name="hand_over",
    )(*found)
    return (
        res.reshape(latents.shape),
        lgr.reshape(latents.shape),
        jnp.transpose(gi, (1, 0, 2)),
        go.T,
        gu,
        gd.T,
    )


def hand_over(*refs):
    given, outs, held, sems = refs[:6], refs[6:12], refs[12:18], refs[18]
    into = [pltpu.make_async_copy(a, b, sems.at[0, i]) for i, (a, b) in enumerate(zip(given, held))]
    back = [pltpu.make_async_copy(a, b, sems.at[1, i]) for i, (a, b) in enumerate(zip(held, outs))]
    for c in into:
        c.start()
    for c, d in zip(into, back):
        c.wait()
        d.start()
    for d in back:
        d.wait()


def solution(mesh):
    placed = (
        P("dp", "seq", "tensor", None),
        P("dp", None, None),
        P(None, None, "tensor"),
        P("tensor", None),
        P(None, "tensor"),
        P("tensor", None),
        P("dp", "seq", "tensor", None),
    )
    return jax.shard_map(
        body,
        mesh=mesh,
        in_specs=placed,
        out_specs=(
            P("dp", "seq", "tensor", None),
            P("dp", "seq", "tensor", None),
            P(("dp", "seq"), None, "tensor"),
            P("tensor", ("dp", "seq")),
            P(("dp", "seq"), "tensor"),
            P("tensor", ("dp", "seq")),
        ),
        check_vma=False,
    )
```

```python
import math

import jax
import jax.numpy as jnp
from jax import lax
from jax.experimental import pallas as pl
from jax.experimental.pallas import tpu as pltpu
from jax.sharding import PartitionSpec as P

HEAD_DIM = 72
HEADS = 4
D = 1152
W = 288
WP = 384
SCALE = 1.0 / math.sqrt(HEAD_DIM)
EPS = 1e-6
MESH = pl.DeviceIdType.MESH
F32 = jnp.float32
BF16 = jnp.bfloat16
GELU_C = math.sqrt(2.0 / math.pi)

NN = (((1,), (0,)), ((), ()))
NT = (((1,), (1,)), ((), ()))
TN = (((0,), (0,)), ((), ()))


def rem(a, b):
    return lax.rem(a, b)


def div(a, b):
    return lax.div(a, b)


def dot(a, b, dims):
    return lax.dot_general(a, b, dims, preferred_element_type=F32)


def norm(rows):
    center = jnp.mean(rows, axis=-1, keepdims=True)
    centred = rows - center
    spread = jnp.mean(centred * centred, axis=-1, keepdims=True)
    inverse = lax.rsqrt(spread + EPS)
    return centred * inverse, inverse


def norm_back(normed, inverse, up):
    mean_grad = jnp.mean(up, axis=-1, keepdims=True)
    mean_cross = jnp.mean(up * normed, axis=-1, keepdims=True)
    return (up - mean_grad - normed * mean_cross) * inverse


JOBS = (("u", 1152, True), ("d", 1152, False), ("o", 640, True), ("p", 512, False), ("i", 512, True), ("v", 384, False))
CI = 896


def scratch_spec():
    vm = lambda *s, t=BF16: pltpu.VMEM(s, t)
    dma = lambda *s: pltpu.SemaphoreType.DMA(s)
    spec = {
        "xs": vm(8, 2, 8, D), "cy": vm(4, 2, 8, 8, D), "cg": vm(4, 8, 2, 8, D),
        "win": vm(3, WP, D), "wo": vm(4, 48, 8, D), "wup": vm(D, D), "wdown": vm(D, D),
        "f": vm(4, 128, D), "s": vm(4, 128, D), "g": vm(4, 128, D), "ao": vm(128, D),
        "p5": vm(4, 128, D), "p7": vm(4, 128, D), "ag": vm(4, 128, D, t=F32),
        "r5": vm(4, 128, D), "r7": vm(4, 128, D), "r8": vm(4, 128, D),
        "qkv": vm(4, 128, 3 * WP), "probs": vm(4, 512, 128, t=F32),
        "as": vm(4, 128, WP), "at": vm(4, 128, WP), "ds": vm(4, 128, WP), "da": vm(4, 128, WP), "attc": vm(128, D),
        "act": vm(4, 128, D), "hg": vm(4, 128, D), "dqkv": vm(4, 128, 3 * WP), "dqc": vm(4, 128, CI),
        "mid": vm(128, D, t=F32), "mg": vm(128, D, t=F32),
        "ro": vm(8, 2, 8, D), "lo": vm(8, 2, 8, D), "rl": vm(2, 8, 8, D), "ll": vm(2, 8, 8, D),
        "oy": vm(4, 40, WP), "or": vm(4, 40, WP),
        "wsem": dma(6),
        "ys": dma(10, 6), "yr": dma(10, 6),
        "ss": dma(7, 8), "sr": dma(7, 8),
        "osem": dma(2),
        "js": dma(6, 7), "jr": dma(6, 7),
        "ws": dma(4, 4), "wr": dma(4, 4),
    }
    for name, n, x_first in JOBS:
        spec["G" + name] = vm(2, 2, 4, 9, 8, n)
        spec["A" + name] = vm(2, 4, 9, 8, n)
        if x_first:
            spec["B" + name] = vm(3, 2, 9, 8, n)
            spec["H" + name] = vm(2, 9, 8, n)
        else:
            spec["B" + name] = vm(3, 4, 5, 8, n)
            spec["H" + name] = vm(4, 5, 8, n)
        spec["C" + name] = vm(3, 5, 8, n)
    return spec


SPEC = scratch_spec()

TO = {1: 3, 2: 1, 3: 2}
BACK = {1: 2, 2: 1, 3: 3}
HOPS = ((0, 1, 0, 1), (1, 1, 0, 1), (1, 3, 0, 2), (0, 3, 0, 2), (0, 1, 1, 3), (1, 3, 2, 3))
PARTS_C = (lambda v: v.at[0], lambda v: v.at[1])
PARTS_T = (lambda v: v.at[pl.ds(0, 64)], lambda v: v.at[pl.ds(64, 64)])


def kernel(lat, cot, mod, in_w, out_w, up_w, down_w, res, lgr, gu, gd, gi, go, *scratch):
    r = dict(zip(SPEC, scratch))
    dp, seq, me = lax.axis_index("dp"), lax.axis_index("seq"), lax.axis_index("tensor")
    core, z_lo = rem(dp, 2), div(dp, 2)
    x, z_hi = div(seq, 2), rem(seq, 2)
    z = z_hi * 2 + z_lo

    def remote(src, dst, send, recv, where):
        return pltpu.make_async_remote_copy(src_ref=src, dst_ref=dst, send_sem=send, recv_sem=recv, device_id=where, device_id_type=MESH)

    def local(src, dst, sem):
        return pltpu.make_async_copy(src, dst, sem)

    def seq_peer(k):
        return (dp, rem(seq + k, 8), me)

    def y_peer(k):
        return (dp, seq, rem(me + k, 4))

    def core_peer():
        return (dp + 1 - 2 * core, seq, me)

    def x_peer(k):
        return (dp, rem(x + k, 4) * 2 + z_hi, me)

    def z_peer(k):
        other = rem(z + k, 4)
        return (rem(other, 2) * 2 + core, x * 2 + div(other, 2), me)

    weights = [local(in_w.at[j], r["win"].at[j, pl.ds(0, W)], r["wsem"].at[j]) for j in range(3)]
    weights += [
        local(out_w, r["wo"].at[0, pl.ds(0, 36)], r["wsem"].at[3]),
        local(up_w, r["wup"], r["wsem"].at[4]),
        local(down_w, r["wdown"], r["wsem"].at[5]),
    ]

    barrier = pltpu.get_barrier_semaphore()
    peers = [seq_peer(k) for k in range(1, 8)] + [y_peer(k) for k in range(1, 4)] + [core_peer()]
    peers += [z_peer(1), z_peer(3)]
    for where in peers:
        pl.semaphore_signal(barrier, inc=1, device_id=where, device_id_type=MESH)
    pl.semaphore_wait(barrier, len(peers))

    def hop(ph, buf, parts, n, src=None):
        half, to, at, there = HOPS[n]
        given = buf.at[at] if src is None or at else src
        return remote(parts[half](given), parts[half](buf.at[there]), r["ys"].at[ph, n], r["yr"].at[ph, n], y_peer(to))

    def gather_start(ph, buf, parts, src=None, hops=(0, 2, 1, 3)):
        for n in hops:
            hop(ph, buf, parts, n, src).start()

    def gather_pass(ph, buf, parts):
        hop(ph, buf, parts, 0).wait_recv()
        hop(ph, buf, parts, 4).start()
        hop(ph, buf, parts, 2).wait_recv()
        hop(ph, buf, parts, 5).start()

    def gather_near(ph, buf, parts):
        hop(ph, buf, parts, 1).wait_recv()
        hop(ph, buf, parts, 3).wait_recv()

    def gather_far(ph, buf, parts):
        hop(ph, buf, parts, 4).wait_recv()
        hop(ph, buf, parts, 5).wait_recv()

    def gather_sent(ph, buf, parts, src=None):
        for n in range(6):
            hop(ph, buf, parts, n, src).wait_send()

    def part(ph, src, dst, k):
        return remote(src.at[k], dst.at[BACK[k]], r["ys"].at[ph, k], r["yr"].at[ph, BACK[k]], y_peer(TO[k]))

    def part_wait(ph, src, dst, slots=(1, 2, 3)):
        for k in slots:
            part(ph, src, dst, BACK[k]).wait_recv()

    def part_send_wait(ph, src, dst):
        for k in (1, 2, 3):
            part(ph, src, dst, k).wait_send()

    def part_sum(src, dst, h):
        rows = slice(64 * h, 64 * h + 64)
        total = src[0, rows, :].astype(F32)
        for k in (1, 2, 3):
            total = total + dst[k, rows, :].astype(F32)
        return total

    def exchange_in(row_, src, dst):
        for k in range(1, 8):
            to = rem(seq + k, 8)
            remote(src.at[:, to], dst.at[seq], r["ss"].at[row_, k], r["sr"].at[row_, k], seq_peer(k)).start()
        local(src.at[:, seq], dst.at[seq], r["sr"].at[row_, 0]).start()

    def exchange_in_sent(row_, src, dst):
        for k in range(1, 8):
            to = rem(seq + k, 8)
            remote(src.at[:, to], dst.at[seq], r["ss"].at[row_, k], r["sr"].at[row_, k], seq_peer(k)).wait_send()

    def exchange_in_wait(row_, src, dst):
        local(src.at[:, seq], dst.at[seq], r["sr"].at[row_, 0]).wait()
        for k in range(1, 8):
            frm = rem(seq + 8 - k, 8)
            remote(src.at[:, frm], dst.at[frm], r["ss"].at[row_, k], r["sr"].at[row_, k], seq_peer(k)).wait_recv()

    def exchange_out(row_, src, dst):
        for k in range(1, 8):
            to = rem(seq + k, 8)
            remote(src.at[to], dst.at[:, seq], r["ss"].at[row_, k], r["sr"].at[row_, k], seq_peer(k)).start()
        local(src.at[seq], dst.at[:, seq], r["sr"].at[row_, 0]).start()

    def exchange_out_wait(row_, src, dst):
        local(src.at[seq], dst.at[:, seq], r["sr"].at[row_, 0]).wait()
        for k in range(1, 8):
            frm = rem(seq + 8 - k, 8)
            remote(src.at[frm], dst.at[:, frm], r["ss"].at[row_, k], r["sr"].at[row_, k], seq_peer(k)).wait()

    SHARE = {1: (core == 1, z, z_peer), 2: (core == 0, x, x_peer), 3: (core == z_lo, x, x_peer)}

    def rows_of(q):
        return pl.ds(9 * q, 9)

    def share_y(slot):
        _, q, _ = SHARE[slot]
        return remote(out_w.at[rows_of(q)], r["wo"].at[slot, rows_of(q)], r["ws"].at[slot, 0], r["wr"].at[slot, 0], y_peer(TO[BACK[slot]]))

    def share_line(slot, k, back):
        _, q, peer = SHARE[slot]
        at = rem(q + 4 - k, 4) if back else q
        piece = r["wo"].at[slot, rows_of(at)]
        return remote(piece, piece, r["ws"].at[slot, k], r["wr"].at[slot, k], peer(k))

    def share_core(slot):
        piece = r["wo"].at[slot, pl.ds(0, 36)]
        return remote(piece, piece, r["ws"].at[0, slot], r["wr"].at[0, slot], core_peer())

    def share_start():
        for slot in (1, 2, 3):
            @pl.when(SHARE[slot][0])
            def _(slot=slot):
                share_y(slot).start()

    def share_second():
        for slot in (1, 2, 3):
            @pl.when(SHARE[slot][0])
            def _(slot=slot):
                share_y(slot).wait_recv()
                for k in (2, 1, 3):
                    share_line(slot, k, False).start()

    def share_third():
        for slot in (1, 2, 3):
            @pl.when(SHARE[slot][0])
            def _(slot=slot):
                for k in (1, 2, 3):
                    share_line(slot, k, True).wait_recv()
                share_core(slot).start()

    def share_wait():
        for slot in (1, 2, 3):
            @pl.when(jnp.logical_not(SHARE[slot][0]))
            def _(slot=slot):
                share_core(slot).wait_recv()

    def share_sent():
        for slot in (1, 2, 3):
            @pl.when(SHARE[slot][0])
            def _(slot=slot):
                share_y(slot).wait_send()
                for k in (1, 2, 3):
                    share_line(slot, k, False).wait_send()
                share_core(slot).wait_send()

    def row(i):
        return mod[i]

    def halves(ref, h):
        return ref[4 * h : 4 * h + 4].astype(F32).reshape(64, D)

    lane = lax.broadcasted_iota(jnp.int32, (128, WP), 1)
    head_masks = [(lane >= HEAD_DIM * h) & (lane < HEAD_DIM * (h + 1)) for h in range(HEADS)]
    same_pixel = rem(lax.broadcasted_iota(jnp.int32, (512, 128), 0), 8) == rem(lax.broadcasted_iota(jnp.int32, (512, 128), 1), 8)

    def stacked(v):
        zero = jnp.zeros_like(v)
        return jnp.concatenate([jnp.where(m, v, zero) for m in head_masks], axis=0)

    def side_by_side(v):
        return jnp.concatenate([v[128 * h : 128 * h + 128] for h in range(HEADS)], axis=1)

    def columns(n):
        return pl.ds(pl.multiple_of(n * 384, 384), 384)

    exchange_in(0, lat, r["xs"])
    share_start()
    gather_start(1, r["cy"], PARTS_C, cot, (0, 2))
    for c in weights:
        c.start()
    for j in range(3):
        r["win"][j, W:] = jnp.zeros((WP - W, D), BF16)
    for k in range(4):
        r["wo"][k, 36:] = jnp.zeros((12, 8, D), BF16)
    r["dqc"][:, :, 768:] = jnp.zeros((4, 128, 128), BF16)

    exchange_in_wait(0, lat, r["xs"])
    for h in range(2):
        normed, _ = norm(halves(r["xs"], h))
        r["f"][0, 64 * h : 64 * h + 64, :] = (normed * (1.0 + row(1)) + row(0)).astype(BF16)
    gather_start(0, r["f"], PARTS_T)
    share_second()
    exchange_in(3, cot, r["cg"].at[0])
    for c in weights[:4]:
        c.wait()

    def attend(lo, n):
        block = r["f"][lo : lo + n].reshape(n * 128, D)
        for j in range(3):
            r["qkv"][lo : lo + n, :, j * WP : (j + 1) * WP] = dot(block, r["win"][j], NT).astype(BF16).reshape(n, 128, WP)
        for t in range(lo, lo + n):
            q, kk, v = (r["qkv"][t, :, j * WP : (j + 1) * WP] for j in range(3))
            scores = dot(stacked(q), kk, NT) * SCALE
            scores = jnp.where(same_pixel, scores, -1e30)
            raised = jnp.exp(scores - jnp.max(scores, axis=-1, keepdims=True))
            probs = raised / jnp.sum(raised, axis=-1, keepdims=True)
            r["probs"][t] = probs
            att = dot(side_by_side(probs.astype(BF16)), stacked(v), NN).astype(BF16)
            if t == 0:
                r["at"][0] = att
            else:
                r["as"][t] = att
                part(2, r["as"], r["at"], t).start()

    attend(0, 1)
    gather_pass(0, r["f"], PARTS_T)
    gather_start(1, r["cy"], PARTS_C, cot, (1, 3))
    gather_near(0, r["f"], PARTS_T)
    attend(1, 2)
    share_third()
    gather_far(0, r["f"], PARTS_T)
    attend(3, 1)
    gather_pass(1, r["cy"], PARTS_C)
    gather_near(1, r["cy"], PARTS_C)
    exchange_in(1, r["cy"].at[1], r["cg"].at[1])
    exchange_in(2, r["cy"].at[2], r["cg"].at[2])

    def branch_block(k, row_, src):
        exchange_in_wait(row_, src, r["cg"].at[k])
        for h in range(2):
            r["g"][k, 64 * h : 64 * h + 64, :] = (row(5) * r["cg"][k, 4 * h : 4 * h + 4].astype(F32).reshape(64, D)).astype(BF16)

    def branch_back(lo, m):
        def step(n, c):
            block = r["g"][lo : lo + m].reshape(m * 128, D)
            r["ag"][lo : lo + m, :, columns(n)] = dot(block, r["wdown"][columns(n), :], NT).reshape(m, 128, 384)
            return c

        lax.fori_loop(0, 3, step, 0)

    share_wait()
    part_wait(2, r["as"], r["at"])

    attended = jnp.concatenate([r["at"][k] for k in range(4)], axis=1)
    for n in range(3):
        cols = slice(n * 384, n * 384 + 384)
        r["mid"][:, cols] = dot(attended, r["wo"][:, :, :, cols].reshape(4 * WP, 384), NN)
    for h in range(2):
        rows = slice(64 * h, 64 * h + 64)
        midway = halves(r["xs"], h) + row(2) * r["mid"][rows, :]
        r["mid"][rows, :] = midway
        normed, _ = norm(midway)
        r["s"][0, rows, :] = (normed * (1.0 + row(4)) + row(3)).astype(BF16)
    gather_start(3, r["s"], PARTS_T)

    def mlp(lo, m):
        def hidden_cols(n, c):
            v = dot(r["s"][lo : lo + m].reshape(m * 128, D), r["wup"][:, columns(n)], NN)
            ag = r["ag"][lo : lo + m, :, columns(n)].reshape(m * 128, 384)
            th = jnp.tanh(GELU_C * (v + 0.044715 * (v * v * v)))
            r["act"][lo : lo + m, :, columns(n)] = (0.5 * v * (1.0 + th)).astype(BF16).reshape(m, 128, 384)
            slope = 0.5 * (1.0 + th) + (0.5 * v) * ((1.0 - th * th) * (GELU_C * (1.0 + (3.0 * 0.044715) * (v * v))))
            r["hg"][lo : lo + m, :, columns(n)] = (ag * slope).astype(BF16).reshape(m, 128, 384)
            return c

        lax.fori_loop(0, 3, hidden_cols, 0)

        def grad_cols(n, c):
            out = dot(r["hg"][lo : lo + m].reshape(m * 128, D), r["wup"][columns(n), :], NT)
            r["p5"][lo : lo + m, :, columns(n)] = out.astype(BF16).reshape(m, 128, 384)
            return c

        lax.fori_loop(0, 3, grad_cols, 0)
        for t in range(max(lo, 1), lo + m):
            part(4, r["p5"], r["r5"], t).start()

    branch_block(0, 3, cot)
    weights[4].wait()
    weights[5].wait()
    branch_block(1, 1, r["cy"].at[1])
    branch_block(2, 2, r["cy"].at[2])
    branch_back(0, 3)
    gather_far(1, r["cy"], PARTS_C)
    exchange_in(4, r["cy"].at[3], r["cg"].at[3])
    gather_pass(3, r["s"], PARTS_T)
    mlp(0, 1)
    for k in range(4):
        r["attc"][:, W * k : W * k + W] = r["at"][k, :, :W]
    gather_near(3, r["s"], PARTS_T)
    mlp(1, 2)
    branch_block(3, 4, r["cy"].at[3])
    branch_back(3, 1)
    gather_far(3, r["s"], PARTS_T)
    mlp(3, 1)

    def weight_grad(left_of, right_of, width, *targets):
        def rows_step(m, c):
            out = dot(left_of(columns(m)), right_of(), TN).astype(BF16).reshape(48, 8, width)
            for q in range(16):
                grp = m * 16 + q
                outer = div(grp, 3)
                for name, at, size in targets:
                    to = r["G" + name].at[div(outer, 8), rem(div(outer, 4), 2), rem(outer, 4), pl.ds(rem(grp, 3) * 3, 3)]
                    to[...] = out[3 * q : 3 * q + 3, :, at : at + size]
            return c

        lax.fori_loop(0, 3, rows_step, 0)

    def every(name):
        return lambda cols: r[name][:, :, cols].reshape(512, 384)

    def job_core(index, start):
        name, n, _ = JOBS[index]
        c = remote(r["G" + name].at[:, 1 - core], r["A" + name], r["js"].at[index, 0], r["jr"].at[index, 0], core_peer())
        if start:
            c.start()
        else:
            c.wait()

    def job_core_sum(index):
        name, n, _ = JOBS[index]

        def step(i, c):
            a, b = div(i, 4), rem(i, 4)
            total = r["A" + name][a, b].astype(F32) + r["G" + name][a, core, b].astype(F32)
            r["A" + name][a, b] = total.astype(BF16)
            return c

        lax.fori_loop(0, 8, step, 0)

    def job_first(index, start):
        name, n, x_first = JOBS[index]
        for k in (2, 1, 3):
            if x_first:
                src = r["A" + name].at[:, rem(x + k, 4)]
                where = x_peer(k)
            else:
                other = rem(z + k, 4)
                src = r["A" + name].at[rem(other, 2), :, pl.ds(4 * div(other, 2), 5)]
                where = z_peer(k)
            c = remote(src, r["B" + name].at[k - 1], r["js"].at[index, k], r["jr"].at[index, k], where)
            if start:
                c.start()
            else:
                c.wait()

    def job_first_sum(index):
        name, n, x_first = JOBS[index]
        for a in range(2 if x_first else 4):
            mine = r["A" + name][a, x] if x_first else r["A" + name][z_lo, a, pl.ds(4 * z_hi, 5)]
            total = mine.astype(F32)
            for k in range(3):
                total = total + r["B" + name][k, a].astype(F32)
            r["H" + name][a] = total.astype(BF16)

    def job_second(index, start):
        name, n, x_first = JOBS[index]
        for k in (2, 1, 3):
            if x_first:
                other = rem(z + k, 4)
                src = r["H" + name].at[rem(other, 2), pl.ds(4 * div(other, 2), 5)]
                where = z_peer(k)
            else:
                src = r["H" + name].at[rem(x + k, 4)]
                where = x_peer(k)
            c = remote(src, r["C" + name].at[k - 1], r["js"].at[index, 3 + k], r["jr"].at[index, 3 + k], where)
            if start:
                c.start()
            else:
                c.wait()

    def job_second_sum(index):
        name, n, x_first = JOBS[index]
        mine = r["H" + name][z_lo, pl.ds(4 * z_hi, 5)] if x_first else r["H" + name][x]
        total = mine.astype(F32)
        for k in range(3):
            total = total + r["C" + name][k].astype(F32)
        total = total.reshape(40, n)
        return jnp.where(z_hi == 0, total[:36], total[4:])

    def core_step(index):
        job_core(index, False)
        job_core_sum(index)
        job_first(index, True)

    def first_step(index):
        job_first(index, False)
        job_first_sum(index)
        job_second(index, True)

    weight_grad(every("s"), lambda: r["hg"][...].reshape(512, D), D, ("u", 0, D))
    job_core(0, True)
    weight_grad(every("g"), lambda: r["act"][...].reshape(512, D), D, ("d", 0, D))
    job_core(1, True)
    core_step(0)
    core_step(1)

    part_wait(4, r["p5"], r["r5"])
    for h in range(2):
        rows = slice(64 * h, 64 * h + 64)
        normed, inverse = norm(r["mid"][rows, :])
        back = norm_back(normed, inverse, part_sum(r["p5"], r["r5"], h) * (1.0 + row(4)))
        mg = halves(r["cg"].at[0], h) + back
        r["mg"][rows, :] = mg
        r["ao"][rows, :] = (row(2) * mg).astype(BF16)
    for k in (3, 1, 2, 0):
        grad = dot(r["ao"][...], r["wo"][k].reshape(WP, D), NT).astype(BF16)
        if k:
            r["ds"][k] = grad
            part(5, r["ds"], r["da"], k).start()
        else:
            r["da"][0] = grad
    weight_grad(lambda cols: r["ao"][:, cols], lambda: r["attc"][...], D, ("o", 0, 640), ("p", 640, 512))
    job_core(2, True)
    job_core(3, True)
    part_send_wait(4, r["p5"], r["r5"])

    def result_cols(n, c):
        out = dot(r["act"][...].reshape(512, D), r["wdown"][:, columns(n)], NN)
        r["p5"][:, :, columns(n)] = out.astype(BF16).reshape(4, 128, 384)
        return c

    lax.fori_loop(0, 3, result_cols, 0)
    part(7, r["p5"], r["r8"], 1).start()
    part(7, r["p5"], r["r8"], 2).start()

    def attend_back(lo, m):
        for t in range(lo, lo + m):
            q, kk, v = (r["qkv"][t, :, j * WP : (j + 1) * WP] for j in range(3))
            qs, gs = stacked(q), stacked(r["da"][t])
            probs = r["probs"][t]
            dv = dot(probs.astype(BF16), gs, TN)
            dp_ = dot(gs, v, NT)
            ds = (probs * (dp_ - jnp.sum(probs * dp_, axis=-1, keepdims=True)) * SCALE).astype(BF16)
            dq = dot(side_by_side(ds), stacked(kk), NN)
            dk = dot(ds, qs, TN)
            for j, piece in enumerate((dq, dk, dv)):
                piece = piece.astype(BF16)
                r["dqkv"][t, :, j * WP : (j + 1) * WP] = piece
                r["dqc"][t, :, j * W : (j + 1) * W] = piece[:, :W]
        for n in range(3):
            cols = slice(n * 384, n * 384 + 384)
            total = dot(r["dqkv"][lo : lo + m].reshape(m * 128, D), r["win"][:, :, cols].reshape(D, 384), NN)
            r["p7"][lo : lo + m, :, cols] = total.astype(BF16).reshape(m, 128, 384)
        for t in range(max(lo, 1), lo + m):
            part(6, r["p7"], r["r7"], t).start()

    attend_back(0, 1)
    core_step(2)
    core_step(3)
    part_wait(5, r["ds"], r["da"], (1, 2))
    attend_back(1, 2)
    part_wait(5, r["ds"], r["da"], (3,))
    attend_back(3, 1)

    weight_grad(every("f"), lambda: r["dqc"][...].reshape(512, CI), CI, ("i", 0, 512), ("v", 512, 384))
    job_core(4, True)
    job_core(5, True)
    first_step(0)
    first_step(1)
    core_step(4)
    core_step(5)
    first_step(2)
    first_step(3)

    part_wait(6, r["p7"], r["r7"])
    part(7, r["p5"], r["r8"], 3).start()
    for h in range(2):
        rows = slice(64 * h, 64 * h + 64)
        normed, inverse = norm(halves(r["xs"], h))
        back = norm_back(normed, inverse, part_sum(r["p7"], r["r7"], h) * (1.0 + row(1)))
        out = r["mg"][rows, :] + back
        r["lo"][4 * h : 4 * h + 4] = out.astype(BF16).reshape(4, 2, 8, D)
    exchange_out(6, r["lo"], r["ll"])
    for index, out in ((0, gu), (1, gd)):
        job_second(index, False)
        out[...] = job_second_sum(index).astype(BF16)
    job_second(2, False)
    job_second(3, False)
    both = jnp.concatenate([job_second_sum(2), job_second_sum(3)], axis=1)
    for k in range(4):
        r["oy"][k, :36, :W] = both[:, W * k : W * k + W].astype(BF16)
    for k in (3, 1, 2):
        part(8, r["oy"], r["or"], k).start()
    first_step(4)
    first_step(5)

    part_wait(7, r["p5"], r["r8"])
    for h in range(2):
        rows = slice(64 * h, 64 * h + 64)
        out = r["mid"][rows, :] + row(5) * part_sum(r["p5"], r["r8"], h)
        r["ro"][4 * h : 4 * h + 4] = out.astype(BF16).reshape(4, 2, 8, D)
    exchange_out(5, r["ro"], r["rl"])

    part_wait(8, r["oy"], r["or"])
    total = r["oy"][0, :36, :W].astype(F32)
    for k in (1, 2, 3):
        total = total + r["or"][k, :36, :W].astype(F32)
    go[...] = total.astype(BF16)
    exchange_out_wait(6, r["lo"], r["ll"])
    exchange_out_wait(5, r["ro"], r["rl"])
    done = [local(r["rl"], res, r["osem"].at[0]), local(r["ll"], lgr, r["osem"].at[1])]
    for c in done:
        c.start()
    job_second(4, False)
    job_second(5, False)
    both = jnp.concatenate([job_second_sum(4), job_second_sum(5)], axis=1)
    for j in range(3):
        gi[j] = both[:, W * j : W * j + W].astype(BF16)
    for row_, src, dst in (
        (0, lat, r["xs"]),
        (3, cot, r["cg"].at[0]),
        (1, r["cy"].at[1], r["cg"].at[1]),
        (2, r["cy"].at[2], r["cg"].at[2]),
        (4, r["cy"].at[3], r["cg"].at[3]),
    ):
        exchange_in_sent(row_, src, dst)
    gather_sent(1, r["cy"], PARTS_C, cot)
    gather_sent(0, r["f"], PARTS_T)
    gather_sent(3, r["s"], PARTS_T)
    share_sent()
    for ph, src, dst in ((2, "as", "at"), (5, "ds", "da"), (6, "p7", "r7"), (7, "p5", "r8"), (8, "oy", "or")):
        part_send_wait(ph, r[src], r[dst])
    for c in done:
        c.wait()


def body(latents, modulation, in_weight, out_weight, up_weight, down_weight, cotangent):
    vmem = pl.BlockSpec(memory_space=pltpu.VMEM)
    anywhere = pl.BlockSpec(memory_space=pl.ANY)
    out = lambda *s: jax.ShapeDtypeStruct(s, BF16)
    shapes = (out(2, 8, 8, D), out(2, 8, 8, D), out(36, D), out(36, D), out(3, 36, W), out(36, W))
    found = pl.pallas_call(
        kernel,
        out_shape=shapes,
        in_specs=[anywhere, anywhere, vmem, anywhere, anywhere, anywhere, anywhere],
        out_specs=(anywhere, anywhere, vmem, vmem, vmem, vmem),
        scratch_shapes=list(SPEC.values()),
        compiler_params=pltpu.CompilerParams(collective_id=0, has_side_effects=True, vmem_limit_bytes=67043328),
        name="block",
    )(
        latents.reshape(2, 8, 8, D),
        cotangent.reshape(2, 8, 8, D),
        jnp.transpose(modulation, (1, 0, 2)),
        jnp.transpose(in_weight, (1, 2, 0)),
        out_weight.reshape(36, 8, D),
        up_weight,
        down_weight,
    )
    res, lgr, gu, gd, gi, go = pl.pallas_call(
        hand_over,
        out_shape=shapes,
        in_specs=[anywhere] * 6,
        out_specs=(anywhere,) * 6,
        scratch_shapes=[pltpu.VMEM(v.shape, BF16) for v in shapes] + [pltpu.SemaphoreType.DMA((2, 6))],
        name="hand_over",
    )(*found)
    return (
        res.reshape(latents.shape),
        lgr.reshape(latents.shape),
        jnp.transpose(gi, (1, 0, 2)),
        go.T,
        gu,
        gd.T,
    )


def hand_over(*refs):
    given, outs, held, sems = refs[:6], refs[6:12], refs[12:18], refs[18]
    into = [pltpu.make_async_copy(a, b, sems.at[0, i]) for i, (a, b) in enumerate(zip(given, held))]
    back = [pltpu.make_async_copy(a, b, sems.at[1, i]) for i, (a, b) in enumerate(zip(held, outs))]
    for c in into:
        c.start()
    for c, d in zip(into, back):
        c.wait()
        d.start()
    for d in back:
        d.wait()


def solution(mesh):
    placed = (
        P("dp", "seq", "tensor", None),
        P("dp", None, None),
        P(None, None, "tensor"),
        P("tensor", None),
        P(None, "tensor"),
        P("tensor", None),
        P("dp", "seq", "tensor", None),
    )
    return jax.shard_map(
        body,
        mesh=mesh,
        in_specs=placed,
        out_specs=(
            P("dp", "seq", "tensor", None),
            P("dp", "seq", "tensor", None),
            P(("dp", "seq"), None, "tensor"),
            P("tensor", ("dp", "seq")),
            P(("dp", "seq"), "tensor"),
            P("tensor", ("dp", "seq")),
        ),
        check_vma=False,
    )
```

```python
import math

import jax
import jax.numpy as jnp
from jax import lax
from jax.experimental import pallas as pl
from jax.experimental.pallas import tpu as pltpu
from jax.sharding import PartitionSpec as P

HEAD_DIM = 72
HEADS = 4
D = 1152
W = 288
WP = 384
SCALE = 1.0 / math.sqrt(HEAD_DIM)
EPS = 1e-6
MESH = pl.DeviceIdType.MESH
F32 = jnp.float32
BF16 = jnp.bfloat16
GELU_C = math.sqrt(2.0 / math.pi)

NN = (((1,), (0,)), ((), ()))
NT = (((1,), (1,)), ((), ()))
TN = (((0,), (0,)), ((), ()))


def rem(a, b):
    return lax.rem(a, b)


def div(a, b):
    return lax.div(a, b)


def dot(a, b, dims):
    return lax.dot_general(a, b, dims, preferred_element_type=F32)


def norm(rows):
    center = jnp.mean(rows, axis=-1, keepdims=True)
    centred = rows - center
    spread = jnp.mean(centred * centred, axis=-1, keepdims=True)
    inverse = lax.rsqrt(spread + EPS)
    return centred * inverse, inverse


def norm_back(normed, inverse, up):
    mean_grad = jnp.mean(up, axis=-1, keepdims=True)
    mean_cross = jnp.mean(up * normed, axis=-1, keepdims=True)
    return (up - mean_grad - normed * mean_cross) * inverse


JOBS = (("u", 1152, True), ("d", 1152, False), ("o", 640, True), ("p", 512, False), ("i", 512, True), ("v", 384, False))
CI = 896


def scratch_spec():
    vm = lambda *s, t=BF16: pltpu.VMEM(s, t)
    dma = lambda *s: pltpu.SemaphoreType.DMA(s)
    spec = {
        "xs": vm(8, 2, 8, D), "cy": vm(4, 2, 8, 8, D), "cg": vm(4, 8, 2, 8, D),
        "win": vm(3, WP, D), "wo": vm(4, 48, 8, D), "wup": vm(D, D), "wdown": vm(D, D),
        "f": vm(4, 128, D), "s": vm(4, 128, D), "g": vm(4, 128, D), "ao": vm(128, D),
        "p5": vm(4, 128, D), "p7": vm(4, 128, D), "ag": vm(4, 128, D, t=F32),
        "r5": vm(4, 128, D), "r7": vm(4, 128, D), "p8": vm(4, 128, D), "t8": vm(2, 64, D), "r8": vm(2, 128, D),
        "qkv": vm(4, 128, 3 * WP), "probs": vm(4, 512, 128, t=F32),
        "as": vm(4, 128, WP), "at": vm(4, 128, WP), "ds": vm(4, 128, WP), "da": vm(4, 128, WP), "attc": vm(128, D),
        "act": vm(4, 128, D), "hg": vm(4, 128, D), "dqkv": vm(4, 128, 3 * WP), "dqc": vm(4, 128, CI),
        "mid": vm(128, D, t=F32), "mg": vm(128, D, t=F32),
        "ro": vm(8, 2, 8, D), "lo": vm(8, 2, 8, D), "rl": vm(2, 8, 8, D), "ll": vm(2, 8, 8, D),
        "oy": vm(4, 40, WP), "or": vm(4, 40, WP),
        "wsem": dma(7), "mod": vm(6, 1, D, t=F32),
        "ys": dma(10, 6), "yr": dma(10, 6),
        "ss": dma(7, 8), "sr": dma(7, 8),
        "osem": dma(2),
        "js": dma(6, 10), "jr": dma(6, 10),
        "ws": dma(4, 4), "wr": dma(4, 4),
    }
    for name, n, x_first in JOBS:
        spec["G" + name] = vm(2, 2, 4, 9, 8, n)
        spec["A" + name] = vm(2, 4, 9, 8, n)
        if x_first:
            spec["B" + name] = vm(2, 2, 9, 8, n)
            spec["T" + name] = vm(2, 1, 9, 8, n)
            spec["H" + name] = vm(2, 9, 8, n)
        else:
            spec["B" + name] = vm(2, 4, 5, 8, n)
            spec["T" + name] = vm(2, 2, 5, 8, n)
            spec["H" + name] = vm(4, 5, 8, n)
        spec["C" + name] = vm(3, 5, 8, n)
    return spec


SPEC = scratch_spec()

TO = {1: 3, 2: 1, 3: 2}
BACK = {1: 2, 2: 1, 3: 3}
HOPS = ((0, 1, 0, 1), (1, 1, 0, 1), (1, 3, 0, 2), (0, 3, 0, 2), (0, 1, 1, 3), (1, 3, 2, 3))
PARTS_C = (lambda v: v.at[0], lambda v: v.at[1])
PARTS_T = (lambda v: v.at[pl.ds(0, 64)], lambda v: v.at[pl.ds(64, 64)])


def kernel(lat, cot, mod_in, in_w, out_w, up_w, down_w, res, lgr, gu, gd, gi, go, *scratch):
    r = dict(zip(SPEC, scratch))
    dp, seq, me = lax.axis_index("dp"), lax.axis_index("seq"), lax.axis_index("tensor")
    core, z_lo = rem(dp, 2), div(dp, 2)
    x, z_hi = div(seq, 2), rem(seq, 2)
    z = z_hi * 2 + z_lo

    def remote(src, dst, send, recv, where):
        return pltpu.make_async_remote_copy(src_ref=src, dst_ref=dst, send_sem=send, recv_sem=recv, device_id=where, device_id_type=MESH)

    def local(src, dst, sem):
        return pltpu.make_async_copy(src, dst, sem)

    def seq_peer(k):
        return (dp, rem(seq + k, 8), me)

    def y_peer(k):
        return (dp, seq, rem(me + k, 4))

    def core_peer():
        return (dp + 1 - 2 * core, seq, me)

    def x_peer(k):
        return (dp, rem(x + k, 4) * 2 + z_hi, me)

    def z_peer(k):
        other = rem(z + k, 4)
        return (rem(other, 2) * 2 + core, x * 2 + div(other, 2), me)

    weights = [local(in_w.at[j], r["win"].at[j, pl.ds(0, W)], r["wsem"].at[j]) for j in range(3)]
    weights += [
        local(out_w, r["wo"].at[0, pl.ds(0, 36)], r["wsem"].at[3]),
        local(up_w, r["wup"], r["wsem"].at[4]),
        local(down_w, r["wdown"], r["wsem"].at[5]),
    ]

    mod = r["mod"]
    mod_copy = local(mod_in, mod, r["wsem"].at[6])
    mod_copy.start()
    barrier = pltpu.get_barrier_semaphore()
    peers = [seq_peer(k) for k in range(1, 8)] + [y_peer(k) for k in range(1, 4)] + [core_peer()]
    peers += [z_peer(1), z_peer(3)]
    for where in peers:
        pl.semaphore_signal(barrier, inc=1, device_id=where, device_id_type=MESH)
    pl.semaphore_wait(barrier, len(peers))

    def hop(ph, buf, parts, n, src=None):
        half, to, at, there = HOPS[n]
        given = buf.at[at] if src is None or at else src
        return remote(parts[half](given), parts[half](buf.at[there]), r["ys"].at[ph, n], r["yr"].at[ph, n], y_peer(to))

    def gather_start(ph, buf, parts, src=None, hops=(0, 2, 1, 3)):
        for n in hops:
            hop(ph, buf, parts, n, src).start()

    def gather_pass(ph, buf, parts):
        hop(ph, buf, parts, 0).wait_recv()
        hop(ph, buf, parts, 4).start()
        hop(ph, buf, parts, 2).wait_recv()
        hop(ph, buf, parts, 5).start()

    def gather_near(ph, buf, parts):
        hop(ph, buf, parts, 1).wait_recv()
        hop(ph, buf, parts, 3).wait_recv()

    def gather_far(ph, buf, parts):
        hop(ph, buf, parts, 4).wait_recv()
        hop(ph, buf, parts, 5).wait_recv()

    def gather_sent(ph, buf, parts, src=None):
        for n in range(6):
            hop(ph, buf, parts, n, src).wait_send()

    def part(ph, src, dst, k):
        return remote(src.at[k], dst.at[BACK[k]], r["ys"].at[ph, k], r["yr"].at[ph, BACK[k]], y_peer(TO[k]))

    def part_wait(ph, src, dst, slots=(1, 2, 3)):
        for k in slots:
            part(ph, src, dst, BACK[k]).wait_recv()

    def part_send_wait(ph, src, dst):
        for k in (1, 2, 3):
            part(ph, src, dst, k).wait_send()

    def part_sum(src, dst, h):
        rows = slice(64 * h, 64 * h + 64)
        total = src[0, rows, :].astype(F32)
        for k in (1, 2, 3):
            total = total + dst[k, rows, :].astype(F32)
        return total

    def exchange_in(row_, src, dst):
        for k in range(1, 8):
            to = rem(seq + k, 8)
            remote(src.at[:, to], dst.at[seq], r["ss"].at[row_, k], r["sr"].at[row_, k], seq_peer(k)).start()
        local(src.at[:, seq], dst.at[seq], r["sr"].at[row_, 0]).start()

    def exchange_in_sent(row_, src, dst):
        for k in range(1, 8):
            to = rem(seq + k, 8)
            remote(src.at[:, to], dst.at[seq], r["ss"].at[row_, k], r["sr"].at[row_, k], seq_peer(k)).wait_send()

    def exchange_in_wait(row_, src, dst):
        local(src.at[:, seq], dst.at[seq], r["sr"].at[row_, 0]).wait()
        for k in range(1, 8):
            frm = rem(seq + 8 - k, 8)
            remote(src.at[:, frm], dst.at[frm], r["ss"].at[row_, k], r["sr"].at[row_, k], seq_peer(k)).wait_recv()

    def exchange_out(row_, src, dst):
        for k in range(1, 8):
            to = rem(seq + k, 8)
            remote(src.at[to], dst.at[:, seq], r["ss"].at[row_, k], r["sr"].at[row_, k], seq_peer(k)).start()
        local(src.at[seq], dst.at[:, seq], r["sr"].at[row_, 0]).start()

    def exchange_out_wait(row_, src, dst):
        local(src.at[seq], dst.at[:, seq], r["sr"].at[row_, 0]).wait()
        for k in range(1, 8):
            frm = rem(seq + 8 - k, 8)
            remote(src.at[frm], dst.at[:, frm], r["ss"].at[row_, k], r["sr"].at[row_, k], seq_peer(k)).wait()

    SHARE = {1: (core == 1, z, z_peer), 2: (core == 0, x, x_peer), 3: (core == z_lo, x, x_peer)}

    def rows_of(q):
        return pl.ds(9 * q, 9)

    def share_y(slot):
        _, q, _ = SHARE[slot]
        return remote(out_w.at[rows_of(q)], r["wo"].at[slot, rows_of(q)], r["ws"].at[slot, 0], r["wr"].at[slot, 0], y_peer(TO[BACK[slot]]))

    def share_line(slot, k, back):
        _, q, peer = SHARE[slot]
        at = rem(q + 4 - k, 4) if back else q
        piece = r["wo"].at[slot, rows_of(at)]
        return remote(piece, piece, r["ws"].at[slot, k], r["wr"].at[slot, k], peer(k))

    def share_core(slot):
        piece = r["wo"].at[slot, pl.ds(0, 36)]
        return remote(piece, piece, r["ws"].at[0, slot], r["wr"].at[0, slot], core_peer())

    def share_start():
        for slot in (1, 2, 3):
            @pl.when(SHARE[slot][0])
            def _(slot=slot):
                share_y(slot).start()

    def share_second():
        for slot in (1, 2, 3):
            @pl.when(SHARE[slot][0])
            def _(slot=slot):
                share_y(slot).wait_recv()
                for k in (2, 1, 3):
                    share_line(slot, k, False).start()

    def share_third():
        for slot in (1, 2, 3):
            @pl.when(SHARE[slot][0])
            def _(slot=slot):
                for k in (1, 2, 3):
                    share_line(slot, k, True).wait_recv()
                share_core(slot).start()

    def share_wait():
        for slot in (1, 2, 3):
            @pl.when(jnp.logical_not(SHARE[slot][0]))
            def _(slot=slot):
                share_core(slot).wait_recv()

    def share_sent():
        for slot in (1, 2, 3):
            @pl.when(SHARE[slot][0])
            def _(slot=slot):
                share_y(slot).wait_send()
                for k in (1, 2, 3):
                    share_line(slot, k, False).wait_send()
                share_core(slot).wait_send()

    def row(i):
        return mod[i]

    def halves(ref, h):
        return ref[4 * h : 4 * h + 4].astype(F32).reshape(64, D)

    lane = lax.broadcasted_iota(jnp.int32, (128, WP), 1)
    head_masks = [(lane >= HEAD_DIM * h) & (lane < HEAD_DIM * (h + 1)) for h in range(HEADS)]
    same_pixel = rem(lax.broadcasted_iota(jnp.int32, (512, 128), 0), 8) == rem(lax.broadcasted_iota(jnp.int32, (512, 128), 1), 8)

    def stacked(v):
        zero = jnp.zeros_like(v)
        return jnp.concatenate([jnp.where(m, v, zero) for m in head_masks], axis=0)

    def side_by_side(v):
        return jnp.concatenate([v[128 * h : 128 * h + 128] for h in range(HEADS)], axis=1)

    def columns(n):
        return pl.ds(pl.multiple_of(n * 384, 384), 384)

    exchange_in(0, lat, r["xs"])
    share_start()
    gather_start(1, r["cy"], PARTS_C, cot, (0, 2))
    for c in weights:
        c.start()
    for j in range(3):
        r["win"][j, W:] = jnp.zeros((WP - W, D), BF16)
    for k in range(4):
        r["wo"][k, 36:] = jnp.zeros((12, 8, D), BF16)
    r["dqc"][:, :, 768:] = jnp.zeros((4, 128, 128), BF16)

    mod_copy.wait()
    exchange_in_wait(0, lat, r["xs"])
    for h in range(2):
        normed, _ = norm(halves(r["xs"], h))
        r["f"][0, 64 * h : 64 * h + 64, :] = (normed * (1.0 + row(1)) + row(0)).astype(BF16)
    gather_start(0, r["f"], PARTS_T)
    share_second()
    exchange_in(3, cot, r["cg"].at[0])
    for c in weights[:4]:
        c.wait()

    def attend(lo, n):
        block = r["f"][lo : lo + n].reshape(n * 128, D)
        for j in range(3):
            r["qkv"][lo : lo + n, :, j * WP : (j + 1) * WP] = dot(block, r["win"][j], NT).astype(BF16).reshape(n, 128, WP)
        for t in range(lo, lo + n):
            q, kk, v = (r["qkv"][t, :, j * WP : (j + 1) * WP] for j in range(3))
            scores = dot(stacked(q), kk, NT) * SCALE
            scores = jnp.where(same_pixel, scores, -1e30)
            raised = jnp.exp(scores - jnp.max(scores, axis=-1, keepdims=True))
            probs = raised / jnp.sum(raised, axis=-1, keepdims=True)
            r["probs"][t] = probs
            att = dot(side_by_side(probs.astype(BF16)), stacked(v), NN).astype(BF16)
            if t == 0:
                r["at"][0] = att
            else:
                r["as"][t] = att
                part(2, r["as"], r["at"], t).start()

    attend(0, 1)
    gather_pass(0, r["f"], PARTS_T)
    gather_start(1, r["cy"], PARTS_C, cot, (1, 3))
    gather_near(0, r["f"], PARTS_T)
    attend(1, 2)
    share_third()
    gather_far(0, r["f"], PARTS_T)
    attend(3, 1)
    gather_pass(1, r["cy"], PARTS_C)
    gather_near(1, r["cy"], PARTS_C)
    exchange_in(1, r["cy"].at[1], r["cg"].at[1])
    exchange_in(2, r["cy"].at[2], r["cg"].at[2])

    def branch_block(k, row_, src):
        exchange_in_wait(row_, src, r["cg"].at[k])
        for h in range(2):
            r["g"][k, 64 * h : 64 * h + 64, :] = (row(5) * r["cg"][k, 4 * h : 4 * h + 4].astype(F32).reshape(64, D)).astype(BF16)

    def branch_back(lo, m):
        def step(n, c):
            block = r["g"][lo : lo + m].reshape(m * 128, D)
            r["ag"][lo : lo + m, :, columns(n)] = dot(block, r["wdown"][columns(n), :], NT).reshape(m, 128, 384)
            return c

        lax.fori_loop(0, 3, step, 0)

    share_wait()
    part_wait(2, r["as"], r["at"])

    attended = jnp.concatenate([r["at"][k] for k in range(4)], axis=1)
    for n in range(3):
        cols = slice(n * 384, n * 384 + 384)
        r["mid"][:, cols] = dot(attended, r["wo"][:, :, :, cols].reshape(4 * WP, 384), NN)
    for h in range(2):
        rows = slice(64 * h, 64 * h + 64)
        midway = halves(r["xs"], h) + row(2) * r["mid"][rows, :]
        r["mid"][rows, :] = midway
        normed, _ = norm(midway)
        r["s"][0, rows, :] = (normed * (1.0 + row(4)) + row(3)).astype(BF16)
    gather_start(3, r["s"], PARTS_T)
    gather_far(1, r["cy"], PARTS_C)
    exchange_in(4, r["cy"].at[3], r["cg"].at[3])

    def mlp(lo, m):
        def hidden_cols(n, c):
            v = dot(r["s"][lo : lo + m].reshape(m * 128, D), r["wup"][:, columns(n)], NN)
            ag = r["ag"][lo : lo + m, :, columns(n)].reshape(m * 128, 384)
            th = jnp.tanh(GELU_C * (v + 0.044715 * (v * v * v)))
            r["act"][lo : lo + m, :, columns(n)] = (0.5 * v * (1.0 + th)).astype(BF16).reshape(m, 128, 384)
            slope = 0.5 * (1.0 + th) + (0.5 * v) * ((1.0 - th * th) * (GELU_C * (1.0 + (3.0 * 0.044715) * (v * v))))
            r["hg"][lo : lo + m, :, columns(n)] = (ag * slope).astype(BF16).reshape(m, 128, 384)
            return c

        lax.fori_loop(0, 3, hidden_cols, 0)

        def grad_cols(n, c):
            out = dot(r["hg"][lo : lo + m].reshape(m * 128, D), r["wup"][columns(n), :], NT)
            r["p5"][lo : lo + m, :, columns(n)] = out.astype(BF16).reshape(m, 128, 384)
            return c

        lax.fori_loop(0, 3, grad_cols, 0)
        for t in range(max(lo, 1), lo + m):
            part(4, r["p5"], r["r5"], t).start()

    branch_block(0, 3, cot)
    weights[4].wait()
    weights[5].wait()
    branch_block(1, 1, r["cy"].at[1])
    branch_block(2, 2, r["cy"].at[2])
    branch_back(0, 3)
    gather_pass(3, r["s"], PARTS_T)
    mlp(0, 1)
    for k in range(4):
        r["attc"][:, W * k : W * k + W] = r["at"][k, :, :W]
    gather_near(3, r["s"], PARTS_T)
    mlp(1, 2)
    branch_block(3, 4, r["cy"].at[3])
    branch_back(3, 1)
    gather_far(3, r["s"], PARTS_T)
    mlp(3, 1)

    def weight_grad(left_of, right_of, width, *targets):
        def rows_step(m, c):
            out = dot(left_of(columns(m)), right_of(), TN).astype(BF16).reshape(48, 8, width)
            for q in range(16):
                grp = m * 16 + q
                outer = div(grp, 3)
                for name, at, size in targets:
                    to = r["G" + name].at[div(outer, 8), rem(div(outer, 4), 2), rem(outer, 4), pl.ds(rem(grp, 3) * 3, 3)]
                    to[...] = out[3 * q : 3 * q + 3, :, at : at + size]
            return c

        lax.fori_loop(0, 3, rows_step, 0)

    def every(name):
        return lambda cols: r[name][:, :, cols].reshape(512, 384)

    def job_core(index, start):
        name, n, _ = JOBS[index]
        c = remote(r["G" + name].at[:, 1 - core], r["A" + name], r["js"].at[index, 0], r["jr"].at[index, 0], core_peer())
        if start:
            c.start()
        else:
            c.wait()

    def job_core_sum(index):
        name, n, _ = JOBS[index]

        def step(i, c):
            a, b = div(i, 4), rem(i, 4)
            total = r["A" + name][a, b].astype(F32) + r["G" + name][a, core, b].astype(F32)
            r["A" + name][a, b] = total.astype(BF16)
            return c

        lax.fori_loop(0, 8, step, 0)

    def ring(index):
        name, n, x_first = JOBS[index]
        half = 1 if x_first else 2

        def piece(k, h):
            part_of = pl.ds(h * half, half)
            if x_first:
                return r["A" + name].at[part_of, rem(x + k, 4)]
            at = rem(z + k, 4)
            return r["A" + name].at[rem(at, 2), part_of, pl.ds(4 * div(at, 2), 5)]

        def send(src, dst, m, k):
            return remote(src, dst, r["js"].at[index, m], r["jr"].at[index, m], (x_peer if x_first else z_peer)(k))

        through, landed = r["T" + name], r["B" + name]
        first, last = pl.ds(0, half), pl.ds(half, half)

        def copy(m):
            src, dst, k = (
                (piece(2, 0), through.at[0], 1),
                (piece(2, 1), through.at[1], 3),
                (piece(1, 1), landed.at[0, last], 1),
                (piece(3, 0), landed.at[1, first], 3),
                (through.at[0], landed.at[0, first], 1),
                (through.at[1], landed.at[1, last], 3),
            )[m]
            return send(src, dst, m + 1, k)

        return piece, copy

    def job_first(index, start):
        _, copy = ring(index)
        if start:
            for m in range(4):
                copy(m).start()
        else:
            for m in range(2):
                copy(m).wait_send()
            for m in range(2, 6):
                copy(m).wait()

    def relay(index):
        name = JOBS[index][0]
        piece, copy = ring(index)
        for h, k in ((0, 1), (1, 3)):
            copy(h).wait_recv()
            total = r["T" + name][h].astype(F32) + piece(k, h)[...].astype(F32)
            r["T" + name][h] = total.astype(BF16)
            copy(4 + h).start()

    def job_first_sum(index):
        name, n, x_first = JOBS[index]
        for a in range(2 if x_first else 4):
            mine = r["A" + name][a, x] if x_first else r["A" + name][z_lo, a, pl.ds(4 * z_hi, 5)]
            total = mine.astype(F32)
            for k in range(2):
                total = total + r["B" + name][k, a].astype(F32)
            r["H" + name][a] = total.astype(BF16)

    def job_second(index, start):
        name, n, x_first = JOBS[index]
        for k in (2, 1, 3):
            if x_first:
                other = rem(z + k, 4)
                src = r["H" + name].at[rem(other, 2), pl.ds(4 * div(other, 2), 5)]
                where = z_peer(k)
            else:
                src = r["H" + name].at[rem(x + k, 4)]
                where = x_peer(k)
            c = remote(src, r["C" + name].at[k - 1], r["js"].at[index, 6 + k], r["jr"].at[index, 6 + k], where)
            if start:
                c.start()
            else:
                c.wait()

    def job_second_sum(index):
        name, n, x_first = JOBS[index]
        mine = r["H" + name][z_lo, pl.ds(4 * z_hi, 5)] if x_first else r["H" + name][x]
        total = mine.astype(F32)
        for k in range(3):
            total = total + r["C" + name][k].astype(F32)
        total = total.reshape(40, n)
        return jnp.where(z_hi == 0, total[:36], total[4:])

    def core_step(index):
        job_core(index, False)
        job_core_sum(index)
        job_first(index, True)

    def first_step(index):
        job_first(index, False)
        job_first_sum(index)
        job_second(index, True)

    weight_grad(every("s"), lambda: r["hg"][...].reshape(512, D), D, ("u", 0, D))
    job_core(0, True)
    weight_grad(every("g"), lambda: r["act"][...].reshape(512, D), D, ("d", 0, D))
    job_core(1, True)

    def result_cols(n, c):
        out = dot(r["act"][...].reshape(512, D), r["wdown"][:, columns(n)], NN)
        r["p8"][:, :, columns(n)] = out.astype(BF16).reshape(4, 128, 384)
        return c

    lax.fori_loop(0, 3, result_cols, 0)

    low, high = pl.ds(0, 64), pl.ds(64, 64)

    def result_part(m):
        src, dst, to = (
            (r["p8"].at[3, low], r["t8"].at[0], 1),
            (r["p8"].at[3, high], r["t8"].at[1], 3),
            (r["p8"].at[2, high], r["r8"].at[0, high], 1),
            (r["p8"].at[1, low], r["r8"].at[1, low], 3),
            (r["t8"].at[0], r["r8"].at[0, low], 1),
            (r["t8"].at[1], r["r8"].at[1, high], 3),
        )[m]
        return remote(src, dst, r["ys"].at[7, m], r["yr"].at[7, m], y_peer(to))

    core_step(0)
    core_step(1)

    part_wait(4, r["p5"], r["r5"])
    for h in range(2):
        rows = slice(64 * h, 64 * h + 64)
        normed, inverse = norm(r["mid"][rows, :])
        back = norm_back(normed, inverse, part_sum(r["p5"], r["r5"], h) * (1.0 + row(4)))
        mg = halves(r["cg"].at[0], h) + back
        r["mg"][rows, :] = mg
        r["ao"][rows, :] = (row(2) * mg).astype(BF16)
    for k in (3, 1, 2, 0):
        grad = dot(r["ao"][...], r["wo"][k].reshape(WP, D), NT).astype(BF16)
        if k:
            r["ds"][k] = grad
            part(5, r["ds"], r["da"], k).start()
        else:
            r["da"][0] = grad
    for m in range(4):
        result_part(m).start()
    weight_grad(lambda cols: r["ao"][:, cols], lambda: r["attc"][...], D, ("o", 0, 640), ("p", 640, 512))
    job_core(2, True)
    job_core(3, True)
    relay(0)
    relay(1)
    def attend_back(lo, m):
        for t in range(lo, lo + m):
            q, kk, v = (r["qkv"][t, :, j * WP : (j + 1) * WP] for j in range(3))
            qs, gs = stacked(q), stacked(r["da"][t])
            probs = r["probs"][t]
            dv = dot(probs.astype(BF16), gs, TN)
            dp_ = dot(gs, v, NT)
            ds = (probs * (dp_ - jnp.sum(probs * dp_, axis=-1, keepdims=True)) * SCALE).astype(BF16)
            dq = dot(side_by_side(ds), stacked(kk), NN)
            dk = dot(ds, qs, TN)
            for j, piece in enumerate((dq, dk, dv)):
                piece = piece.astype(BF16)
                r["dqkv"][t, :, j * WP : (j + 1) * WP] = piece
                r["dqc"][t, :, j * W : (j + 1) * W] = piece[:, :W]
        for n in range(3):
            cols = slice(n * 384, n * 384 + 384)
            total = dot(r["dqkv"][lo : lo + m].reshape(m * 128, D), r["win"][:, :, cols].reshape(D, 384), NN)
            r["p7"][lo : lo + m, :, cols] = total.astype(BF16).reshape(m, 128, 384)
        for t in range(max(lo, 1), lo + m):
            part(6, r["p7"], r["r7"], t).start()

    attend_back(0, 1)
    core_step(2)
    core_step(3)
    part_wait(5, r["ds"], r["da"], (1, 2))
    attend_back(1, 2)
    part_wait(5, r["ds"], r["da"], (3,))
    attend_back(3, 1)

    weight_grad(every("f"), lambda: r["dqc"][...].reshape(512, CI), CI, ("i", 0, 512), ("v", 512, 384))
    job_core(4, True)
    job_core(5, True)
    relay(2)
    relay(3)
    first_step(0)
    first_step(1)
    for m in range(2):
        result_part(m).wait_recv()
        mine = r["p8"][2, 0:64] if m == 0 else r["p8"][1, 64:128]
        r["t8"][m] = (r["t8"][m].astype(F32) + mine.astype(F32)).astype(BF16)
        result_part(4 + m).start()
    core_step(4)
    core_step(5)
    first_step(2)
    first_step(3)
    relay(4)
    relay(5)

    part_wait(6, r["p7"], r["r7"])
    for h in range(2):
        rows = slice(64 * h, 64 * h + 64)
        normed, inverse = norm(halves(r["xs"], h))
        back = norm_back(normed, inverse, part_sum(r["p7"], r["r7"], h) * (1.0 + row(1)))
        out = r["mg"][rows, :] + back
        r["lo"][4 * h : 4 * h + 4] = out.astype(BF16).reshape(4, 2, 8, D)
    exchange_out(6, r["lo"], r["ll"])
    for index, out in ((0, gu), (1, gd)):
        job_second(index, False)
        out[...] = job_second_sum(index).astype(BF16)
    job_second(2, False)
    job_second(3, False)
    both = jnp.concatenate([job_second_sum(2), job_second_sum(3)], axis=1)
    for k in range(4):
        r["oy"][k, :36, :W] = both[:, W * k : W * k + W].astype(BF16)
    for k in (3, 1, 2):
        part(8, r["oy"], r["or"], k).start()
    first_step(4)
    first_step(5)

    for m in range(2, 6):
        result_part(m).wait_recv()
    for h in range(2):
        rows = slice(64 * h, 64 * h + 64)
        total = r["p8"][0, rows, :].astype(F32) + r["r8"][0, rows, :].astype(F32) + r["r8"][1, rows, :].astype(F32)
        out = r["mid"][rows, :] + row(5) * total
        r["ro"][4 * h : 4 * h + 4] = out.astype(BF16).reshape(4, 2, 8, D)
    exchange_out(5, r["ro"], r["rl"])

    part_wait(8, r["oy"], r["or"])
    total = r["oy"][0, :36, :W].astype(F32)
    for k in (1, 2, 3):
        total = total + r["or"][k, :36, :W].astype(F32)
    go[...] = total.astype(BF16)
    exchange_out_wait(6, r["lo"], r["ll"])
    exchange_out_wait(5, r["ro"], r["rl"])
    done = [local(r["rl"], res, r["osem"].at[0]), local(r["ll"], lgr, r["osem"].at[1])]
    for c in done:
        c.start()
    job_second(4, False)
    job_second(5, False)
    both = jnp.concatenate([job_second_sum(4), job_second_sum(5)], axis=1)
    for j in range(3):
        gi[j] = both[:, W * j : W * j + W].astype(BF16)
    for row_, src, dst in (
        (0, lat, r["xs"]),
        (3, cot, r["cg"].at[0]),
        (1, r["cy"].at[1], r["cg"].at[1]),
        (2, r["cy"].at[2], r["cg"].at[2]),
        (4, r["cy"].at[3], r["cg"].at[3]),
    ):
        exchange_in_sent(row_, src, dst)
    gather_sent(1, r["cy"], PARTS_C, cot)
    gather_sent(0, r["f"], PARTS_T)
    gather_sent(3, r["s"], PARTS_T)
    share_sent()
    for m in range(6):
        result_part(m).wait_send()
    for ph, src, dst in ((2, "as", "at"), (5, "ds", "da"), (6, "p7", "r7"), (4, "p5", "r5"), (8, "oy", "or")):
        part_send_wait(ph, r[src], r[dst])
    for c in done:
        c.wait()


def body(latents, modulation, in_weight, out_weight, up_weight, down_weight, cotangent):
    vmem = pl.BlockSpec(memory_space=pltpu.VMEM)
    anywhere = pl.BlockSpec(memory_space=pl.ANY)
    out = lambda *s: jax.ShapeDtypeStruct(s, BF16)
    shapes = (out(2, 8, 8, D), out(2, 8, 8, D), out(36, D), out(36, D), out(3, 36, W), out(36, W))
    found = pl.pallas_call(
        kernel,
        out_shape=shapes,
        in_specs=[anywhere] * 7,
        out_specs=(anywhere, anywhere, vmem, vmem, vmem, vmem),
        scratch_shapes=list(SPEC.values()),
        compiler_params=pltpu.CompilerParams(collective_id=0, has_side_effects=True, vmem_limit_bytes=67043328),
        name="block",
    )(
        latents.reshape(2, 8, 8, D),
        cotangent.reshape(2, 8, 8, D),
        jnp.transpose(modulation, (1, 0, 2)),
        jnp.transpose(in_weight, (1, 2, 0)),
        out_weight.reshape(36, 8, D),
        up_weight,
        down_weight,
    )
    res, lgr, gu, gd, gi, go = pl.pallas_call(
        hand_over,
        out_shape=shapes,
        in_specs=[anywhere] * 6,
        out_specs=(anywhere,) * 6,
        scratch_shapes=[pltpu.VMEM(v.shape, BF16) for v in shapes] + [pltpu.SemaphoreType.DMA((2, 6))],
        name="hand_over",
    )(*found)
    return (
        res.reshape(latents.shape),
        lgr.reshape(latents.shape),
        jnp.transpose(gi, (1, 0, 2)),
        go.T,
        gu,
        gd.T,
    )


def hand_over(*refs):
    given, outs, held, sems = refs[:6], refs[6:12], refs[12:18], refs[18]
    into = [pltpu.make_async_copy(a, b, sems.at[0, i]) for i, (a, b) in enumerate(zip(given, held))]
    back = [pltpu.make_async_copy(a, b, sems.at[1, i]) for i, (a, b) in enumerate(zip(held, outs))]
    for c in into:
        c.start()
    for c, d in zip(into, back):
        c.wait()
        d.start()
    for d in back:
        d.wait()


def solution(mesh):
    placed = (
        P("dp", "seq", "tensor", None),
        P("dp", None, None),
        P(None, None, "tensor"),
        P("tensor", None),
        P(None, "tensor"),
        P("tensor", None),
        P("dp", "seq", "tensor", None),
    )
    return jax.shard_map(
        body,
        mesh=mesh,
        in_specs=placed,
        out_specs=(
            P("dp", "seq", "tensor", None),
            P("dp", "seq", "tensor", None),
            P(("dp", "seq"), None, "tensor"),
            P("tensor", ("dp", "seq")),
            P(("dp", "seq"), "tensor"),
            P("tensor", ("dp", "seq")),
        ),
        check_vma=False,
    )
```

```python
import math

import jax
import jax.numpy as jnp
from jax import lax
from jax.experimental import pallas as pl
from jax.experimental.pallas import tpu as pltpu
from jax.sharding import PartitionSpec as P

HEAD_DIM = 72
HEADS = 4
D = 1152
W = 288
WP = 384
SCALE = 1.0 / math.sqrt(HEAD_DIM)
EPS = 1e-6
MESH = pl.DeviceIdType.MESH
F32 = jnp.float32
BF16 = jnp.bfloat16
GELU_C = math.sqrt(2.0 / math.pi)

NN = (((1,), (0,)), ((), ()))
NT = (((1,), (1,)), ((), ()))
TN = (((0,), (0,)), ((), ()))


def rem(a, b):
    return lax.rem(a, b)


def div(a, b):
    return lax.div(a, b)


def dot(a, b, dims):
    return lax.dot_general(a, b, dims, preferred_element_type=F32)


def norm(rows):
    center = jnp.mean(rows, axis=-1, keepdims=True)
    centred = rows - center
    spread = jnp.mean(centred * centred, axis=-1, keepdims=True)
    inverse = lax.rsqrt(spread + EPS)
    return centred * inverse, inverse


def norm_back(normed, inverse, up):
    mean_grad = jnp.mean(up, axis=-1, keepdims=True)
    mean_cross = jnp.mean(up * normed, axis=-1, keepdims=True)
    return (up - mean_grad - normed * mean_cross) * inverse


JOBS = (("u", 1152, True), ("d", 1152, False), ("o", 640, True), ("p", 512, False), ("i", 512, True), ("v", 384, False))
CI = 896


def scratch_spec():
    vm = lambda *s, t=BF16: pltpu.VMEM(s, t)
    dma = lambda *s: pltpu.SemaphoreType.DMA(s)
    spec = {
        "xs": vm(8, 2, 8, D), "cy": vm(4, 2, 8, 8, D), "cg": vm(4, 8, 2, 8, D),
        "win": vm(3, WP, D), "wo": vm(4, 48, 8, D), "wup": vm(D, D), "wdown": vm(D, D),
        "f": vm(4, 128, D), "s": vm(4, 128, D), "g": vm(4, 128, D), "ao": vm(128, D),
        "p5": vm(4, 128, D), "p7": vm(4, 128, D), "ag": vm(4, 128, D, t=F32),
        "r5": vm(4, 128, D), "t7": vm(2, 64, D), "r7": vm(2, 128, D), "p8": vm(4, 128, D), "t8": vm(2, 64, D), "r8": vm(2, 128, D),
        "qkv": vm(4, 128, 3 * WP), "probs": vm(4, 512, 128, t=F32),
        "as": vm(4, 128, WP), "at": vm(4, 128, WP), "ds": vm(4, 128, WP), "da": vm(4, 128, WP), "attc": vm(128, D),
        "act": vm(4, 128, D), "hg": vm(4, 128, D), "dqkv": vm(4, 128, 3 * WP), "dqc": vm(4, 128, CI),
        "mid": vm(128, D, t=F32), "mg": vm(128, D, t=F32),
        "ro": vm(8, 2, 8, D), "lo": vm(8, 2, 8, D), "rl": vm(2, 8, 8, D), "ll": vm(2, 8, 8, D),
        "oy": vm(4, 40, WP), "or": vm(4, 40, WP),
        "wsem": dma(7), "mod": vm(6, 1, D, t=F32),
        "ys": dma(10, 6), "yr": dma(10, 6),
        "ss": dma(7, 8), "sr": dma(7, 8),
        "osem": dma(2),
        "js": dma(6, 10), "jr": dma(6, 10),
        "ws": dma(4, 4), "wr": dma(4, 4),
    }
    for name, n, x_first in JOBS:
        spec["G" + name] = vm(2, 2, 4, 9, 8, n)
        spec["A" + name] = vm(2, 4, 9, 8, n)
        if x_first:
            spec["B" + name] = vm(2, 2, 9, 8, n)
            spec["T" + name] = vm(2, 1, 9, 8, n)
            spec["H" + name] = vm(2, 9, 8, n)
        else:
            spec["B" + name] = vm(2, 4, 5, 8, n)
            spec["T" + name] = vm(2, 2, 5, 8, n)
            spec["H" + name] = vm(4, 5, 8, n)
        spec["C" + name] = vm(3, 5, 8, n)
    return spec


SPEC = scratch_spec()

TO = {1: 3, 2: 1, 3: 2}
BACK = {1: 2, 2: 1, 3: 3}
HOPS = ((0, 1, 0, 1), (1, 1, 0, 1), (1, 3, 0, 2), (0, 3, 0, 2), (0, 1, 1, 3), (1, 3, 2, 3))
PARTS_C = (lambda v: v.at[0], lambda v: v.at[1])
PARTS_T = (lambda v: v.at[pl.ds(0, 64)], lambda v: v.at[pl.ds(64, 64)])


def kernel(lat, cot, mod_in, in_w, out_w, up_w, down_w, res, lgr, gu, gd, gi, go, *scratch):
    r = dict(zip(SPEC, scratch))
    dp, seq, me = lax.axis_index("dp"), lax.axis_index("seq"), lax.axis_index("tensor")
    core, z_lo = rem(dp, 2), div(dp, 2)
    x, z_hi = div(seq, 2), rem(seq, 2)
    z = z_hi * 2 + z_lo

    def remote(src, dst, send, recv, where):
        return pltpu.make_async_remote_copy(src_ref=src, dst_ref=dst, send_sem=send, recv_sem=recv, device_id=where, device_id_type=MESH)

    def local(src, dst, sem):
        return pltpu.make_async_copy(src, dst, sem)

    def seq_peer(k):
        return (dp, rem(seq + k, 8), me)

    def y_peer(k):
        return (dp, seq, rem(me + k, 4))

    def core_peer():
        return (dp + 1 - 2 * core, seq, me)

    def x_peer(k):
        return (dp, rem(x + k, 4) * 2 + z_hi, me)

    def z_peer(k):
        other = rem(z + k, 4)
        return (rem(other, 2) * 2 + core, x * 2 + div(other, 2), me)

    weights = [local(in_w.at[j], r["win"].at[j, pl.ds(0, W)], r["wsem"].at[j]) for j in range(3)]
    weights += [
        local(out_w, r["wo"].at[0, pl.ds(0, 36)], r["wsem"].at[3]),
        local(up_w, r["wup"], r["wsem"].at[4]),
        local(down_w, r["wdown"], r["wsem"].at[5]),
    ]

    mod = r["mod"]
    mod_copy = local(mod_in, mod, r["wsem"].at[6])
    mod_copy.start()
    barrier = pltpu.get_barrier_semaphore()
    peers = [seq_peer(k) for k in range(1, 8)] + [y_peer(k) for k in range(1, 4)] + [core_peer()]
    peers += [z_peer(1), z_peer(3)]
    for where in peers:
        pl.semaphore_signal(barrier, inc=1, device_id=where, device_id_type=MESH)
    pl.semaphore_wait(barrier, len(peers))

    def hop(ph, buf, parts, n, src=None):
        half, to, at, there = HOPS[n]
        given = buf.at[at] if src is None or at else src
        return remote(parts[half](given), parts[half](buf.at[there]), r["ys"].at[ph, n], r["yr"].at[ph, n], y_peer(to))

    def gather_start(ph, buf, parts, src=None, hops=(0, 2, 1, 3)):
        for n in hops:
            hop(ph, buf, parts, n, src).start()

    def gather_pass(ph, buf, parts):
        hop(ph, buf, parts, 0).wait_recv()
        hop(ph, buf, parts, 4).start()
        hop(ph, buf, parts, 2).wait_recv()
        hop(ph, buf, parts, 5).start()

    def gather_near(ph, buf, parts):
        hop(ph, buf, parts, 1).wait_recv()
        hop(ph, buf, parts, 3).wait_recv()

    def gather_far(ph, buf, parts):
        hop(ph, buf, parts, 4).wait_recv()
        hop(ph, buf, parts, 5).wait_recv()

    def gather_sent(ph, buf, parts, src=None):
        for n in range(6):
            hop(ph, buf, parts, n, src).wait_send()

    def part(ph, src, dst, k):
        return remote(src.at[k], dst.at[BACK[k]], r["ys"].at[ph, k], r["yr"].at[ph, BACK[k]], y_peer(TO[k]))

    def part_wait(ph, src, dst, slots=(1, 2, 3)):
        for k in slots:
            part(ph, src, dst, BACK[k]).wait_recv()

    def part_send_wait(ph, src, dst):
        for k in (1, 2, 3):
            part(ph, src, dst, k).wait_send()

    def part_sum(src, dst, h):
        rows = slice(64 * h, 64 * h + 64)
        total = src[0, rows, :].astype(F32)
        for k in (1, 2, 3):
            total = total + dst[k, rows, :].astype(F32)
        return total

    def exchange_in(row_, src, dst):
        for k in range(1, 8):
            to = rem(seq + k, 8)
            remote(src.at[:, to], dst.at[seq], r["ss"].at[row_, k], r["sr"].at[row_, k], seq_peer(k)).start()
        local(src.at[:, seq], dst.at[seq], r["sr"].at[row_, 0]).start()

    def exchange_in_sent(row_, src, dst):
        for k in range(1, 8):
            to = rem(seq + k, 8)
            remote(src.at[:, to], dst.at[seq], r["ss"].at[row_, k], r["sr"].at[row_, k], seq_peer(k)).wait_send()

    def exchange_in_wait(row_, src, dst):
        local(src.at[:, seq], dst.at[seq], r["sr"].at[row_, 0]).wait()
        for k in range(1, 8):
            frm = rem(seq + 8 - k, 8)
            remote(src.at[:, frm], dst.at[frm], r["ss"].at[row_, k], r["sr"].at[row_, k], seq_peer(k)).wait_recv()

    def exchange_out(row_, src, dst):
        for k in range(1, 8):
            to = rem(seq + k, 8)
            remote(src.at[to], dst.at[:, seq], r["ss"].at[row_, k], r["sr"].at[row_, k], seq_peer(k)).start()
        local(src.at[seq], dst.at[:, seq], r["sr"].at[row_, 0]).start()

    def exchange_out_wait(row_, src, dst):
        local(src.at[seq], dst.at[:, seq], r["sr"].at[row_, 0]).wait()
        for k in range(1, 8):
            frm = rem(seq + 8 - k, 8)
            remote(src.at[frm], dst.at[:, frm], r["ss"].at[row_, k], r["sr"].at[row_, k], seq_peer(k)).wait()

    SHARE = {1: (core == 1, z, z_peer), 2: (core == 0, x, x_peer), 3: (core == z_lo, x, x_peer)}

    def rows_of(q):
        return pl.ds(9 * q, 9)

    def share_y(slot):
        _, q, _ = SHARE[slot]
        return remote(out_w.at[rows_of(q)], r["wo"].at[slot, rows_of(q)], r["ws"].at[slot, 0], r["wr"].at[slot, 0], y_peer(TO[BACK[slot]]))

    def share_line(slot, k, back):
        _, q, peer = SHARE[slot]
        at = rem(q + 4 - k, 4) if back else q
        piece = r["wo"].at[slot, rows_of(at)]
        return remote(piece, piece, r["ws"].at[slot, k], r["wr"].at[slot, k], peer(k))

    def share_core(slot):
        piece = r["wo"].at[slot, pl.ds(0, 36)]
        return remote(piece, piece, r["ws"].at[0, slot], r["wr"].at[0, slot], core_peer())

    def share_start():
        for slot in (1, 2, 3):
            @pl.when(SHARE[slot][0])
            def _(slot=slot):
                share_y(slot).start()

    def share_second():
        for slot in (1, 2, 3):
            @pl.when(SHARE[slot][0])
            def _(slot=slot):
                share_y(slot).wait_recv()
                for k in (2, 1, 3):
                    share_line(slot, k, False).start()

    def share_third():
        for slot in (1, 2, 3):
            @pl.when(SHARE[slot][0])
            def _(slot=slot):
                for k in (1, 2, 3):
                    share_line(slot, k, True).wait_recv()
                share_core(slot).start()

    def share_wait():
        for slot in (1, 2, 3):
            @pl.when(jnp.logical_not(SHARE[slot][0]))
            def _(slot=slot):
                share_core(slot).wait_recv()

    def share_sent():
        for slot in (1, 2, 3):
            @pl.when(SHARE[slot][0])
            def _(slot=slot):
                share_y(slot).wait_send()
                for k in (1, 2, 3):
                    share_line(slot, k, False).wait_send()
                share_core(slot).wait_send()

    def row(i):
        return mod[i]

    def halves(ref, h):
        return ref[4 * h : 4 * h + 4].astype(F32).reshape(64, D)

    lane = lax.broadcasted_iota(jnp.int32, (128, WP), 1)
    head_masks = [(lane >= HEAD_DIM * h) & (lane < HEAD_DIM * (h + 1)) for h in range(HEADS)]
    same_pixel = rem(lax.broadcasted_iota(jnp.int32, (512, 128), 0), 8) == rem(lax.broadcasted_iota(jnp.int32, (512, 128), 1), 8)

    def stacked(v):
        zero = jnp.zeros_like(v)
        return jnp.concatenate([jnp.where(m, v, zero) for m in head_masks], axis=0)

    def side_by_side(v):
        return jnp.concatenate([v[128 * h : 128 * h + 128] for h in range(HEADS)], axis=1)

    def columns(n):
        return pl.ds(pl.multiple_of(n * 384, 384), 384)

    exchange_in(0, lat, r["xs"])
    share_start()
    gather_start(1, r["cy"], PARTS_C, cot, (0, 2))
    for c in weights[:4]:
        c.start()
    for j in range(3):
        r["win"][j, W:] = jnp.zeros((WP - W, D), BF16)
    for k in range(4):
        r["wo"][k, 36:] = jnp.zeros((12, 8, D), BF16)
    r["dqc"][:, :, 768:] = jnp.zeros((4, 128, 128), BF16)

    mod_copy.wait()
    exchange_in_wait(0, lat, r["xs"])
    for h in range(2):
        normed, _ = norm(halves(r["xs"], h))
        r["f"][0, 64 * h : 64 * h + 64, :] = (normed * (1.0 + row(1)) + row(0)).astype(BF16)
    gather_start(0, r["f"], PARTS_T)
    for c in weights[4:]:
        c.start()
    share_second()
    exchange_in(3, cot, r["cg"].at[0])
    for c in weights[:4]:
        c.wait()

    def attend(lo, n):
        block = r["f"][lo : lo + n].reshape(n * 128, D)
        for j in range(3):
            r["qkv"][lo : lo + n, :, j * WP : (j + 1) * WP] = dot(block, r["win"][j], NT).astype(BF16).reshape(n, 128, WP)
        for t in range(lo, lo + n):
            q, kk, v = (r["qkv"][t, :, j * WP : (j + 1) * WP] for j in range(3))
            scores = dot(stacked(q), kk, NT) * SCALE
            scores = jnp.where(same_pixel, scores, -1e30)
            raised = jnp.exp(scores - jnp.max(scores, axis=-1, keepdims=True))
            probs = raised / jnp.sum(raised, axis=-1, keepdims=True)
            r["probs"][t] = probs
            att = dot(side_by_side(probs.astype(BF16)), stacked(v), NN).astype(BF16)
            if t == 0:
                r["at"][0] = att
            else:
                r["as"][t] = att
                part(2, r["as"], r["at"], t).start()

    attend(0, 1)
    gather_pass(0, r["f"], PARTS_T)
    gather_start(1, r["cy"], PARTS_C, cot, (1, 3))
    gather_near(0, r["f"], PARTS_T)
    attend(1, 2)
    share_third()
    gather_far(0, r["f"], PARTS_T)
    attend(3, 1)
    gather_pass(1, r["cy"], PARTS_C)
    gather_near(1, r["cy"], PARTS_C)
    exchange_in(1, r["cy"].at[1], r["cg"].at[1])
    exchange_in(2, r["cy"].at[2], r["cg"].at[2])

    def branch_block(k, row_, src):
        exchange_in_wait(row_, src, r["cg"].at[k])
        for h in range(2):
            r["g"][k, 64 * h : 64 * h + 64, :] = (row(5) * r["cg"][k, 4 * h : 4 * h + 4].astype(F32).reshape(64, D)).astype(BF16)

    def branch_back(lo, m):
        def step(n, c):
            block = r["g"][lo : lo + m].reshape(m * 128, D)
            r["ag"][lo : lo + m, :, columns(n)] = dot(block, r["wdown"][columns(n), :], NT).reshape(m, 128, 384)
            return c

        lax.fori_loop(0, 3, step, 0)

    branch_block(0, 3, cot)
    weights[4].wait()
    weights[5].wait()
    branch_back(0, 1)
    share_wait()
    part_wait(2, r["as"], r["at"])

    attended = jnp.concatenate([r["at"][k] for k in range(4)], axis=1)
    for n in range(3):
        cols = slice(n * 384, n * 384 + 384)
        r["mid"][:, cols] = dot(attended, r["wo"][:, :, :, cols].reshape(4 * WP, 384), NN)
    for h in range(2):
        rows = slice(64 * h, 64 * h + 64)
        midway = halves(r["xs"], h) + row(2) * r["mid"][rows, :]
        r["mid"][rows, :] = midway
        normed, _ = norm(midway)
        r["s"][0, rows, :] = (normed * (1.0 + row(4)) + row(3)).astype(BF16)
    gather_start(3, r["s"], PARTS_T)
    gather_far(1, r["cy"], PARTS_C)
    exchange_in(4, r["cy"].at[3], r["cg"].at[3])

    def mlp(lo, m):
        def hidden_cols(n, c):
            v = dot(r["s"][lo : lo + m].reshape(m * 128, D), r["wup"][:, columns(n)], NN)
            ag = r["ag"][lo : lo + m, :, columns(n)].reshape(m * 128, 384)
            th = jnp.tanh(GELU_C * (v + 0.044715 * (v * v * v)))
            r["act"][lo : lo + m, :, columns(n)] = (0.5 * v * (1.0 + th)).astype(BF16).reshape(m, 128, 384)
            slope = 0.5 * (1.0 + th) + (0.5 * v) * ((1.0 - th * th) * (GELU_C * (1.0 + (3.0 * 0.044715) * (v * v))))
            r["hg"][lo : lo + m, :, columns(n)] = (ag * slope).astype(BF16).reshape(m, 128, 384)
            return c

        lax.fori_loop(0, 3, hidden_cols, 0)

        def grad_cols(n, c):
            out = dot(r["hg"][lo : lo + m].reshape(m * 128, D), r["wup"][columns(n), :], NT)
            r["p5"][lo : lo + m, :, columns(n)] = out.astype(BF16).reshape(m, 128, 384)
            return c

        lax.fori_loop(0, 3, grad_cols, 0)
        for t in range(max(lo, 1), lo + m):
            part(4, r["p5"], r["r5"], t).start()

    mlp(0, 1)
    for k in range(4):
        r["attc"][:, W * k : W * k + W] = r["at"][k, :, :W]
    gather_pass(3, r["s"], PARTS_T)
    branch_block(1, 1, r["cy"].at[1])
    branch_block(2, 2, r["cy"].at[2])
    branch_back(1, 2)
    gather_near(3, r["s"], PARTS_T)
    mlp(1, 2)
    branch_block(3, 4, r["cy"].at[3])
    branch_back(3, 1)
    gather_far(3, r["s"], PARTS_T)
    mlp(3, 1)

    def weight_grad(left_of, right_of, width, *targets):
        def rows_step(m, c):
            out = dot(left_of(columns(m)), right_of(), TN).astype(BF16).reshape(48, 8, width)
            for q in range(16):
                grp = m * 16 + q
                outer = div(grp, 3)
                for name, at, size in targets:
                    to = r["G" + name].at[div(outer, 8), rem(div(outer, 4), 2), rem(outer, 4), pl.ds(rem(grp, 3) * 3, 3)]
                    to[...] = out[3 * q : 3 * q + 3, :, at : at + size]
            return c

        lax.fori_loop(0, 3, rows_step, 0)

    def every(name):
        return lambda cols: r[name][:, :, cols].reshape(512, 384)

    def job_core(index, start):
        name, n, _ = JOBS[index]
        c = remote(r["G" + name].at[:, 1 - core], r["A" + name], r["js"].at[index, 0], r["jr"].at[index, 0], core_peer())
        if start:
            c.start()
        else:
            c.wait()

    def job_core_sum(index):
        name, n, _ = JOBS[index]

        def step(i, c):
            a, b = div(i, 4), rem(i, 4)
            total = r["A" + name][a, b].astype(F32) + r["G" + name][a, core, b].astype(F32)
            r["A" + name][a, b] = total.astype(BF16)
            return c

        lax.fori_loop(0, 8, step, 0)

    def ring(index):
        name, n, x_first = JOBS[index]
        half = 1 if x_first else 2

        def piece(k, h):
            part_of = pl.ds(h * half, half)
            if x_first:
                return r["A" + name].at[part_of, rem(x + k, 4)]
            at = rem(z + k, 4)
            return r["A" + name].at[rem(at, 2), part_of, pl.ds(4 * div(at, 2), 5)]

        def send(src, dst, m, k):
            return remote(src, dst, r["js"].at[index, m], r["jr"].at[index, m], (x_peer if x_first else z_peer)(k))

        through, landed = r["T" + name], r["B" + name]
        first, last = pl.ds(0, half), pl.ds(half, half)

        def copy(m):
            src, dst, k = (
                (piece(2, 0), through.at[0], 1),
                (piece(2, 1), through.at[1], 3),
                (piece(1, 1), landed.at[0, last], 1),
                (piece(3, 0), landed.at[1, first], 3),
                (through.at[0], landed.at[0, first], 1),
                (through.at[1], landed.at[1, last], 3),
            )[m]
            return send(src, dst, m + 1, k)

        return piece, copy

    def job_first(index, start):
        _, copy = ring(index)
        if start:
            for m in range(4):
                copy(m).start()
        else:
            for m in range(2):
                copy(m).wait_send()
            for m in range(2, 6):
                copy(m).wait()

    def relay(index):
        name = JOBS[index][0]
        piece, copy = ring(index)
        for h, k in ((0, 1), (1, 3)):
            copy(h).wait_recv()
            total = r["T" + name][h].astype(F32) + piece(k, h)[...].astype(F32)
            r["T" + name][h] = total.astype(BF16)
            copy(4 + h).start()

    def job_first_sum(index):
        name, n, x_first = JOBS[index]
        for a in range(2 if x_first else 4):
            mine = r["A" + name][a, x] if x_first else r["A" + name][z_lo, a, pl.ds(4 * z_hi, 5)]
            total = mine.astype(F32)
            for k in range(2):
                total = total + r["B" + name][k, a].astype(F32)
            r["H" + name][a] = total.astype(BF16)

    def job_second(index, start):
        name, n, x_first = JOBS[index]
        for k in (2, 1, 3):
            if x_first:
                other = rem(z + k, 4)
                src = r["H" + name].at[rem(other, 2), pl.ds(4 * div(other, 2), 5)]
                where = z_peer(k)
            else:
                src = r["H" + name].at[rem(x + k, 4)]
                where = x_peer(k)
            c = remote(src, r["C" + name].at[k - 1], r["js"].at[index, 6 + k], r["jr"].at[index, 6 + k], where)
            if start:
                c.start()
            else:
                c.wait()

    def job_second_sum(index):
        name, n, x_first = JOBS[index]
        mine = r["H" + name][z_lo, pl.ds(4 * z_hi, 5)] if x_first else r["H" + name][x]
        total = mine.astype(F32)
        for k in range(3):
            total = total + r["C" + name][k].astype(F32)
        total = total.reshape(40, n)
        return jnp.where(z_hi == 0, total[:36], total[4:])

    def core_step(index):
        job_core(index, False)
        job_core_sum(index)
        job_first(index, True)

    def first_step(index):
        job_first(index, False)
        job_first_sum(index)
        job_second(index, True)

    weight_grad(every("s"), lambda: r["hg"][...].reshape(512, D), D, ("u", 0, D))
    job_core(0, True)
    weight_grad(every("g"), lambda: r["act"][...].reshape(512, D), D, ("d", 0, D))
    job_core(1, True)

    def result_cols(n, c):
        out = dot(r["act"][...].reshape(512, D), r["wdown"][:, columns(n)], NN)
        r["p8"][:, :, columns(n)] = out.astype(BF16).reshape(4, 128, 384)
        return c

    lax.fori_loop(0, 3, result_cols, 0)

    low, high = pl.ds(0, 64), pl.ds(64, 64)

    def halved(ph, p, t, q, m):
        src, dst, to = (
            (r[p].at[3, low], r[t].at[0], 1),
            (r[p].at[3, high], r[t].at[1], 3),
            (r[p].at[2, high], r[q].at[0, high], 1),
            (r[p].at[1, low], r[q].at[1, low], 3),
            (r[t].at[0], r[q].at[0, low], 1),
            (r[t].at[1], r[q].at[1, high], 3),
        )[m]
        return remote(src, dst, r["ys"].at[ph, m], r["yr"].at[ph, m], y_peer(to))

    def halved_relay(ph, p, t, q):
        for m in range(2):
            halved(ph, p, t, q, m).wait_recv()
            mine = r[p][2, 0:64] if m == 0 else r[p][1, 64:128]
            r[t][m] = (r[t][m].astype(F32) + mine.astype(F32)).astype(BF16)
            halved(ph, p, t, q, 4 + m).start()

    def halved_wait(ph, p, t, q):
        for m in range(2, 6):
            halved(ph, p, t, q, m).wait_recv()

    def halved_sum(p, q, h):
        rows = slice(64 * h, 64 * h + 64)
        return r[p][0, rows, :].astype(F32) + r[q][0, rows, :].astype(F32) + r[q][1, rows, :].astype(F32)

    RESULT = (7, "p8", "t8", "r8")
    INPUT = (6, "p7", "t7", "r7")

    core_step(0)
    core_step(1)

    part_wait(4, r["p5"], r["r5"])
    for h in range(2):
        rows = slice(64 * h, 64 * h + 64)
        normed, inverse = norm(r["mid"][rows, :])
        back = norm_back(normed, inverse, part_sum(r["p5"], r["r5"], h) * (1.0 + row(4)))
        mg = halves(r["cg"].at[0], h) + back
        r["mg"][rows, :] = mg
        r["ao"][rows, :] = (row(2) * mg).astype(BF16)
    for k in (3, 1, 2, 0):
        grad = dot(r["ao"][...], r["wo"][k].reshape(WP, D), NT).astype(BF16)
        if k:
            r["ds"][k] = grad
            part(5, r["ds"], r["da"], k).start()
        else:
            r["da"][0] = grad
    for m in range(4):
        halved(*RESULT, m).start()
    weight_grad(lambda cols: r["ao"][:, cols], lambda: r["attc"][...], D, ("o", 0, 640), ("p", 640, 512))
    job_core(2, True)
    job_core(3, True)
    relay(0)
    relay(1)
    def attend_back(lo, m):
        for t in range(lo, lo + m):
            q, kk, v = (r["qkv"][t, :, j * WP : (j + 1) * WP] for j in range(3))
            qs, gs = stacked(q), stacked(r["da"][t])
            probs = r["probs"][t]
            dv = dot(probs.astype(BF16), gs, TN)
            dp_ = dot(gs, v, NT)
            ds = (probs * (dp_ - jnp.sum(probs * dp_, axis=-1, keepdims=True)) * SCALE).astype(BF16)
            dq = dot(side_by_side(ds), stacked(kk), NN)
            dk = dot(ds, qs, TN)
            for j, piece in enumerate((dq, dk, dv)):
                piece = piece.astype(BF16)
                r["dqkv"][t, :, j * WP : (j + 1) * WP] = piece
                r["dqc"][t, :, j * W : (j + 1) * W] = piece[:, :W]
        for n in range(3):
            cols = slice(n * 384, n * 384 + 384)
            total = dot(r["dqkv"][lo : lo + m].reshape(m * 128, D), r["win"][:, :, cols].reshape(D, 384), NN)
            r["p7"][lo : lo + m, :, cols] = total.astype(BF16).reshape(m, 128, 384)

    attend_back(0, 1)
    core_step(2)
    core_step(3)
    part_wait(5, r["ds"], r["da"], (3,))
    attend_back(3, 1)
    halved(*INPUT, 0).start()
    halved(*INPUT, 1).start()
    part_wait(5, r["ds"], r["da"], (1, 2))
    attend_back(1, 2)
    halved(*INPUT, 2).start()
    halved(*INPUT, 3).start()

    weight_grad(every("f"), lambda: r["dqc"][...].reshape(512, CI), CI, ("i", 0, 512), ("v", 512, 384))
    job_core(4, True)
    job_core(5, True)
    halved_relay(*INPUT)
    halved_relay(*RESULT)
    relay(2)
    relay(3)
    first_step(0)
    first_step(1)
    core_step(4)
    core_step(5)
    halved_wait(*INPUT)
    for h in range(2):
        rows = slice(64 * h, 64 * h + 64)
        normed, inverse = norm(halves(r["xs"], h))
        back = norm_back(normed, inverse, halved_sum("p7", "r7", h) * (1.0 + row(1)))
        out = r["mg"][rows, :] + back
        r["lo"][4 * h : 4 * h + 4] = out.astype(BF16).reshape(4, 2, 8, D)
    exchange_out(6, r["lo"], r["ll"])
    first_step(2)
    first_step(3)
    relay(4)
    relay(5)

    halved_wait(*RESULT)
    for h in range(2):
        rows = slice(64 * h, 64 * h + 64)
        out = r["mid"][rows, :] + row(5) * halved_sum("p8", "r8", h)
        r["ro"][4 * h : 4 * h + 4] = out.astype(BF16).reshape(4, 2, 8, D)
    exchange_out(5, r["ro"], r["rl"])


    for index, out in ((0, gu), (1, gd)):
        job_second(index, False)
        out[...] = job_second_sum(index).astype(BF16)
    job_second(2, False)
    job_second(3, False)
    both = jnp.concatenate([job_second_sum(2), job_second_sum(3)], axis=1)
    for k in range(4):
        r["oy"][k, :36, :W] = both[:, W * k : W * k + W].astype(BF16)
    for k in (3, 1, 2):
        part(8, r["oy"], r["or"], k).start()
    first_step(4)
    first_step(5)

    part_wait(8, r["oy"], r["or"])
    total = r["oy"][0, :36, :W].astype(F32)
    for k in (1, 2, 3):
        total = total + r["or"][k, :36, :W].astype(F32)
    go[...] = total.astype(BF16)
    exchange_out_wait(6, r["lo"], r["ll"])
    exchange_out_wait(5, r["ro"], r["rl"])
    done = [local(r["rl"], res, r["osem"].at[0]), local(r["ll"], lgr, r["osem"].at[1])]
    for c in done:
        c.start()
    job_second(4, False)
    job_second(5, False)
    both = jnp.concatenate([job_second_sum(4), job_second_sum(5)], axis=1)
    for j in range(3):
        gi[j] = both[:, W * j : W * j + W].astype(BF16)
    for row_, src, dst in (
        (0, lat, r["xs"]),
        (3, cot, r["cg"].at[0]),
        (1, r["cy"].at[1], r["cg"].at[1]),
        (2, r["cy"].at[2], r["cg"].at[2]),
        (4, r["cy"].at[3], r["cg"].at[3]),
    ):
        exchange_in_sent(row_, src, dst)
    gather_sent(1, r["cy"], PARTS_C, cot)
    gather_sent(0, r["f"], PARTS_T)
    gather_sent(3, r["s"], PARTS_T)
    share_sent()
    for m in range(6):
        halved(*RESULT, m).wait_send()
        halved(*INPUT, m).wait_send()
    for ph, src, dst in ((2, "as", "at"), (5, "ds", "da"), (4, "p5", "r5"), (8, "oy", "or")):
        part_send_wait(ph, r[src], r[dst])
    for c in done:
        c.wait()


def body(latents, modulation, in_weight, out_weight, up_weight, down_weight, cotangent):
    vmem = pl.BlockSpec(memory_space=pltpu.VMEM)
    anywhere = pl.BlockSpec(memory_space=pl.ANY)
    out = lambda *s: jax.ShapeDtypeStruct(s, BF16)
    shapes = (out(2, 8, 8, D), out(2, 8, 8, D), out(36, D), out(36, D), out(3, 36, W), out(36, W))
    found = pl.pallas_call(
        kernel,
        out_shape=shapes,
        in_specs=[anywhere] * 7,
        out_specs=(anywhere, anywhere, vmem, vmem, vmem, vmem),
        scratch_shapes=list(SPEC.values()),
        compiler_params=pltpu.CompilerParams(collective_id=0, has_side_effects=True, vmem_limit_bytes=67043328),
        name="block",
    )(
        latents.reshape(2, 8, 8, D),
        cotangent.reshape(2, 8, 8, D),
        jnp.transpose(modulation, (1, 0, 2)),
        jnp.transpose(in_weight, (1, 2, 0)),
        out_weight.reshape(36, 8, D),
        up_weight,
        down_weight,
    )
    res, lgr, gu, gd, gi, go = pl.pallas_call(
        hand_over,
        out_shape=shapes,
        in_specs=[anywhere] * 6,
        out_specs=(anywhere,) * 6,
        scratch_shapes=[pltpu.VMEM(v.shape, BF16) for v in shapes] + [pltpu.SemaphoreType.DMA((2, 6))],
        name="hand_over",
    )(*found)
    return (
        res.reshape(latents.shape),
        lgr.reshape(latents.shape),
        jnp.transpose(gi, (1, 0, 2)),
        go.T,
        gu,
        gd.T,
    )


def hand_over(*refs):
    given, outs, held, sems = refs[:6], refs[6:12], refs[12:18], refs[18]
    into = [pltpu.make_async_copy(a, b, sems.at[0, i]) for i, (a, b) in enumerate(zip(given, held))]
    back = [pltpu.make_async_copy(a, b, sems.at[1, i]) for i, (a, b) in enumerate(zip(held, outs))]
    for c in into:
        c.start()
    for c, d in zip(into, back):
        c.wait()
        d.start()
    for d in back:
        d.wait()


def solution(mesh):
    placed = (
        P("dp", "seq", "tensor", None),
        P("dp", None, None),
        P(None, None, "tensor"),
        P("tensor", None),
        P(None, "tensor"),
        P("tensor", None),
        P("dp", "seq", "tensor", None),
    )
    return jax.shard_map(
        body,
        mesh=mesh,
        in_specs=placed,
        out_specs=(
            P("dp", "seq", "tensor", None),
            P("dp", "seq", "tensor", None),
            P(("dp", "seq"), None, "tensor"),
            P("tensor", ("dp", "seq")),
            P(("dp", "seq"), "tensor"),
            P("tensor", ("dp", "seq")),
        ),
        check_vma=False,
    )
```

```python
import math

import jax
import jax.numpy as jnp
from jax import lax
from jax.experimental import pallas as pl
from jax.experimental.pallas import tpu as pltpu
from jax.sharding import PartitionSpec as P

HEAD_DIM = 72
HEADS = 4
D = 1152
W = 288
WP = 384
SCALE = 1.0 / math.sqrt(HEAD_DIM)
EPS = 1e-6
MESH = pl.DeviceIdType.MESH
F32 = jnp.float32
BF16 = jnp.bfloat16
GELU_C = math.sqrt(2.0 / math.pi)

NN = (((1,), (0,)), ((), ()))
NT = (((1,), (1,)), ((), ()))
TN = (((0,), (0,)), ((), ()))


def rem(a, b):
    return lax.rem(a, b)


def div(a, b):
    return lax.div(a, b)


def dot(a, b, dims):
    return lax.dot_general(a, b, dims, preferred_element_type=F32)


def norm(rows):
    center = jnp.mean(rows, axis=-1, keepdims=True)
    centred = rows - center
    spread = jnp.mean(centred * centred, axis=-1, keepdims=True)
    inverse = lax.rsqrt(spread + EPS)
    return centred * inverse, inverse


def norm_back(normed, inverse, up):
    mean_grad = jnp.mean(up, axis=-1, keepdims=True)
    mean_cross = jnp.mean(up * normed, axis=-1, keepdims=True)
    return (up - mean_grad - normed * mean_cross) * inverse


JOBS = (("u", 1152, True), ("d", 1152, False), ("o", 640, True), ("p", 512, False), ("i", 512, True), ("v", 384, False))
CI = 896


def scratch_spec():
    vm = lambda *s, t=BF16: pltpu.VMEM(s, t)
    dma = lambda *s: pltpu.SemaphoreType.DMA(s)
    spec = {
        "xs": vm(8, 2, 8, D), "cy": vm(4, 2, 8, 8, D), "cg": vm(4, 8, 2, 8, D),
        "win": vm(3, WP, D), "wo": vm(4, 48, 8, D), "wup": vm(D, D), "wdown": vm(D, D),
        "f": vm(4, 128, D), "s": vm(4, 128, D), "g": vm(4, 128, D), "ao": vm(128, D),
        "p5": vm(4, 128, D), "p7": vm(4, 128, D), "ag": vm(4, 128, D, t=F32),
        "r5": vm(4, 128, D), "t7": vm(2, 64, D), "r7": vm(2, 128, D), "p8": vm(4, 128, D), "t8": vm(2, 64, D), "r8": vm(2, 128, D),
        "qkv": vm(4, 128, 3 * WP), "probs": vm(4, 512, 128, t=F32),
        "as": vm(4, 128, WP), "at": vm(4, 128, WP), "ds": vm(4, 128, WP), "da": vm(4, 128, WP), "attc": vm(128, D),
        "act": vm(4, 128, D), "hg": vm(4, 128, D), "dqkv": vm(4, 128, 3 * WP), "dqc": vm(4, 128, CI),
        "mid": vm(128, D, t=F32), "mg": vm(128, D, t=F32),
        "ro": vm(8, 2, 8, D), "lo": vm(8, 2, 8, D), "rl": vm(2, 8, 8, D), "ll": vm(2, 8, 8, D),
        "oy": vm(4, 40, WP), "or": vm(4, 40, WP),
        "wsem": dma(7), "mod": vm(6, 1, D, t=F32),
        "ys": dma(10, 6), "yr": dma(10, 6),
        "ss": dma(7, 8), "sr": dma(7, 8),
        "osem": dma(2),
        "js": dma(6, 10), "jr": dma(6, 10),
        "ws": dma(4, 4), "wr": dma(4, 4),
    }
    for name, n, x_first in JOBS:
        spec["G" + name] = vm(2, 2, 4, 9, 8, n)
        spec["A" + name] = vm(2, 4, 9, 8, n)
        if x_first:
            spec["B" + name] = vm(2, 2, 9, 8, n)
            spec["T" + name] = vm(2, 1, 9, 8, n)
            spec["H" + name] = vm(2, 9, 8, n)
        else:
            spec["B" + name] = vm(2, 4, 5, 8, n)
            spec["T" + name] = vm(2, 2, 5, 8, n)
            spec["H" + name] = vm(4, 5, 8, n)
        spec["C" + name] = vm(3, 5, 8, n)
    return spec


SPEC = scratch_spec()

TO = {1: 3, 2: 1, 3: 2}
BACK = {1: 2, 2: 1, 3: 3}
HOPS = ((0, 1, 0, 1), (1, 1, 0, 1), (1, 3, 0, 2), (0, 3, 0, 2), (0, 1, 1, 3), (1, 3, 2, 3))
PARTS_C = (lambda v: v.at[0], lambda v: v.at[1])
PARTS_T = (lambda v: v.at[pl.ds(0, 64)], lambda v: v.at[pl.ds(64, 64)])


def kernel(lat, cot, mod_in, in_w, out_w, up_w, down_w, res, lgr, gu, gd, gi, go, *scratch):
    r = dict(zip(SPEC, scratch))
    dp, seq, me = lax.axis_index("dp"), lax.axis_index("seq"), lax.axis_index("tensor")
    core, z_lo = rem(dp, 2), div(dp, 2)
    x, z_hi = div(seq, 2), rem(seq, 2)
    z = z_hi * 2 + z_lo

    def remote(src, dst, send, recv, where):
        return pltpu.make_async_remote_copy(src_ref=src, dst_ref=dst, send_sem=send, recv_sem=recv, device_id=where, device_id_type=MESH)

    def local(src, dst, sem):
        return pltpu.make_async_copy(src, dst, sem)

    def seq_peer(k):
        return (dp, rem(seq + k, 8), me)

    def y_peer(k):
        return (dp, seq, rem(me + k, 4))

    def core_peer():
        return (dp + 1 - 2 * core, seq, me)

    def x_peer(k):
        return (dp, rem(x + k, 4) * 2 + z_hi, me)

    def z_peer(k):
        other = rem(z + k, 4)
        return (rem(other, 2) * 2 + core, x * 2 + div(other, 2), me)

    weights = [local(in_w.at[j], r["win"].at[j, pl.ds(0, W)], r["wsem"].at[j]) for j in range(3)]
    weights += [
        local(out_w, r["wo"].at[0, pl.ds(0, 36)], r["wsem"].at[3]),
        local(up_w, r["wup"], r["wsem"].at[4]),
        local(down_w, r["wdown"], r["wsem"].at[5]),
    ]

    mod = r["mod"]
    mod_copy = local(mod_in, mod, r["wsem"].at[6])
    mod_copy.start()
    barrier = pltpu.get_barrier_semaphore()
    peers = [seq_peer(k) for k in range(1, 8)] + [y_peer(k) for k in range(1, 4)] + [core_peer()]
    peers += [z_peer(1), z_peer(3)]
    for where in peers:
        pl.semaphore_signal(barrier, inc=1, device_id=where, device_id_type=MESH)
    pl.semaphore_wait(barrier, len(peers))

    def hop(ph, buf, parts, n, src=None):
        half, to, at, there = HOPS[n]
        given = buf.at[at] if src is None or at else src
        return remote(parts[half](given), parts[half](buf.at[there]), r["ys"].at[ph, n], r["yr"].at[ph, n], y_peer(to))

    def gather_start(ph, buf, parts, src=None, hops=(0, 2, 1, 3)):
        for n in hops:
            hop(ph, buf, parts, n, src).start()

    def gather_pass(ph, buf, parts):
        hop(ph, buf, parts, 0).wait_recv()
        hop(ph, buf, parts, 4).start()
        hop(ph, buf, parts, 2).wait_recv()
        hop(ph, buf, parts, 5).start()

    def gather_near(ph, buf, parts):
        hop(ph, buf, parts, 1).wait_recv()
        hop(ph, buf, parts, 3).wait_recv()

    def gather_far(ph, buf, parts):
        hop(ph, buf, parts, 4).wait_recv()
        hop(ph, buf, parts, 5).wait_recv()

    def gather_sent(ph, buf, parts, src=None):
        for n in range(6):
            hop(ph, buf, parts, n, src).wait_send()

    def part(ph, src, dst, k):
        return remote(src.at[k], dst.at[BACK[k]], r["ys"].at[ph, k], r["yr"].at[ph, BACK[k]], y_peer(TO[k]))

    def part_wait(ph, src, dst, slots=(1, 2, 3)):
        for k in slots:
            part(ph, src, dst, BACK[k]).wait_recv()

    def part_send_wait(ph, src, dst):
        for k in (1, 2, 3):
            part(ph, src, dst, k).wait_send()

    def part_sum(src, dst, h):
        rows = slice(64 * h, 64 * h + 64)
        total = src[0, rows, :].astype(F32)
        for k in (1, 2, 3):
            total = total + dst[k, rows, :].astype(F32)
        return total

    def exchange_in(row_, src, dst):
        for k in range(1, 8):
            to = rem(seq + k, 8)
            remote(src.at[:, to], dst.at[seq], r["ss"].at[row_, k], r["sr"].at[row_, k], seq_peer(k)).start()
        local(src.at[:, seq], dst.at[seq], r["sr"].at[row_, 0]).start()

    def exchange_in_sent(row_, src, dst):
        for k in range(1, 8):
            to = rem(seq + k, 8)
            remote(src.at[:, to], dst.at[seq], r["ss"].at[row_, k], r["sr"].at[row_, k], seq_peer(k)).wait_send()

    def exchange_in_wait(row_, src, dst):
        local(src.at[:, seq], dst.at[seq], r["sr"].at[row_, 0]).wait()
        for k in range(1, 8):
            frm = rem(seq + 8 - k, 8)
            remote(src.at[:, frm], dst.at[frm], r["ss"].at[row_, k], r["sr"].at[row_, k], seq_peer(k)).wait_recv()

    def exchange_out(row_, src, dst):
        for k in range(1, 8):
            to = rem(seq + k, 8)
            remote(src.at[to], dst.at[:, seq], r["ss"].at[row_, k], r["sr"].at[row_, k], seq_peer(k)).start()
        local(src.at[seq], dst.at[:, seq], r["sr"].at[row_, 0]).start()

    def exchange_out_wait(row_, src, dst):
        local(src.at[seq], dst.at[:, seq], r["sr"].at[row_, 0]).wait()
        for k in range(1, 8):
            frm = rem(seq + 8 - k, 8)
            remote(src.at[frm], dst.at[:, frm], r["ss"].at[row_, k], r["sr"].at[row_, k], seq_peer(k)).wait()

    SHARE = {1: (core == 1, z, z_peer), 2: (core == 0, x, x_peer), 3: (core == z_lo, x, x_peer)}

    def rows_of(q):
        return pl.ds(9 * q, 9)

    def share_y(slot):
        _, q, _ = SHARE[slot]
        return remote(out_w.at[rows_of(q)], r["wo"].at[slot, rows_of(q)], r["ws"].at[slot, 0], r["wr"].at[slot, 0], y_peer(TO[BACK[slot]]))

    def share_line(slot, k, back):
        _, q, peer = SHARE[slot]
        at = rem(q + 4 - k, 4) if back else q
        piece = r["wo"].at[slot, rows_of(at)]
        return remote(piece, piece, r["ws"].at[slot, k], r["wr"].at[slot, k], peer(k))

    def share_core(slot):
        piece = r["wo"].at[slot, pl.ds(0, 36)]
        return remote(piece, piece, r["ws"].at[0, slot], r["wr"].at[0, slot], core_peer())

    def share_start():
        for slot in (1, 2, 3):
            @pl.when(SHARE[slot][0])
            def _(slot=slot):
                share_y(slot).start()

    def share_second():
        for slot in (1, 2, 3):
            @pl.when(SHARE[slot][0])
            def _(slot=slot):
                share_y(slot).wait_recv()
                for k in (2, 1, 3):
                    share_line(slot, k, False).start()

    def share_third():
        for slot in (1, 2, 3):
            @pl.when(SHARE[slot][0])
            def _(slot=slot):
                for k in (1, 2, 3):
                    share_line(slot, k, True).wait_recv()
                share_core(slot).start()

    def share_wait():
        for slot in (1, 2, 3):
            @pl.when(jnp.logical_not(SHARE[slot][0]))
            def _(slot=slot):
                share_core(slot).wait_recv()

    def share_sent():
        for slot in (1, 2, 3):
            @pl.when(SHARE[slot][0])
            def _(slot=slot):
                share_y(slot).wait_send()
                for k in (1, 2, 3):
                    share_line(slot, k, False).wait_send()
                share_core(slot).wait_send()

    def row(i):
        return mod[i]

    def halves(ref, h):
        return ref[4 * h : 4 * h + 4].astype(F32).reshape(64, D)

    lane = lax.broadcasted_iota(jnp.int32, (128, WP), 1)
    head_masks = [(lane >= HEAD_DIM * h) & (lane < HEAD_DIM * (h + 1)) for h in range(HEADS)]
    same_pixel = rem(lax.broadcasted_iota(jnp.int32, (512, 128), 0), 8) == rem(lax.broadcasted_iota(jnp.int32, (512, 128), 1), 8)

    def stacked(v):
        zero = jnp.zeros_like(v)
        return jnp.concatenate([jnp.where(m, v, zero) for m in head_masks], axis=0)

    def side_by_side(v):
        return jnp.concatenate([v[128 * h : 128 * h + 128] for h in range(HEADS)], axis=1)

    def columns(n):
        return pl.ds(pl.multiple_of(n * 384, 384), 384)

    exchange_in(0, lat, r["xs"])
    share_start()
    gather_start(1, r["cy"], PARTS_C, cot, (0, 2))
    for c in weights[:4]:
        c.start()
    for j in range(3):
        r["win"][j, W:] = jnp.zeros((WP - W, D), BF16)
    for k in range(4):
        r["wo"][k, 36:] = jnp.zeros((12, 8, D), BF16)
    r["dqc"][:, :, 768:] = jnp.zeros((4, 128, 128), BF16)

    mod_copy.wait()
    exchange_in_wait(0, lat, r["xs"])
    for h in range(2):
        normed, _ = norm(halves(r["xs"], h))
        r["f"][0, 64 * h : 64 * h + 64, :] = (normed * (1.0 + row(1)) + row(0)).astype(BF16)
    gather_start(0, r["f"], PARTS_T)
    for c in weights[4:]:
        c.start()
    share_second()
    exchange_in(3, cot, r["cg"].at[0])
    for c in weights[:4]:
        c.wait()

    def attend(lo, n):
        block = r["f"][lo : lo + n].reshape(n * 128, D)
        for j in range(3):
            r["qkv"][lo : lo + n, :, j * WP : (j + 1) * WP] = dot(block, r["win"][j], NT).astype(BF16).reshape(n, 128, WP)
        for t in range(lo, lo + n):
            q, kk, v = (r["qkv"][t, :, j * WP : (j + 1) * WP] for j in range(3))
            scores = dot(stacked(q), kk, NT) * SCALE
            scores = jnp.where(same_pixel, scores, -1e30)
            raised = jnp.exp(scores - jnp.max(scores, axis=-1, keepdims=True))
            probs = raised / jnp.sum(raised, axis=-1, keepdims=True)
            r["probs"][t] = probs
            att = dot(side_by_side(probs.astype(BF16)), stacked(v), NN).astype(BF16)
            if t == 0:
                r["at"][0] = att
            else:
                r["as"][t] = att
                part(2, r["as"], r["at"], t).start()

    attend(0, 1)
    gather_pass(0, r["f"], PARTS_T)
    gather_start(1, r["cy"], PARTS_C, cot, (1, 3))
    gather_near(0, r["f"], PARTS_T)
    attend(1, 2)
    share_third()
    gather_far(0, r["f"], PARTS_T)
    attend(3, 1)
    gather_pass(1, r["cy"], PARTS_C)
    gather_near(1, r["cy"], PARTS_C)
    exchange_in(1, r["cy"].at[1], r["cg"].at[1])
    exchange_in(2, r["cy"].at[2], r["cg"].at[2])

    def branch_block(k, row_, src):
        exchange_in_wait(row_, src, r["cg"].at[k])
        for h in range(2):
            r["g"][k, 64 * h : 64 * h + 64, :] = (row(5) * r["cg"][k, 4 * h : 4 * h + 4].astype(F32).reshape(64, D)).astype(BF16)

    def branch_back(lo, m):
        def step(n, c):
            block = r["g"][lo : lo + m].reshape(m * 128, D)
            r["ag"][lo : lo + m, :, columns(n)] = dot(block, r["wdown"][columns(n), :], NT).reshape(m, 128, 384)
            return c

        lax.fori_loop(0, 3, step, 0)

    branch_block(0, 3, cot)
    weights[4].wait()
    weights[5].wait()
    branch_back(0, 1)
    share_wait()
    part_wait(2, r["as"], r["at"])

    attended = jnp.concatenate([r["at"][k] for k in range(4)], axis=1)
    for n in range(3):
        cols = slice(n * 384, n * 384 + 384)
        r["mid"][:, cols] = dot(attended, r["wo"][:, :, :, cols].reshape(4 * WP, 384), NN)
    for h in range(2):
        rows = slice(64 * h, 64 * h + 64)
        midway = halves(r["xs"], h) + row(2) * r["mid"][rows, :]
        r["mid"][rows, :] = midway
        normed, _ = norm(midway)
        r["s"][0, rows, :] = (normed * (1.0 + row(4)) + row(3)).astype(BF16)
    gather_start(3, r["s"], PARTS_T)
    gather_far(1, r["cy"], PARTS_C)
    exchange_in(4, r["cy"].at[3], r["cg"].at[3])

    def mlp(lo, m):
        def hidden_cols(n, c):
            v = dot(r["s"][lo : lo + m].reshape(m * 128, D), r["wup"][:, columns(n)], NN)
            ag = r["ag"][lo : lo + m, :, columns(n)].reshape(m * 128, 384)
            th = jnp.tanh(GELU_C * (v + 0.044715 * (v * v * v)))
            r["act"][lo : lo + m, :, columns(n)] = (0.5 * v * (1.0 + th)).astype(BF16).reshape(m, 128, 384)
            slope = 0.5 * (1.0 + th) + (0.5 * v) * ((1.0 - th * th) * (GELU_C * (1.0 + (3.0 * 0.044715) * (v * v))))
            r["hg"][lo : lo + m, :, columns(n)] = (ag * slope).astype(BF16).reshape(m, 128, 384)
            return c

        lax.fori_loop(0, 3, hidden_cols, 0)

        def grad_cols(n, c):
            out = dot(r["hg"][lo : lo + m].reshape(m * 128, D), r["wup"][columns(n), :], NT)
            r["p5"][lo : lo + m, :, columns(n)] = out.astype(BF16).reshape(m, 128, 384)
            return c

        lax.fori_loop(0, 3, grad_cols, 0)
        for t in range(max(lo, 1), lo + m):
            part(4, r["p5"], r["r5"], t).start()

    mlp(0, 1)
    for k in range(4):
        r["attc"][:, W * k : W * k + W] = r["at"][k, :, :W]
    gather_pass(3, r["s"], PARTS_T)
    branch_block(1, 1, r["cy"].at[1])
    branch_block(2, 2, r["cy"].at[2])
    branch_back(1, 2)
    gather_near(3, r["s"], PARTS_T)
    mlp(1, 2)
    branch_block(3, 4, r["cy"].at[3])
    branch_back(3, 1)
    gather_far(3, r["s"], PARTS_T)
    mlp(3, 1)

    def weight_grad(left_of, right_of, width, *targets):
        def rows_step(m, c):
            out = dot(left_of(columns(m)), right_of(), TN).astype(BF16).reshape(48, 8, width)
            for q in range(16):
                grp = m * 16 + q
                outer = div(grp, 3)
                for name, at, size in targets:
                    to = r["G" + name].at[div(outer, 8), rem(div(outer, 4), 2), rem(outer, 4), pl.ds(rem(grp, 3) * 3, 3)]
                    to[...] = out[3 * q : 3 * q + 3, :, at : at + size]
            return c

        lax.fori_loop(0, 3, rows_step, 0)

    def every(name):
        return lambda cols: r[name][:, :, cols].reshape(512, 384)

    def job_core(index, start):
        name, n, _ = JOBS[index]
        c = remote(r["G" + name].at[:, 1 - core], r["A" + name], r["js"].at[index, 0], r["jr"].at[index, 0], core_peer())
        if start:
            c.start()
        else:
            c.wait()

    def job_core_sum(index):
        name, n, _ = JOBS[index]

        def step(i, c):
            a, b = div(i, 4), rem(i, 4)
            total = r["A" + name][a, b].astype(F32) + r["G" + name][a, core, b].astype(F32)
            r["A" + name][a, b] = total.astype(BF16)
            return c

        lax.fori_loop(0, 8, step, 0)

    def ring(index):
        name, n, x_first = JOBS[index]
        half = 1 if x_first else 2

        def piece(k, h):
            part_of = pl.ds(h * half, half)
            if x_first:
                return r["A" + name].at[part_of, rem(x + k, 4)]
            at = rem(z + k, 4)
            return r["A" + name].at[rem(at, 2), part_of, pl.ds(4 * div(at, 2), 5)]

        def send(src, dst, m, k):
            return remote(src, dst, r["js"].at[index, m], r["jr"].at[index, m], (x_peer if x_first else z_peer)(k))

        through, landed = r["T" + name], r["B" + name]
        first, last = pl.ds(0, half), pl.ds(half, half)

        def copy(m):
            src, dst, k = (
                (piece(2, 0), through.at[0], 1),
                (piece(2, 1), through.at[1], 3),
                (piece(1, 1), landed.at[0, last], 1),
                (piece(3, 0), landed.at[1, first], 3),
                (through.at[0], landed.at[0, first], 1),
                (through.at[1], landed.at[1, last], 3),
            )[m]
            return send(src, dst, m + 1, k)

        return piece, copy

    def job_first(index, start):
        _, copy = ring(index)
        if start:
            for m in range(4):
                copy(m).start()
        else:
            for m in range(2):
                copy(m).wait_send()
            for m in range(2, 6):
                copy(m).wait()

    def relay(index):
        name = JOBS[index][0]
        piece, copy = ring(index)
        for h, k in ((0, 1), (1, 3)):
            copy(h).wait_recv()
            total = r["T" + name][h].astype(F32) + piece(k, h)[...].astype(F32)
            r["T" + name][h] = total.astype(BF16)
            copy(4 + h).start()

    def job_first_sum(index):
        name, n, x_first = JOBS[index]
        for a in range(2 if x_first else 4):
            mine = r["A" + name][a, x] if x_first else r["A" + name][z_lo, a, pl.ds(4 * z_hi, 5)]
            total = mine.astype(F32)
            for k in range(2):
                total = total + r["B" + name][k, a].astype(F32)
            r["H" + name][a] = total.astype(BF16)

    def job_second(index, start):
        name, n, x_first = JOBS[index]
        for k in (2, 1, 3):
            if x_first:
                other = rem(z + k, 4)
                src = r["H" + name].at[rem(other, 2), pl.ds(4 * div(other, 2), 5)]
                where = z_peer(k)
            else:
                src = r["H" + name].at[rem(x + k, 4)]
                where = x_peer(k)
            c = remote(src, r["C" + name].at[k - 1], r["js"].at[index, 6 + k], r["jr"].at[index, 6 + k], where)
            if start:
                c.start()
            else:
                c.wait()

    def job_second_sum(index):
        name, n, x_first = JOBS[index]
        mine = r["H" + name][z_lo, pl.ds(4 * z_hi, 5)] if x_first else r["H" + name][x]
        total = mine.astype(F32)
        for k in range(3):
            total = total + r["C" + name][k].astype(F32)
        total = total.reshape(40, n)
        return jnp.where(z_hi == 0, total[:36], total[4:])

    def core_step(index):
        job_core(index, False)
        job_core_sum(index)
        job_first(index, True)

    def first_step(index):
        job_first(index, False)
        job_first_sum(index)
        job_second(index, True)

    weight_grad(every("s"), lambda: r["hg"][...].reshape(512, D), D, ("u", 0, D))
    job_core(0, True)
    weight_grad(every("g"), lambda: r["act"][...].reshape(512, D), D, ("d", 0, D))
    job_core(1, True)

    low, high = pl.ds(0, 64), pl.ds(64, 64)

    def halved(ph, p, t, q, m):
        src, dst, to = (
            (r[p].at[3, low], r[t].at[0], 1),
            (r[p].at[3, high], r[t].at[1], 3),
            (r[p].at[2, high], r[q].at[0, high], 1),
            (r[p].at[1, low], r[q].at[1, low], 3),
            (r[t].at[0], r[q].at[0, low], 1),
            (r[t].at[1], r[q].at[1, high], 3),
        )[m]
        return remote(src, dst, r["ys"].at[ph, m], r["yr"].at[ph, m], y_peer(to))

    def halved_relay(ph, p, t, q):
        for m in range(2):
            halved(ph, p, t, q, m).wait_recv()
            mine = r[p][2, 0:64] if m == 0 else r[p][1, 64:128]
            r[t][m] = (r[t][m].astype(F32) + mine.astype(F32)).astype(BF16)
            halved(ph, p, t, q, 4 + m).start()

    def halved_wait(ph, p, t, q):
        for m in range(2, 6):
            halved(ph, p, t, q, m).wait_recv()

    def halved_sum(p, q, h):
        rows = slice(64 * h, 64 * h + 64)
        return r[p][0, rows, :].astype(F32) + r[q][0, rows, :].astype(F32) + r[q][1, rows, :].astype(F32)

    RESULT = (7, "p8", "t8", "r8")
    INPUT = (6, "p7", "t7", "r7")

    core_step(0)
    core_step(1)

    part_wait(4, r["p5"], r["r5"])
    for h in range(2):
        rows = slice(64 * h, 64 * h + 64)
        normed, inverse = norm(r["mid"][rows, :])
        back = norm_back(normed, inverse, part_sum(r["p5"], r["r5"], h) * (1.0 + row(4)))
        mg = halves(r["cg"].at[0], h) + back
        r["mg"][rows, :] = mg
        r["ao"][rows, :] = (row(2) * mg).astype(BF16)
    for k in (3, 1, 2, 0):
        grad = dot(r["ao"][...], r["wo"][k].reshape(WP, D), NT).astype(BF16)
        if k:
            r["ds"][k] = grad
            part(5, r["ds"], r["da"], k).start()
        else:
            r["da"][0] = grad
    def result_cols(n, c):
        out = dot(r["act"][...].reshape(512, D), r["wdown"][:, columns(n)], NN)
        r["p8"][:, :, columns(n)] = out.astype(BF16).reshape(4, 128, 384)
        return c

    lax.fori_loop(0, 3, result_cols, 0)
    for m in range(2):
        halved(*RESULT, m).start()
    weight_grad(lambda cols: r["ao"][:, cols], lambda: r["attc"][...], D, ("o", 0, 640), ("p", 640, 512))
    job_core(2, True)
    job_core(3, True)
    relay(0)
    relay(1)
    def attend_back(lo, m):
        for t in range(lo, lo + m):
            q, kk, v = (r["qkv"][t, :, j * WP : (j + 1) * WP] for j in range(3))
            qs, gs = stacked(q), stacked(r["da"][t])
            probs = r["probs"][t]
            dv = dot(probs.astype(BF16), gs, TN)
            dp_ = dot(gs, v, NT)
            ds = (probs * (dp_ - jnp.sum(probs * dp_, axis=-1, keepdims=True)) * SCALE).astype(BF16)
            dq = dot(side_by_side(ds), stacked(kk), NN)
            dk = dot(ds, qs, TN)
            for j, piece in enumerate((dq, dk, dv)):
                piece = piece.astype(BF16)
                r["dqkv"][t, :, j * WP : (j + 1) * WP] = piece
                r["dqc"][t, :, j * W : (j + 1) * W] = piece[:, :W]
        for n in range(3):
            cols = slice(n * 384, n * 384 + 384)
            total = dot(r["dqkv"][lo : lo + m].reshape(m * 128, D), r["win"][:, :, cols].reshape(D, 384), NN)
            r["p7"][lo : lo + m, :, cols] = total.astype(BF16).reshape(m, 128, 384)

    attend_back(0, 1)
    core_step(2)
    core_step(3)
    part_wait(5, r["ds"], r["da"], (3,))
    attend_back(3, 1)
    halved(*INPUT, 0).start()
    halved(*INPUT, 1).start()
    part_wait(5, r["ds"], r["da"], (1, 2))
    attend_back(1, 2)
    halved(*INPUT, 2).start()
    halved(*INPUT, 3).start()

    weight_grad(every("f"), lambda: r["dqc"][...].reshape(512, CI), CI, ("i", 0, 512), ("v", 512, 384))
    job_core(4, True)
    job_core(5, True)
    halved_relay(*INPUT)
    for m in (2, 3):
        halved(*RESULT, m).start()
    halved_relay(*RESULT)
    relay(2)
    relay(3)
    first_step(0)
    first_step(1)
    core_step(4)
    core_step(5)
    halved_wait(*INPUT)
    for h in range(2):
        rows = slice(64 * h, 64 * h + 64)
        normed, inverse = norm(halves(r["xs"], h))
        back = norm_back(normed, inverse, halved_sum("p7", "r7", h) * (1.0 + row(1)))
        out = r["mg"][rows, :] + back
        r["lo"][4 * h : 4 * h + 4] = out.astype(BF16).reshape(4, 2, 8, D)
    exchange_out(6, r["lo"], r["ll"])
    first_step(2)
    first_step(3)
    relay(4)
    relay(5)

    halved_wait(*RESULT)
    for h in range(2):
        rows = slice(64 * h, 64 * h + 64)
        out = r["mid"][rows, :] + row(5) * halved_sum("p8", "r8", h)
        r["ro"][4 * h : 4 * h + 4] = out.astype(BF16).reshape(4, 2, 8, D)
    exchange_out(5, r["ro"], r["rl"])


    for index, out in ((0, gu), (1, gd)):
        job_second(index, False)
        out[...] = job_second_sum(index).astype(BF16)
    job_second(2, False)
    job_second(3, False)
    both = jnp.concatenate([job_second_sum(2), job_second_sum(3)], axis=1)
    for k in range(4):
        r["oy"][k, :36, :W] = both[:, W * k : W * k + W].astype(BF16)
    for k in (3, 1, 2):
        part(8, r["oy"], r["or"], k).start()
    first_step(4)
    first_step(5)

    part_wait(8, r["oy"], r["or"])
    total = r["oy"][0, :36, :W].astype(F32)
    for k in (1, 2, 3):
        total = total + r["or"][k, :36, :W].astype(F32)
    go[...] = total.astype(BF16)
    exchange_out_wait(6, r["lo"], r["ll"])
    exchange_out_wait(5, r["ro"], r["rl"])
    done = [local(r["rl"], res, r["osem"].at[0]), local(r["ll"], lgr, r["osem"].at[1])]
    for c in done:
        c.start()
    job_second(4, False)
    job_second(5, False)
    both = jnp.concatenate([job_second_sum(4), job_second_sum(5)], axis=1)
    for j in range(3):
        gi[j] = both[:, W * j : W * j + W].astype(BF16)
    for row_, src, dst in (
        (0, lat, r["xs"]),
        (3, cot, r["cg"].at[0]),
        (1, r["cy"].at[1], r["cg"].at[1]),
        (2, r["cy"].at[2], r["cg"].at[2]),
        (4, r["cy"].at[3], r["cg"].at[3]),
    ):
        exchange_in_sent(row_, src, dst)
    gather_sent(1, r["cy"], PARTS_C, cot)
    gather_sent(0, r["f"], PARTS_T)
    gather_sent(3, r["s"], PARTS_T)
    share_sent()
    for m in range(6):
        halved(*RESULT, m).wait_send()
        halved(*INPUT, m).wait_send()
    for ph, src, dst in ((2, "as", "at"), (5, "ds", "da"), (4, "p5", "r5"), (8, "oy", "or")):
        part_send_wait(ph, r[src], r[dst])
    for c in done:
        c.wait()


def body(latents, modulation, in_weight, out_weight, up_weight, down_weight, cotangent):
    vmem = pl.BlockSpec(memory_space=pltpu.VMEM)
    anywhere = pl.BlockSpec(memory_space=pl.ANY)
    out = lambda *s: jax.ShapeDtypeStruct(s, BF16)
    shapes = (out(2, 8, 8, D), out(2, 8, 8, D), out(36, D), out(36, D), out(3, 36, W), out(36, W))
    found = pl.pallas_call(
        kernel,
        out_shape=shapes,
        in_specs=[anywhere] * 7,
        out_specs=(anywhere, anywhere, vmem, vmem, vmem, vmem),
        scratch_shapes=list(SPEC.values()),
        compiler_params=pltpu.CompilerParams(collective_id=0, has_side_effects=True, vmem_limit_bytes=67043328),
        name="block",
    )(
        latents.reshape(2, 8, 8, D),
        cotangent.reshape(2, 8, 8, D),
        jnp.transpose(modulation, (1, 0, 2)),
        jnp.transpose(in_weight, (1, 2, 0)),
        out_weight.reshape(36, 8, D),
        up_weight,
        down_weight,
    )
    res, lgr, gu, gd, gi, go = pl.pallas_call(
        hand_over,
        out_shape=shapes,
        in_specs=[anywhere] * 6,
        out_specs=(anywhere,) * 6,
        scratch_shapes=[pltpu.VMEM(v.shape, BF16) for v in shapes] + [pltpu.SemaphoreType.DMA((2, 6))],
        name="hand_over",
    )(*found)
    return (
        res.reshape(latents.shape),
        lgr.reshape(latents.shape),
        jnp.transpose(gi, (1, 0, 2)),
        go.T,
        gu,
        gd.T,
    )


def hand_over(*refs):
    given, outs, held, sems = refs[:6], refs[6:12], refs[12:18], refs[18]
    into = [pltpu.make_async_copy(a, b, sems.at[0, i]) for i, (a, b) in enumerate(zip(given, held))]
    back = [pltpu.make_async_copy(a, b, sems.at[1, i]) for i, (a, b) in enumerate(zip(held, outs))]
    for c in into:
        c.start()
    for c, d in zip(into, back):
        c.wait()
        d.start()
    for d in back:
        d.wait()


def solution(mesh):
    placed = (
        P("dp", "seq", "tensor", None),
        P("dp", None, None),
        P(None, None, "tensor"),
        P("tensor", None),
        P(None, "tensor"),
        P("tensor", None),
        P("dp", "seq", "tensor", None),
    )
    return jax.shard_map(
        body,
        mesh=mesh,
        in_specs=placed,
        out_specs=(
            P("dp", "seq", "tensor", None),
            P("dp", "seq", "tensor", None),
            P(("dp", "seq"), None, "tensor"),
            P("tensor", ("dp", "seq")),
            P(("dp", "seq"), "tensor"),
            P("tensor", ("dp", "seq")),
        ),
        check_vma=False,
    )
```

```python
import math

import jax
import jax.numpy as jnp
from jax import lax
from jax.experimental import pallas as pl
from jax.experimental.pallas import tpu as pltpu
from jax.sharding import PartitionSpec as P

HEAD_DIM = 72
HEADS = 4
D = 1152
W = 288
WP = 384
SCALE = 1.0 / math.sqrt(HEAD_DIM)
EPS = 1e-6
MESH = pl.DeviceIdType.MESH
F32 = jnp.float32
BF16 = jnp.bfloat16
GELU_C = math.sqrt(2.0 / math.pi)

NN = (((1,), (0,)), ((), ()))
NT = (((1,), (1,)), ((), ()))
TN = (((0,), (0,)), ((), ()))


def rem(a, b):
    return lax.rem(a, b)


def div(a, b):
    return lax.div(a, b)


def dot(a, b, dims):
    return lax.dot_general(a, b, dims, preferred_element_type=F32)


def norm(rows):
    center = jnp.mean(rows, axis=-1, keepdims=True)
    centred = rows - center
    spread = jnp.mean(centred * centred, axis=-1, keepdims=True)
    inverse = lax.rsqrt(spread + EPS)
    return centred * inverse, inverse


def norm_back(normed, inverse, up):
    mean_grad = jnp.mean(up, axis=-1, keepdims=True)
    mean_cross = jnp.mean(up * normed, axis=-1, keepdims=True)
    return (up - mean_grad - normed * mean_cross) * inverse


JOBS = (("u", 1152, True), ("d", 1152, False), ("o", 640, True), ("p", 512, False), ("i", 512, True), ("v", 384, False))
CI = 896


def scratch_spec():
    vm = lambda *s, t=BF16: pltpu.VMEM(s, t)
    dma = lambda *s: pltpu.SemaphoreType.DMA(s)
    spec = {
        "xs": vm(8, 2, 8, D), "cy": vm(4, 2, 8, 8, D), "cg": vm(4, 8, 2, 8, D),
        "win": vm(3, WP, D), "wo": vm(4, 48, 8, D), "wup": vm(D, D), "wdown": vm(D, D),
        "f": vm(4, 128, D), "s": vm(4, 128, D), "g": vm(4, 128, D), "ao": vm(128, D),
        "p5": vm(4, 128, D), "p7": vm(4, 128, D), "ag": vm(4, 128, D, t=F32),
        "r5": vm(4, 128, D), "t7": vm(2, 64, D), "r7": vm(2, 128, D), "p8": vm(4, 128, D), "t8": vm(2, 64, D), "r8": vm(2, 128, D),
        "qkv": vm(4, 128, 3 * WP), "probs": vm(4, 512, 128, t=F32),
        "as": vm(4, 128, WP), "at": vm(4, 128, WP), "ds": vm(4, 128, WP), "da": vm(4, 128, WP), "attc": vm(128, D),
        "act": vm(4, 128, D), "hg": vm(4, 128, D), "dqkv": vm(4, 128, 3 * WP), "dqc": vm(4, 128, CI),
        "mid": vm(128, D, t=F32), "mg": vm(128, D, t=F32),
        "ro": vm(8, 2, 8, D), "lo": vm(8, 2, 8, D), "rl": vm(2, 8, 8, D), "ll": vm(2, 8, 8, D),
        "oy": vm(4, 40, WP), "or": vm(4, 40, WP),
        "wsem": dma(7), "mod": vm(6, 1, D, t=F32),
        "ys": dma(10, 6), "yr": dma(10, 6),
        "ss": dma(7, 8), "sr": dma(7, 8),
        "osem": dma(2),
        "js": dma(6, 10), "jr": dma(6, 10),
        "ws": dma(4, 4), "wr": dma(4, 4),
    }
    for name, n, x_first in JOBS:
        spec["G" + name] = vm(2, 2, 4, 9, 8, n)
        spec["A" + name] = vm(2, 4, 9, 8, n)
        if x_first:
            spec["B" + name] = vm(2, 2, 9, 8, n)
            spec["T" + name] = vm(2, 1, 9, 8, n)
            spec["H" + name] = vm(2, 9, 8, n)
        else:
            spec["B" + name] = vm(2, 4, 5, 8, n)
            spec["T" + name] = vm(2, 2, 5, 8, n)
            spec["H" + name] = vm(4, 5, 8, n)
        spec["C" + name] = vm(3, 5, 8, n)
    return spec


SPEC = scratch_spec()

TO = {1: 3, 2: 1, 3: 2}
BACK = {1: 2, 2: 1, 3: 3}
HOPS = ((0, 1, 0, 1), (1, 1, 0, 1), (1, 3, 0, 2), (0, 3, 0, 2), (0, 1, 1, 3), (1, 3, 2, 3))
PARTS_C = (lambda v: v.at[0], lambda v: v.at[1])
PARTS_T = (lambda v: v.at[pl.ds(0, 64)], lambda v: v.at[pl.ds(64, 64)])


def kernel(lat, cot, mod_in, in_w, out_w, up_w, down_w, res, lgr, gu, gd, gi, go, *scratch):
    r = dict(zip(SPEC, scratch))
    dp, seq, me = lax.axis_index("dp"), lax.axis_index("seq"), lax.axis_index("tensor")
    core, z_lo = rem(dp, 2), div(dp, 2)
    x, z_hi = div(seq, 2), rem(seq, 2)
    z = z_hi * 2 + z_lo

    def remote(src, dst, send, recv, where):
        return pltpu.make_async_remote_copy(src_ref=src, dst_ref=dst, send_sem=send, recv_sem=recv, device_id=where, device_id_type=MESH)

    def local(src, dst, sem):
        return pltpu.make_async_copy(src, dst, sem)

    def seq_peer(k):
        return (dp, rem(seq + k, 8), me)

    def y_peer(k):
        return (dp, seq, rem(me + k, 4))

    def core_peer():
        return (dp + 1 - 2 * core, seq, me)

    def x_peer(k):
        return (dp, rem(x + k, 4) * 2 + z_hi, me)

    def z_peer(k):
        other = rem(z + k, 4)
        return (rem(other, 2) * 2 + core, x * 2 + div(other, 2), me)

    weights = [local(in_w.at[j], r["win"].at[j, pl.ds(0, W)], r["wsem"].at[j]) for j in range(3)]
    weights += [
        local(out_w, r["wo"].at[0, pl.ds(0, 36)], r["wsem"].at[3]),
        local(up_w, r["wup"], r["wsem"].at[4]),
        local(down_w, r["wdown"], r["wsem"].at[5]),
    ]

    mod = r["mod"]
    mod_copy = local(mod_in, mod, r["wsem"].at[6])
    mod_copy.start()
    barrier = pltpu.get_barrier_semaphore()
    peers = [seq_peer(k) for k in range(1, 8)] + [y_peer(k) for k in range(1, 4)] + [core_peer()]
    peers += [z_peer(1), z_peer(3)]
    for where in peers:
        pl.semaphore_signal(barrier, inc=1, device_id=where, device_id_type=MESH)
    pl.semaphore_wait(barrier, len(peers))

    def hop(ph, buf, parts, n, src=None):
        half, to, at, there = HOPS[n]
        given = buf.at[at] if src is None or at else src
        return remote(parts[half](given), parts[half](buf.at[there]), r["ys"].at[ph, n], r["yr"].at[ph, n], y_peer(to))

    def gather_start(ph, buf, parts, src=None, hops=(0, 2, 1, 3)):
        for n in hops:
            hop(ph, buf, parts, n, src).start()

    def gather_pass(ph, buf, parts):
        hop(ph, buf, parts, 0).wait_recv()
        hop(ph, buf, parts, 4).start()
        hop(ph, buf, parts, 2).wait_recv()
        hop(ph, buf, parts, 5).start()

    def gather_near(ph, buf, parts):
        hop(ph, buf, parts, 1).wait_recv()
        hop(ph, buf, parts, 3).wait_recv()

    def gather_far(ph, buf, parts):
        hop(ph, buf, parts, 4).wait_recv()
        hop(ph, buf, parts, 5).wait_recv()

    def gather_sent(ph, buf, parts, src=None):
        for n in range(6):
            hop(ph, buf, parts, n, src).wait_send()

    def part(ph, src, dst, k):
        return remote(src.at[k], dst.at[BACK[k]], r["ys"].at[ph, k], r["yr"].at[ph, BACK[k]], y_peer(TO[k]))

    def part_wait(ph, src, dst, slots=(1, 2, 3)):
        for k in slots:
            part(ph, src, dst, BACK[k]).wait_recv()

    def part_send_wait(ph, src, dst):
        for k in (1, 2, 3):
            part(ph, src, dst, k).wait_send()

    def part_sum(src, dst, h):
        rows = slice(64 * h, 64 * h + 64)
        total = src[0, rows, :].astype(F32)
        for k in (1, 2, 3):
            total = total + dst[k, rows, :].astype(F32)
        return total

    def exchange_in(row_, src, dst):
        for k in range(1, 8):
            to = rem(seq + k, 8)
            remote(src.at[:, to], dst.at[seq], r["ss"].at[row_, k], r["sr"].at[row_, k], seq_peer(k)).start()
        local(src.at[:, seq], dst.at[seq], r["sr"].at[row_, 0]).start()

    def exchange_in_sent(row_, src, dst):
        for k in range(1, 8):
            to = rem(seq + k, 8)
            remote(src.at[:, to], dst.at[seq], r["ss"].at[row_, k], r["sr"].at[row_, k], seq_peer(k)).wait_send()

    def exchange_in_wait(row_, src, dst):
        local(src.at[:, seq], dst.at[seq], r["sr"].at[row_, 0]).wait()
        for k in range(1, 8):
            frm = rem(seq + 8 - k, 8)
            remote(src.at[:, frm], dst.at[frm], r["ss"].at[row_, k], r["sr"].at[row_, k], seq_peer(k)).wait_recv()

    def exchange_out(row_, src, dst):
        for k in range(1, 8):
            to = rem(seq + k, 8)
            remote(src.at[to], dst.at[:, seq], r["ss"].at[row_, k], r["sr"].at[row_, k], seq_peer(k)).start()
        local(src.at[seq], dst.at[:, seq], r["sr"].at[row_, 0]).start()

    def exchange_out_wait(row_, src, dst):
        local(src.at[seq], dst.at[:, seq], r["sr"].at[row_, 0]).wait()
        for k in range(1, 8):
            frm = rem(seq + 8 - k, 8)
            remote(src.at[frm], dst.at[:, frm], r["ss"].at[row_, k], r["sr"].at[row_, k], seq_peer(k)).wait()

    SHARE = {1: (core == 1, z, z_peer), 2: (core == 0, x, x_peer), 3: (core == z_lo, x, x_peer)}

    def rows_of(q):
        return pl.ds(9 * q, 9)

    def share_y(slot):
        _, q, _ = SHARE[slot]
        return remote(out_w.at[rows_of(q)], r["wo"].at[slot, rows_of(q)], r["ws"].at[slot, 0], r["wr"].at[slot, 0], y_peer(TO[BACK[slot]]))

    def share_line(slot, k, back):
        _, q, peer = SHARE[slot]
        at = rem(q + 4 - k, 4) if back else q
        piece = r["wo"].at[slot, rows_of(at)]
        return remote(piece, piece, r["ws"].at[slot, k], r["wr"].at[slot, k], peer(k))

    def share_core(slot):
        piece = r["wo"].at[slot, pl.ds(0, 36)]
        return remote(piece, piece, r["ws"].at[0, slot], r["wr"].at[0, slot], core_peer())

    def share_start():
        for slot in (1, 2, 3):
            @pl.when(SHARE[slot][0])
            def _(slot=slot):
                share_y(slot).start()

    def share_second():
        for slot in (1, 2, 3):
            @pl.when(SHARE[slot][0])
            def _(slot=slot):
                share_y(slot).wait_recv()
                for k in (2, 1, 3):
                    share_line(slot, k, False).start()

    def share_third():
        for slot in (1, 2, 3):
            @pl.when(SHARE[slot][0])
            def _(slot=slot):
                for k in (1, 2, 3):
                    share_line(slot, k, True).wait_recv()
                share_core(slot).start()

    def share_wait():
        for slot in (1, 2, 3):
            @pl.when(jnp.logical_not(SHARE[slot][0]))
            def _(slot=slot):
                share_core(slot).wait_recv()

    def share_sent():
        for slot in (1, 2, 3):
            @pl.when(SHARE[slot][0])
            def _(slot=slot):
                share_y(slot).wait_send()
                for k in (1, 2, 3):
                    share_line(slot, k, False).wait_send()
                share_core(slot).wait_send()

    def row(i):
        return mod[i]

    def halves(ref, h):
        return ref[4 * h : 4 * h + 4].astype(F32).reshape(64, D)

    lane = lax.broadcasted_iota(jnp.int32, (128, WP), 1)
    head_masks = [(lane >= HEAD_DIM * h) & (lane < HEAD_DIM * (h + 1)) for h in range(HEADS)]
    same_pixel = rem(lax.broadcasted_iota(jnp.int32, (512, 128), 0), 8) == rem(lax.broadcasted_iota(jnp.int32, (512, 128), 1), 8)

    def stacked(v):
        zero = jnp.zeros_like(v)
        return jnp.concatenate([jnp.where(m, v, zero) for m in head_masks], axis=0)

    def side_by_side(v):
        return jnp.concatenate([v[128 * h : 128 * h + 128] for h in range(HEADS)], axis=1)

    def columns(n):
        return pl.ds(pl.multiple_of(n * 384, 384), 384)

    exchange_in(0, lat, r["xs"])
    share_start()
    gather_start(1, r["cy"], PARTS_C, cot, (0, 2))
    for c in weights[:4]:
        c.start()
    for j in range(3):
        r["win"][j, W:] = jnp.zeros((WP - W, D), BF16)
    for k in range(4):
        r["wo"][k, 36:] = jnp.zeros((12, 8, D), BF16)
    r["dqc"][:, :, 768:] = jnp.zeros((4, 128, 128), BF16)

    mod_copy.wait()
    exchange_in_wait(0, lat, r["xs"])
    for h in range(2):
        normed, _ = norm(halves(r["xs"], h))
        r["f"][0, 64 * h : 64 * h + 64, :] = (normed * (1.0 + row(1)) + row(0)).astype(BF16)
    gather_start(0, r["f"], PARTS_T)
    for c in weights[4:]:
        c.start()
    share_second()
    exchange_in(3, cot, r["cg"].at[0])
    for c in weights[:4]:
        c.wait()

    def attend(lo, n):
        block = r["f"][lo : lo + n].reshape(n * 128, D)
        for j in range(3):
            r["qkv"][lo : lo + n, :, j * WP : (j + 1) * WP] = dot(block, r["win"][j], NT).astype(BF16).reshape(n, 128, WP)
        for t in range(lo, lo + n):
            q, kk, v = (r["qkv"][t, :, j * WP : (j + 1) * WP] for j in range(3))
            scores = dot(stacked(q), kk, NT) * SCALE
            scores = jnp.where(same_pixel, scores, -1e30)
            raised = jnp.exp(scores - jnp.max(scores, axis=-1, keepdims=True))
            probs = raised / jnp.sum(raised, axis=-1, keepdims=True)
            r["probs"][t] = probs
            att = dot(side_by_side(probs.astype(BF16)), stacked(v), NN).astype(BF16)
            if t == 0:
                r["at"][0] = att
            else:
                r["as"][t] = att
                part(2, r["as"], r["at"], t).start()

    attend(0, 1)
    gather_pass(0, r["f"], PARTS_T)
    gather_start(1, r["cy"], PARTS_C, cot, (1, 3))
    gather_near(0, r["f"], PARTS_T)
    attend(1, 2)
    share_third()
    gather_far(0, r["f"], PARTS_T)
    attend(3, 1)
    gather_pass(1, r["cy"], PARTS_C)
    gather_near(1, r["cy"], PARTS_C)
    exchange_in(1, r["cy"].at[1], r["cg"].at[1])
    exchange_in(2, r["cy"].at[2], r["cg"].at[2])

    def branch_block(k, row_, src):
        exchange_in_wait(row_, src, r["cg"].at[k])
        for h in range(2):
            r["g"][k, 64 * h : 64 * h + 64, :] = (row(5) * r["cg"][k, 4 * h : 4 * h + 4].astype(F32).reshape(64, D)).astype(BF16)

    def branch_back(lo, m):
        def step(n, c):
            block = r["g"][lo : lo + m].reshape(m * 128, D)
            r["ag"][lo : lo + m, :, columns(n)] = dot(block, r["wdown"][columns(n), :], NT).reshape(m, 128, 384)
            return c

        lax.fori_loop(0, 3, step, 0)

    branch_block(0, 3, cot)
    weights[4].wait()
    weights[5].wait()
    branch_back(0, 1)
    share_wait()
    part_wait(2, r["as"], r["at"])

    attended = jnp.concatenate([r["at"][k] for k in range(4)], axis=1)
    for n in range(3):
        cols = slice(n * 384, n * 384 + 384)
        r["mid"][:, cols] = dot(attended, r["wo"][:, :, :, cols].reshape(4 * WP, 384), NN)
    for h in range(2):
        rows = slice(64 * h, 64 * h + 64)
        midway = halves(r["xs"], h) + row(2) * r["mid"][rows, :]
        r["mid"][rows, :] = midway
        normed, _ = norm(midway)
        r["s"][0, rows, :] = (normed * (1.0 + row(4)) + row(3)).astype(BF16)
    gather_start(3, r["s"], PARTS_T)
    gather_far(1, r["cy"], PARTS_C)
    exchange_in(4, r["cy"].at[3], r["cg"].at[3])

    def mlp(lo, m):
        def hidden_cols(n, c):
            v = dot(r["s"][lo : lo + m].reshape(m * 128, D), r["wup"][:, columns(n)], NN)
            ag = r["ag"][lo : lo + m, :, columns(n)].reshape(m * 128, 384)
            th = jnp.tanh(GELU_C * (v + 0.044715 * (v * v * v)))
            r["act"][lo : lo + m, :, columns(n)] = (0.5 * v * (1.0 + th)).astype(BF16).reshape(m, 128, 384)
            slope = 0.5 * (1.0 + th) + (0.5 * v) * ((1.0 - th * th) * (GELU_C * (1.0 + (3.0 * 0.044715) * (v * v))))
            r["hg"][lo : lo + m, :, columns(n)] = (ag * slope).astype(BF16).reshape(m, 128, 384)
            return c

        lax.fori_loop(0, 3, hidden_cols, 0)

        def grad_cols(n, c):
            out = dot(r["hg"][lo : lo + m].reshape(m * 128, D), r["wup"][columns(n), :], NT)
            r["p5"][lo : lo + m, :, columns(n)] = out.astype(BF16).reshape(m, 128, 384)
            return c

        lax.fori_loop(0, 3, grad_cols, 0)
        for t in range(max(lo, 1), lo + m):
            part(4, r["p5"], r["r5"], t).start()

    mlp(0, 1)
    for k in range(4):
        r["attc"][:, W * k : W * k + W] = r["at"][k, :, :W]
    gather_pass(3, r["s"], PARTS_T)
    branch_block(1, 1, r["cy"].at[1])
    branch_block(2, 2, r["cy"].at[2])
    branch_back(1, 2)
    gather_near(3, r["s"], PARTS_T)
    mlp(1, 2)
    branch_block(3, 4, r["cy"].at[3])
    branch_back(3, 1)
    gather_far(3, r["s"], PARTS_T)
    mlp(3, 1)

    def weight_grad(left_of, right_of, width, *targets):
        def rows_step(m, c):
            out = dot(left_of(columns(m)), right_of(), TN).astype(BF16).reshape(48, 8, width)
            for q in range(16):
                grp = m * 16 + q
                outer = div(grp, 3)
                for name, at, size in targets:
                    to = r["G" + name].at[div(outer, 8), rem(div(outer, 4), 2), rem(outer, 4), pl.ds(rem(grp, 3) * 3, 3)]
                    to[...] = out[3 * q : 3 * q + 3, :, at : at + size]
            return c

        lax.fori_loop(0, 3, rows_step, 0)

    def every(name):
        return lambda cols: r[name][:, :, cols].reshape(512, 384)

    def job_core(index, start):
        name, n, _ = JOBS[index]
        c = remote(r["G" + name].at[:, 1 - core], r["A" + name], r["js"].at[index, 0], r["jr"].at[index, 0], core_peer())
        if start:
            c.start()
        else:
            c.wait()

    def job_core_sum(index):
        name, n, _ = JOBS[index]

        def step(i, c):
            a, b = div(i, 4), rem(i, 4)
            total = r["A" + name][a, b].astype(F32) + r["G" + name][a, core, b].astype(F32)
            r["A" + name][a, b] = total.astype(BF16)
            return c

        lax.fori_loop(0, 8, step, 0)

    def ring(index):
        name, n, x_first = JOBS[index]
        half = 1 if x_first else 2

        def piece(k, h):
            part_of = pl.ds(h * half, half)
            if x_first:
                return r["A" + name].at[part_of, rem(x + k, 4)]
            at = rem(z + k, 4)
            return r["A" + name].at[rem(at, 2), part_of, pl.ds(4 * div(at, 2), 5)]

        def send(src, dst, m, k):
            return remote(src, dst, r["js"].at[index, m], r["jr"].at[index, m], (x_peer if x_first else z_peer)(k))

        through, landed = r["T" + name], r["B" + name]
        first, last = pl.ds(0, half), pl.ds(half, half)

        def copy(m):
            src, dst, k = (
                (piece(2, 0), through.at[0], 1),
                (piece(2, 1), through.at[1], 3),
                (piece(1, 1), landed.at[0, last], 1),
                (piece(3, 0), landed.at[1, first], 3),
                (through.at[0], landed.at[0, first], 1),
                (through.at[1], landed.at[1, last], 3),
            )[m]
            return send(src, dst, m + 1, k)

        return piece, copy

    def job_first(index, start):
        _, copy = ring(index)
        if start:
            for m in range(4):
                copy(m).start()
        else:
            for m in range(2):
                copy(m).wait_send()
            for m in range(2, 6):
                copy(m).wait()

    def relay(index):
        name = JOBS[index][0]
        piece, copy = ring(index)
        for h, k in ((0, 1), (1, 3)):
            copy(h).wait_recv()
            total = r["T" + name][h].astype(F32) + piece(k, h)[...].astype(F32)
            r["T" + name][h] = total.astype(BF16)
            copy(4 + h).start()

    def job_first_sum(index):
        name, n, x_first = JOBS[index]
        for a in range(2 if x_first else 4):
            mine = r["A" + name][a, x] if x_first else r["A" + name][z_lo, a, pl.ds(4 * z_hi, 5)]
            total = mine.astype(F32)
            for k in range(2):
                total = total + r["B" + name][k, a].astype(F32)
            r["H" + name][a] = total.astype(BF16)

    def job_second(index, start):
        name, n, x_first = JOBS[index]
        for k in (2, 1, 3):
            if x_first:
                other = rem(z + k, 4)
                src = r["H" + name].at[rem(other, 2), pl.ds(4 * div(other, 2), 5)]
                where = z_peer(k)
            else:
                src = r["H" + name].at[rem(x + k, 4)]
                where = x_peer(k)
            c = remote(src, r["C" + name].at[k - 1], r["js"].at[index, 6 + k], r["jr"].at[index, 6 + k], where)
            if start:
                c.start()
            else:
                c.wait()

    def job_second_sum(index):
        name, n, x_first = JOBS[index]
        mine = r["H" + name][z_lo, pl.ds(4 * z_hi, 5)] if x_first else r["H" + name][x]
        total = mine.astype(F32)
        for k in range(3):
            total = total + r["C" + name][k].astype(F32)
        total = total.reshape(40, n)
        return jnp.where(z_hi == 0, total[:36], total[4:])

    def core_step(index):
        job_core(index, False)
        job_core_sum(index)
        job_first(index, True)

    def first_step(index):
        job_first(index, False)
        job_first_sum(index)
        job_second(index, True)

    weight_grad(every("s"), lambda: r["hg"][...].reshape(512, D), D, ("u", 0, D))
    job_core(0, True)
    weight_grad(every("g"), lambda: r["act"][...].reshape(512, D), D, ("d", 0, D))
    job_core(1, True)

    low, high = pl.ds(0, 64), pl.ds(64, 64)

    def halved(ph, p, t, q, m):
        src, dst, to = (
            (r[p].at[3, low], r[t].at[0], 1),
            (r[p].at[3, high], r[t].at[1], 3),
            (r[p].at[2, high], r[q].at[0, high], 1),
            (r[p].at[1, low], r[q].at[1, low], 3),
            (r[t].at[0], r[q].at[0, low], 1),
            (r[t].at[1], r[q].at[1, high], 3),
        )[m]
        return remote(src, dst, r["ys"].at[ph, m], r["yr"].at[ph, m], y_peer(to))

    def halved_relay(ph, p, t, q):
        for m in range(2):
            halved(ph, p, t, q, m).wait_recv()
            mine = r[p][2, 0:64] if m == 0 else r[p][1, 64:128]
            r[t][m] = (r[t][m].astype(F32) + mine.astype(F32)).astype(BF16)
            halved(ph, p, t, q, 4 + m).start()

    def halved_wait(ph, p, t, q):
        for m in range(2, 6):
            halved(ph, p, t, q, m).wait_recv()

    def halved_sum(p, q, h):
        rows = slice(64 * h, 64 * h + 64)
        return r[p][0, rows, :].astype(F32) + r[q][0, rows, :].astype(F32) + r[q][1, rows, :].astype(F32)

    RESULT = (7, "p8", "t8", "r8")
    INPUT = (6, "p7", "t7", "r7")

    core_step(0)
    core_step(1)

    part_wait(4, r["p5"], r["r5"])
    for h in range(2):
        rows = slice(64 * h, 64 * h + 64)
        normed, inverse = norm(r["mid"][rows, :])
        back = norm_back(normed, inverse, part_sum(r["p5"], r["r5"], h) * (1.0 + row(4)))
        mg = halves(r["cg"].at[0], h) + back
        r["mg"][rows, :] = mg
        r["ao"][rows, :] = (row(2) * mg).astype(BF16)
    for k in (3, 1, 2, 0):
        grad = dot(r["ao"][...], r["wo"][k].reshape(WP, D), NT).astype(BF16)
        if k:
            r["ds"][k] = grad
            part(5, r["ds"], r["da"], k).start()
        else:
            r["da"][0] = grad
    def result_cols(n, c):
        out = dot(r["act"][...].reshape(512, D), r["wdown"][:, columns(n)], NN)
        r["p8"][:, :, columns(n)] = out.astype(BF16).reshape(4, 128, 384)
        return c

    lax.fori_loop(0, 3, result_cols, 0)
    for m in range(2):
        halved(*RESULT, m).start()
    weight_grad(lambda cols: r["ao"][:, cols], lambda: r["attc"][...], D, ("o", 0, 640), ("p", 640, 512))
    job_core(2, True)
    job_core(3, True)
    relay(0)
    relay(1)
    def attend_back(lo, m):
        for t in range(lo, lo + m):
            q, kk, v = (r["qkv"][t, :, j * WP : (j + 1) * WP] for j in range(3))
            qs, gs = stacked(q), stacked(r["da"][t])
            probs = r["probs"][t]
            dv = dot(probs.astype(BF16), gs, TN)
            dp_ = dot(gs, v, NT)
            ds = (probs * (dp_ - jnp.sum(probs * dp_, axis=-1, keepdims=True)) * SCALE).astype(BF16)
            dq = dot(side_by_side(ds), stacked(kk), NN)
            dk = dot(ds, qs, TN)
            for j, piece in enumerate((dq, dk, dv)):
                piece = piece.astype(BF16)
                r["dqkv"][t, :, j * WP : (j + 1) * WP] = piece
                r["dqc"][t, :, j * W : (j + 1) * W] = piece[:, :W]
        for n in range(3):
            cols = slice(n * 384, n * 384 + 384)
            total = dot(r["dqkv"][lo : lo + m].reshape(m * 128, D), r["win"][:, :, cols].reshape(D, 384), NN)
            r["p7"][lo : lo + m, :, cols] = total.astype(BF16).reshape(m, 128, 384)

    attend_back(0, 1)
    core_step(2)
    core_step(3)
    part_wait(5, r["ds"], r["da"], (3,))
    attend_back(3, 1)
    halved(*INPUT, 0).start()
    halved(*INPUT, 1).start()
    part_wait(5, r["ds"], r["da"], (1, 2))
    attend_back(1, 2)
    halved(*INPUT, 2).start()
    halved(*INPUT, 3).start()

    weight_grad(every("f"), lambda: r["dqc"][...].reshape(512, CI), CI, ("i", 0, 512), ("v", 512, 384))
    job_core(4, True)
    job_core(5, True)
    halved_relay(*INPUT)
    for m in (2, 3):
        halved(*RESULT, m).start()
    halved_relay(*RESULT)
    relay(2)
    relay(3)
    first_step(0)
    first_step(1)
    core_step(4)
    core_step(5)
    first_step(2)
    first_step(3)

    halved_wait(*INPUT)
    for h in range(2):
        rows = slice(64 * h, 64 * h + 64)
        normed, inverse = norm(halves(r["xs"], h))
        back = norm_back(normed, inverse, halved_sum("p7", "r7", h) * (1.0 + row(1)))
        out = r["mg"][rows, :] + back
        r["lo"][4 * h : 4 * h + 4] = out.astype(BF16).reshape(4, 2, 8, D)
    exchange_out(6, r["lo"], r["ll"])
    relay(4)
    relay(5)

    halved_wait(*RESULT)
    for h in range(2):
        rows = slice(64 * h, 64 * h + 64)
        out = r["mid"][rows, :] + row(5) * halved_sum("p8", "r8", h)
        r["ro"][4 * h : 4 * h + 4] = out.astype(BF16).reshape(4, 2, 8, D)
    exchange_out(5, r["ro"], r["rl"])

    for index, out in ((0, gu), (1, gd)):
        job_second(index, False)
        out[...] = job_second_sum(index).astype(BF16)
    job_second(2, False)
    job_second(3, False)
    both = jnp.concatenate([job_second_sum(2), job_second_sum(3)], axis=1)
    for k in range(4):
        r["oy"][k, :36, :W] = both[:, W * k : W * k + W].astype(BF16)
    for k in (3, 1, 2):
        part(8, r["oy"], r["or"], k).start()
    first_step(4)
    first_step(5)

    done = [local(r["rl"], res, r["osem"].at[0]), local(r["ll"], lgr, r["osem"].at[1])]
    exchange_out_wait(6, r["lo"], r["ll"])
    done[1].start()
    part_wait(8, r["oy"], r["or"])
    total = r["oy"][0, :36, :W].astype(F32)
    for k in (1, 2, 3):
        total = total + r["or"][k, :36, :W].astype(F32)
    go[...] = total.astype(BF16)
    exchange_out_wait(5, r["ro"], r["rl"])
    done[0].start()
    job_second(4, False)
    job_second(5, False)
    both = jnp.concatenate([job_second_sum(4), job_second_sum(5)], axis=1)
    for j in range(3):
        gi[j] = both[:, W * j : W * j + W].astype(BF16)
    for row_, src, dst in (
        (0, lat, r["xs"]),
        (3, cot, r["cg"].at[0]),
        (1, r["cy"].at[1], r["cg"].at[1]),
        (2, r["cy"].at[2], r["cg"].at[2]),
        (4, r["cy"].at[3], r["cg"].at[3]),
    ):
        exchange_in_sent(row_, src, dst)
    gather_sent(1, r["cy"], PARTS_C, cot)
    gather_sent(0, r["f"], PARTS_T)
    gather_sent(3, r["s"], PARTS_T)
    share_sent()
    for m in range(6):
        halved(*RESULT, m).wait_send()
        halved(*INPUT, m).wait_send()
    for ph, src, dst in ((2, "as", "at"), (5, "ds", "da"), (4, "p5", "r5"), (8, "oy", "or")):
        part_send_wait(ph, r[src], r[dst])
    for c in done:
        c.wait()


def body(latents, modulation, in_weight, out_weight, up_weight, down_weight, cotangent):
    vmem = pl.BlockSpec(memory_space=pltpu.VMEM)
    anywhere = pl.BlockSpec(memory_space=pl.ANY)
    out = lambda *s: jax.ShapeDtypeStruct(s, BF16)
    shapes = (out(2, 8, 8, D), out(2, 8, 8, D), out(36, D), out(36, D), out(3, 36, W), out(36, W))
    found = pl.pallas_call(
        kernel,
        out_shape=shapes,
        in_specs=[anywhere] * 7,
        out_specs=(anywhere, anywhere, vmem, vmem, vmem, vmem),
        scratch_shapes=list(SPEC.values()),
        compiler_params=pltpu.CompilerParams(collective_id=0, has_side_effects=True, vmem_limit_bytes=67043328),
        name="block",
    )(
        latents.reshape(2, 8, 8, D),
        cotangent.reshape(2, 8, 8, D),
        jnp.transpose(modulation, (1, 0, 2)),
        jnp.transpose(in_weight, (1, 2, 0)),
        out_weight.reshape(36, 8, D),
        up_weight,
        down_weight,
    )
    res, lgr, gu, gd, gi, go = pl.pallas_call(
        hand_over,
        out_shape=shapes,
        in_specs=[anywhere] * 6,
        out_specs=(anywhere,) * 6,
        scratch_shapes=[pltpu.VMEM(v.shape, BF16) for v in shapes] + [pltpu.SemaphoreType.DMA((2, 6))],
        name="hand_over",
    )(*found)
    return (
        res.reshape(latents.shape),
        lgr.reshape(latents.shape),
        jnp.transpose(gi, (1, 0, 2)),
        go.T,
        gu,
        gd.T,
    )


def hand_over(*refs):
    given, outs, held, sems = refs[:6], refs[6:12], refs[12:18], refs[18]
    into = [pltpu.make_async_copy(a, b, sems.at[0, i]) for i, (a, b) in enumerate(zip(given, held))]
    back = [pltpu.make_async_copy(a, b, sems.at[1, i]) for i, (a, b) in enumerate(zip(held, outs))]
    for c in into:
        c.start()
    for c, d in zip(into, back):
        c.wait()
        d.start()
    for d in back:
        d.wait()


def solution(mesh):
    placed = (
        P("dp", "seq", "tensor", None),
        P("dp", None, None),
        P(None, None, "tensor"),
        P("tensor", None),
        P(None, "tensor"),
        P("tensor", None),
        P("dp", "seq", "tensor", None),
    )
    return jax.shard_map(
        body,
        mesh=mesh,
        in_specs=placed,
        out_specs=(
            P("dp", "seq", "tensor", None),
            P("dp", "seq", "tensor", None),
            P(("dp", "seq"), None, "tensor"),
            P("tensor", ("dp", "seq")),
            P(("dp", "seq"), "tensor"),
            P("tensor", ("dp", "seq")),
        ),
        check_vma=False,
    )
```

```python
import math

import jax
import jax.numpy as jnp
from jax import lax
from jax.experimental import pallas as pl
from jax.experimental.pallas import tpu as pltpu
from jax.sharding import PartitionSpec as P

HEAD_DIM = 72
HEADS = 4
D = 1152
W = 288
WP = 384
SCALE = 1.0 / math.sqrt(HEAD_DIM)
EPS = 1e-6
MESH = pl.DeviceIdType.MESH
F32 = jnp.float32
BF16 = jnp.bfloat16
GELU_C = math.sqrt(2.0 / math.pi)

NN = (((1,), (0,)), ((), ()))
NT = (((1,), (1,)), ((), ()))
TN = (((0,), (0,)), ((), ()))


def rem(a, b):
    return lax.rem(a, b)


def div(a, b):
    return lax.div(a, b)


def dot(a, b, dims):
    return lax.dot_general(a, b, dims, preferred_element_type=F32)


def norm(rows):
    center = jnp.mean(rows, axis=-1, keepdims=True)
    centred = rows - center
    spread = jnp.mean(centred * centred, axis=-1, keepdims=True)
    inverse = lax.rsqrt(spread + EPS)
    return centred * inverse, inverse


def norm_back(normed, inverse, up):
    mean_grad = jnp.mean(up, axis=-1, keepdims=True)
    mean_cross = jnp.mean(up * normed, axis=-1, keepdims=True)
    return (up - mean_grad - normed * mean_cross) * inverse


JOBS = (("u", 1152, True), ("d", 1152, False), ("o", 640, True), ("p", 512, False), ("i", 512, True), ("v", 384, False))
CI = 896


def scratch_spec():
    vm = lambda *s, t=BF16: pltpu.VMEM(s, t)
    dma = lambda *s: pltpu.SemaphoreType.DMA(s)
    spec = {
        "xs": vm(8, 2, 8, D), "cy": vm(4, 2, 8, 8, D), "cg": vm(4, 8, 2, 8, D),
        "win": vm(3, WP, D), "wo": vm(4, 48, 8, D), "wup": vm(D, D), "wdown": vm(D, D),
        "f": vm(4, 128, D), "s": vm(4, 128, D), "g": vm(4, 128, D), "ao": vm(128, D),
        "p5": vm(4, 128, D), "p7": vm(4, 128, D), "ag": vm(4, 128, D, t=F32),
        "r5": vm(4, 128, D), "t7": vm(2, 64, D), "r7": vm(2, 128, D), "p8": vm(4, 128, D), "t8": vm(2, 64, D), "r8": vm(2, 128, D),
        "qkv": vm(4, 128, 3 * WP), "probs": vm(4, 512, 128, t=F32),
        "as": vm(4, 128, WP), "at": vm(4, 128, WP), "ds": vm(4, 128, WP), "da": vm(4, 128, WP), "attc": vm(128, D),
        "act": vm(4, 128, D), "hg": vm(4, 128, D), "dqkv": vm(4, 128, 3 * WP), "dqc": vm(4, 128, CI),
        "mid": vm(128, D, t=F32), "mg": vm(128, D, t=F32),
        "ro": vm(8, 2, 8, D), "lo": vm(8, 2, 8, D), "rl": vm(2, 8, 8, D), "ll": vm(2, 8, 8, D),
        "oy": vm(4, 40, WP), "or": vm(4, 40, WP),
        "wsem": dma(7), "mod": vm(6, 1, D, t=F32),
        "ys": dma(10, 6), "yr": dma(10, 6),
        "ss": dma(7, 8), "sr": dma(7, 8),
        "osem": dma(2),
        "js": dma(6, 10), "jr": dma(6, 10),
        "ws": dma(4, 4), "wr": dma(4, 4),
    }
    for name, n, x_first in JOBS:
        spec["G" + name] = vm(2, 2, 4, 9, 8, n)
        spec["A" + name] = vm(2, 4, 9, 8, n)
        if x_first:
            spec["B" + name] = vm(2, 2, 9, 8, n)
            spec["T" + name] = vm(2, 1, 9, 8, n)
            spec["H" + name] = vm(2, 9, 8, n)
        else:
            spec["B" + name] = vm(2, 4, 5, 8, n)
            spec["T" + name] = vm(2, 2, 5, 8, n)
            spec["H" + name] = vm(4, 5, 8, n)
        spec["C" + name] = vm(3, 5, 8, n)
    return spec


SPEC = scratch_spec()

TO = {1: 3, 2: 1, 3: 2}
BACK = {1: 2, 2: 1, 3: 3}
HOPS = ((0, 1, 0, 1), (1, 1, 0, 1), (1, 3, 0, 2), (0, 3, 0, 2), (0, 1, 1, 3), (1, 3, 2, 3))
PARTS_C = (lambda v: v.at[0], lambda v: v.at[1])
PARTS_T = (lambda v: v.at[pl.ds(0, 64)], lambda v: v.at[pl.ds(64, 64)])


def kernel(lat, cot, mod_in, in_w, out_w, up_w, down_w, res, lgr, gu, gd, gi, go, *scratch):
    r = dict(zip(SPEC, scratch))
    dp, seq, me = lax.axis_index("dp"), lax.axis_index("seq"), lax.axis_index("tensor")
    core, z_lo = rem(dp, 2), div(dp, 2)
    x, z_hi = div(seq, 2), rem(seq, 2)
    z = z_hi * 2 + z_lo

    def remote(src, dst, send, recv, where):
        return pltpu.make_async_remote_copy(src_ref=src, dst_ref=dst, send_sem=send, recv_sem=recv, device_id=where, device_id_type=MESH)

    def local(src, dst, sem):
        return pltpu.make_async_copy(src, dst, sem)

    def seq_peer(k):
        return (dp, rem(seq + k, 8), me)

    def y_peer(k):
        return (dp, seq, rem(me + k, 4))

    def core_peer():
        return (dp + 1 - 2 * core, seq, me)

    def x_peer(k):
        return (dp, rem(x + k, 4) * 2 + z_hi, me)

    def z_peer(k):
        other = rem(z + k, 4)
        return (rem(other, 2) * 2 + core, x * 2 + div(other, 2), me)

    weights = [local(in_w.at[j], r["win"].at[j, pl.ds(0, W)], r["wsem"].at[j]) for j in range(3)]
    weights += [
        local(out_w, r["wo"].at[0, pl.ds(0, 36)], r["wsem"].at[3]),
        local(up_w, r["wup"], r["wsem"].at[4]),
        local(down_w, r["wdown"], r["wsem"].at[5]),
    ]

    mod = r["mod"]
    mod_copy = local(mod_in, mod, r["wsem"].at[6])
    mod_copy.start()
    barrier = pltpu.get_barrier_semaphore()
    peers = [seq_peer(k) for k in range(1, 8)] + [y_peer(k) for k in range(1, 4)] + [core_peer()]
    peers += [z_peer(1), z_peer(3)]
    for where in peers:
        pl.semaphore_signal(barrier, inc=1, device_id=where, device_id_type=MESH)
    for c in weights:
        c.start()
    for j in range(3):
        r["win"][j, W:] = jnp.zeros((WP - W, D), BF16)
    for k in range(4):
        r["wo"][k, 36:] = jnp.zeros((12, 8, D), BF16)
    r["dqc"][:, :, 768:] = jnp.zeros((4, 128, 128), BF16)
    pl.semaphore_wait(barrier, len(peers))

    def hop(ph, buf, parts, n, src=None):
        half, to, at, there = HOPS[n]
        given = buf.at[at] if src is None or at else src
        return remote(parts[half](given), parts[half](buf.at[there]), r["ys"].at[ph, n], r["yr"].at[ph, n], y_peer(to))

    def gather_start(ph, buf, parts, src=None, hops=(0, 2, 1, 3)):
        for n in hops:
            hop(ph, buf, parts, n, src).start()

    def gather_pass(ph, buf, parts):
        hop(ph, buf, parts, 0).wait_recv()
        hop(ph, buf, parts, 4).start()
        hop(ph, buf, parts, 2).wait_recv()
        hop(ph, buf, parts, 5).start()

    def gather_near(ph, buf, parts):
        hop(ph, buf, parts, 1).wait_recv()
        hop(ph, buf, parts, 3).wait_recv()

    def gather_far(ph, buf, parts):
        hop(ph, buf, parts, 4).wait_recv()
        hop(ph, buf, parts, 5).wait_recv()

    def gather_sent(ph, buf, parts, src=None):
        for n in range(6):
            hop(ph, buf, parts, n, src).wait_send()

    def part(ph, src, dst, k):
        return remote(src.at[k], dst.at[BACK[k]], r["ys"].at[ph, k], r["yr"].at[ph, BACK[k]], y_peer(TO[k]))

    def part_wait(ph, src, dst, slots=(1, 2, 3)):
        for k in slots:
            part(ph, src, dst, BACK[k]).wait_recv()

    def part_send_wait(ph, src, dst):
        for k in (1, 2, 3):
            part(ph, src, dst, k).wait_send()

    def part_sum(src, dst, h):
        rows = slice(64 * h, 64 * h + 64)
        total = src[0, rows, :].astype(F32)
        for k in (1, 2, 3):
            total = total + dst[k, rows, :].astype(F32)
        return total

    def exchange_in(row_, src, dst):
        for k in range(1, 8):
            to = rem(seq + k, 8)
            remote(src.at[:, to], dst.at[seq], r["ss"].at[row_, k], r["sr"].at[row_, k], seq_peer(k)).start()
        local(src.at[:, seq], dst.at[seq], r["sr"].at[row_, 0]).start()

    def exchange_in_sent(row_, src, dst):
        for k in range(1, 8):
            to = rem(seq + k, 8)
            remote(src.at[:, to], dst.at[seq], r["ss"].at[row_, k], r["sr"].at[row_, k], seq_peer(k)).wait_send()

    def exchange_in_wait(row_, src, dst):
        local(src.at[:, seq], dst.at[seq], r["sr"].at[row_, 0]).wait()
        for k in range(1, 8):
            frm = rem(seq + 8 - k, 8)
            remote(src.at[:, frm], dst.at[frm], r["ss"].at[row_, k], r["sr"].at[row_, k], seq_peer(k)).wait_recv()

    def exchange_out(row_, src, dst):
        for k in range(1, 8):
            to = rem(seq + k, 8)
            remote(src.at[to], dst.at[:, seq], r["ss"].at[row_, k], r["sr"].at[row_, k], seq_peer(k)).start()
        local(src.at[seq], dst.at[:, seq], r["sr"].at[row_, 0]).start()

    def exchange_out_wait(row_, src, dst):
        local(src.at[seq], dst.at[:, seq], r["sr"].at[row_, 0]).wait()
        for k in range(1, 8):
            frm = rem(seq + 8 - k, 8)
            remote(src.at[frm], dst.at[:, frm], r["ss"].at[row_, k], r["sr"].at[row_, k], seq_peer(k)).wait()

    SHARE = {1: (core == 1, z, z_peer), 2: (core == 0, x, x_peer), 3: (core == z_lo, x, x_peer)}

    def rows_of(q):
        return pl.ds(9 * q, 9)

    def share_y(slot):
        _, q, _ = SHARE[slot]
        return remote(out_w.at[rows_of(q)], r["wo"].at[slot, rows_of(q)], r["ws"].at[slot, 0], r["wr"].at[slot, 0], y_peer(TO[BACK[slot]]))

    def share_line(slot, k, back):
        _, q, peer = SHARE[slot]
        at = rem(q + 4 - k, 4) if back else q
        piece = r["wo"].at[slot, rows_of(at)]
        return remote(piece, piece, r["ws"].at[slot, k], r["wr"].at[slot, k], peer(k))

    def share_core(slot):
        piece = r["wo"].at[slot, pl.ds(0, 36)]
        return remote(piece, piece, r["ws"].at[0, slot], r["wr"].at[0, slot], core_peer())

    def share_start():
        for slot in (1, 2, 3):
            @pl.when(SHARE[slot][0])
            def _(slot=slot):
                share_y(slot).start()

    def share_second():
        for slot in (1, 2, 3):
            @pl.when(SHARE[slot][0])
            def _(slot=slot):
                share_y(slot).wait_recv()
                for k in (2, 1, 3):
                    share_line(slot, k, False).start()

    def share_third():
        for slot in (1, 2, 3):
            @pl.when(SHARE[slot][0])
            def _(slot=slot):
                for k in (1, 2, 3):
                    share_line(slot, k, True).wait_recv()
                share_core(slot).start()

    def share_wait():
        for slot in (1, 2, 3):
            @pl.when(jnp.logical_not(SHARE[slot][0]))
            def _(slot=slot):
                share_core(slot).wait_recv()

    def share_sent():
        for slot in (1, 2, 3):
            @pl.when(SHARE[slot][0])
            def _(slot=slot):
                share_y(slot).wait_send()
                for k in (1, 2, 3):
                    share_line(slot, k, False).wait_send()
                share_core(slot).wait_send()

    def row(i):
        return mod[i]

    def halves(ref, h):
        return ref[4 * h : 4 * h + 4].astype(F32).reshape(64, D)

    lane = lax.broadcasted_iota(jnp.int32, (128, WP), 1)
    head_masks = [(lane >= HEAD_DIM * h) & (lane < HEAD_DIM * (h + 1)) for h in range(HEADS)]
    same_pixel = rem(lax.broadcasted_iota(jnp.int32, (512, 128), 0), 8) == rem(lax.broadcasted_iota(jnp.int32, (512, 128), 1), 8)

    def stacked(v):
        zero = jnp.zeros_like(v)
        return jnp.concatenate([jnp.where(m, v, zero) for m in head_masks], axis=0)

    def side_by_side(v):
        return jnp.concatenate([v[128 * h : 128 * h + 128] for h in range(HEADS)], axis=1)

    def columns(n):
        return pl.ds(pl.multiple_of(n * 384, 384), 384)

    exchange_in(0, lat, r["xs"])
    share_start()
    gather_start(1, r["cy"], PARTS_C, cot, (0, 2))

    mod_copy.wait()
    exchange_in_wait(0, lat, r["xs"])
    for h in range(2):
        normed, _ = norm(halves(r["xs"], h))
        r["f"][0, 64 * h : 64 * h + 64, :] = (normed * (1.0 + row(1)) + row(0)).astype(BF16)
    gather_start(0, r["f"], PARTS_T)
    share_second()
    exchange_in(3, cot, r["cg"].at[0])
    for c in weights[:4]:
        c.wait()

    def attend(lo, n):
        block = r["f"][lo : lo + n].reshape(n * 128, D)
        for j in range(3):
            r["qkv"][lo : lo + n, :, j * WP : (j + 1) * WP] = dot(block, r["win"][j], NT).astype(BF16).reshape(n, 128, WP)
        for t in range(lo, lo + n):
            q, kk, v = (r["qkv"][t, :, j * WP : (j + 1) * WP] for j in range(3))
            scores = dot(stacked(q), kk, NT) * SCALE
            scores = jnp.where(same_pixel, scores, -1e30)
            raised = jnp.exp(scores - jnp.max(scores, axis=-1, keepdims=True))
            probs = raised / jnp.sum(raised, axis=-1, keepdims=True)
            r["probs"][t] = probs
            att = dot(side_by_side(probs.astype(BF16)), stacked(v), NN).astype(BF16)
            if t == 0:
                r["at"][0] = att
            else:
                r["as"][t] = att
                part(2, r["as"], r["at"], t).start()

    attend(0, 1)
    gather_pass(0, r["f"], PARTS_T)
    gather_start(1, r["cy"], PARTS_C, cot, (1, 3))
    gather_near(0, r["f"], PARTS_T)
    attend(1, 2)
    share_third()
    gather_far(0, r["f"], PARTS_T)
    attend(3, 1)
    gather_pass(1, r["cy"], PARTS_C)
    gather_near(1, r["cy"], PARTS_C)
    exchange_in(1, r["cy"].at[1], r["cg"].at[1])
    exchange_in(2, r["cy"].at[2], r["cg"].at[2])

    def branch_block(k, row_, src):
        exchange_in_wait(row_, src, r["cg"].at[k])
        for h in range(2):
            r["g"][k, 64 * h : 64 * h + 64, :] = (row(5) * r["cg"][k, 4 * h : 4 * h + 4].astype(F32).reshape(64, D)).astype(BF16)

    def branch_back(lo, m):
        def step(n, c):
            block = r["g"][lo : lo + m].reshape(m * 128, D)
            r["ag"][lo : lo + m, :, columns(n)] = dot(block, r["wdown"][columns(n), :], NT).reshape(m, 128, 384)
            return c

        lax.fori_loop(0, 3, step, 0)

    branch_block(0, 3, cot)
    weights[4].wait()
    weights[5].wait()
    branch_back(0, 1)
    share_wait()
    part_wait(2, r["as"], r["at"])

    attended = jnp.concatenate([r["at"][k] for k in range(4)], axis=1)
    for n in range(3):
        cols = slice(n * 384, n * 384 + 384)
        r["mid"][:, cols] = dot(attended, r["wo"][:, :, :, cols].reshape(4 * WP, 384), NN)
    for h in range(2):
        rows = slice(64 * h, 64 * h + 64)
        midway = halves(r["xs"], h) + row(2) * r["mid"][rows, :]
        r["mid"][rows, :] = midway
        normed, _ = norm(midway)
        r["s"][0, rows, :] = (normed * (1.0 + row(4)) + row(3)).astype(BF16)
    gather_start(3, r["s"], PARTS_T)
    gather_far(1, r["cy"], PARTS_C)
    exchange_in(4, r["cy"].at[3], r["cg"].at[3])

    def mlp(lo, m):
        def hidden_cols(n, c):
            v = dot(r["s"][lo : lo + m].reshape(m * 128, D), r["wup"][:, columns(n)], NN)
            ag = r["ag"][lo : lo + m, :, columns(n)].reshape(m * 128, 384)
            th = jnp.tanh(GELU_C * (v + 0.044715 * (v * v * v)))
            r["act"][lo : lo + m, :, columns(n)] = (0.5 * v * (1.0 + th)).astype(BF16).reshape(m, 128, 384)
            slope = 0.5 * (1.0 + th) + (0.5 * v) * ((1.0 - th * th) * (GELU_C * (1.0 + (3.0 * 0.044715) * (v * v))))
            r["hg"][lo : lo + m, :, columns(n)] = (ag * slope).astype(BF16).reshape(m, 128, 384)
            return c

        lax.fori_loop(0, 3, hidden_cols, 0)

        def grad_cols(n, c):
            out = dot(r["hg"][lo : lo + m].reshape(m * 128, D), r["wup"][columns(n), :], NT)
            r["p5"][lo : lo + m, :, columns(n)] = out.astype(BF16).reshape(m, 128, 384)
            return c

        lax.fori_loop(0, 3, grad_cols, 0)
        for t in range(max(lo, 1), lo + m):
            part(4, r["p5"], r["r5"], t).start()

    mlp(0, 1)
    for k in range(4):
        r["attc"][:, W * k : W * k + W] = r["at"][k, :, :W]
    gather_pass(3, r["s"], PARTS_T)
    branch_block(1, 1, r["cy"].at[1])
    branch_block(2, 2, r["cy"].at[2])
    branch_back(1, 2)
    gather_near(3, r["s"], PARTS_T)
    mlp(1, 2)
    branch_block(3, 4, r["cy"].at[3])
    branch_back(3, 1)
    gather_far(3, r["s"], PARTS_T)
    mlp(3, 1)

    def weight_grad(left_of, right_of, width, *targets):
        def rows_step(m, c):
            out = dot(left_of(columns(m)), right_of(), TN).astype(BF16).reshape(48, 8, width)
            for q in range(16):
                grp = m * 16 + q
                outer = div(grp, 3)
                for name, at, size in targets:
                    to = r["G" + name].at[div(outer, 8), rem(div(outer, 4), 2), rem(outer, 4), pl.ds(rem(grp, 3) * 3, 3)]
                    to[...] = out[3 * q : 3 * q + 3, :, at : at + size]
            return c

        lax.fori_loop(0, 3, rows_step, 0)

    def every(name):
        return lambda cols: r[name][:, :, cols].reshape(512, 384)

    def job_core(index, start):
        name, n, _ = JOBS[index]
        c = remote(r["G" + name].at[:, 1 - core], r["A" + name], r["js"].at[index, 0], r["jr"].at[index, 0], core_peer())
        if start:
            c.start()
        else:
            c.wait()

    def job_core_sum(index):
        name, n, _ = JOBS[index]

        def step(i, c):
            a, b = div(i, 4), rem(i, 4)
            total = r["A" + name][a, b].astype(F32) + r["G" + name][a, core, b].astype(F32)
            r["A" + name][a, b] = total.astype(BF16)
            return c

        lax.fori_loop(0, 8, step, 0)

    def ring(index):
        name, n, x_first = JOBS[index]
        half = 1 if x_first else 2

        def piece(k, h):
            part_of = pl.ds(h * half, half)
            if x_first:
                return r["A" + name].at[part_of, rem(x + k, 4)]
            at = rem(z + k, 4)
            return r["A" + name].at[rem(at, 2), part_of, pl.ds(4 * div(at, 2), 5)]

        def send(src, dst, m, k):
            return remote(src, dst, r["js"].at[index, m], r["jr"].at[index, m], (x_peer if x_first else z_peer)(k))

        through, landed = r["T" + name], r["B" + name]
        first, last = pl.ds(0, half), pl.ds(half, half)

        def copy(m):
            src, dst, k = (
                (piece(2, 0), through.at[0], 1),
                (piece(2, 1), through.at[1], 3),
                (piece(1, 1), landed.at[0, last], 1),
                (piece(3, 0), landed.at[1, first], 3),
                (through.at[0], landed.at[0, first], 1),
                (through.at[1], landed.at[1, last], 3),
            )[m]
            return send(src, dst, m + 1, k)

        return piece, copy

    def job_first(index, start):
        _, copy = ring(index)
        if start:
            for m in range(4):
                copy(m).start()
        else:
            for m in range(2):
                copy(m).wait_send()
            for m in range(2, 6):
                copy(m).wait()

    def relay(index):
        name = JOBS[index][0]
        piece, copy = ring(index)
        for h, k in ((0, 1), (1, 3)):
            copy(h).wait_recv()
            total = r["T" + name][h].astype(F32) + piece(k, h)[...].astype(F32)
            r["T" + name][h] = total.astype(BF16)
            copy(4 + h).start()

    def job_first_sum(index):
        name, n, x_first = JOBS[index]
        for a in range(2 if x_first else 4):
            mine = r["A" + name][a, x] if x_first else r["A" + name][z_lo, a, pl.ds(4 * z_hi, 5)]
            total = mine.astype(F32)
            for k in range(2):
                total = total + r["B" + name][k, a].astype(F32)
            r["H" + name][a] = total.astype(BF16)

    def job_second(index, start):
        name, n, x_first = JOBS[index]
        for k in (2, 1, 3):
            if x_first:
                other = rem(z + k, 4)
                src = r["H" + name].at[rem(other, 2), pl.ds(4 * div(other, 2), 5)]
                where = z_peer(k)
            else:
                src = r["H" + name].at[rem(x + k, 4)]
                where = x_peer(k)
            c = remote(src, r["C" + name].at[k - 1], r["js"].at[index, 6 + k], r["jr"].at[index, 6 + k], where)
            if start:
                c.start()
            else:
                c.wait()

    def job_second_sum(index):
        name, n, x_first = JOBS[index]
        mine = r["H" + name][z_lo, pl.ds(4 * z_hi, 5)] if x_first else r["H" + name][x]
        total = mine.astype(F32)
        for k in range(3):
            total = total + r["C" + name][k].astype(F32)
        total = total.reshape(40, n)
        return jnp.where(z_hi == 0, total[:36], total[4:])

    def core_step(index):
        job_core(index, False)
        job_core_sum(index)
        job_first(index, True)

    def first_step(index):
        job_first(index, False)
        job_first_sum(index)
        job_second(index, True)

    weight_grad(every("s"), lambda: r["hg"][...].reshape(512, D), D, ("u", 0, D))
    job_core(0, True)
    weight_grad(every("g"), lambda: r["act"][...].reshape(512, D), D, ("d", 0, D))
    job_core(1, True)

    low, high = pl.ds(0, 64), pl.ds(64, 64)

    def halved(ph, p, t, q, m):
        src, dst, to = (
            (r[p].at[3, low], r[t].at[0], 1),
            (r[p].at[3, high], r[t].at[1], 3),
            (r[p].at[2, high], r[q].at[0, high], 1),
            (r[p].at[1, low], r[q].at[1, low], 3),
            (r[t].at[0], r[q].at[0, low], 1),
            (r[t].at[1], r[q].at[1, high], 3),
        )[m]
        return remote(src, dst, r["ys"].at[ph, m], r["yr"].at[ph, m], y_peer(to))

    def halved_relay(ph, p, t, q):
        for m in range(2):
            halved(ph, p, t, q, m).wait_recv()
            mine = r[p][2, 0:64] if m == 0 else r[p][1, 64:128]
            r[t][m] = (r[t][m].astype(F32) + mine.astype(F32)).astype(BF16)
            halved(ph, p, t, q, 4 + m).start()

    def halved_wait(ph, p, t, q):
        for m in range(2, 6):
            halved(ph, p, t, q, m).wait_recv()

    def halved_sum(p, q, h):
        rows = slice(64 * h, 64 * h + 64)
        return r[p][0, rows, :].astype(F32) + r[q][0, rows, :].astype(F32) + r[q][1, rows, :].astype(F32)

    RESULT = (7, "p8", "t8", "r8")
    INPUT = (6, "p7", "t7", "r7")

    core_step(0)
    core_step(1)

    part_wait(4, r["p5"], r["r5"])
    for h in range(2):
        rows = slice(64 * h, 64 * h + 64)
        normed, inverse = norm(r["mid"][rows, :])
        back = norm_back(normed, inverse, part_sum(r["p5"], r["r5"], h) * (1.0 + row(4)))
        mg = halves(r["cg"].at[0], h) + back
        r["mg"][rows, :] = mg
        r["ao"][rows, :] = (row(2) * mg).astype(BF16)
    for k in (3, 1, 2, 0):
        grad = dot(r["ao"][...], r["wo"][k].reshape(WP, D), NT).astype(BF16)
        if k:
            r["ds"][k] = grad
            part(5, r["ds"], r["da"], k).start()
        else:
            r["da"][0] = grad
    def result_cols(n, c):
        out = dot(r["act"][...].reshape(512, D), r["wdown"][:, columns(n)], NN)
        r["p8"][:, :, columns(n)] = out.astype(BF16).reshape(4, 128, 384)
        return c

    lax.fori_loop(0, 3, result_cols, 0)
    for m in range(2):
        halved(*RESULT, m).start()
    weight_grad(lambda cols: r["ao"][:, cols], lambda: r["attc"][...], D, ("o", 0, 640), ("p", 640, 512))
    job_core(2, True)
    job_core(3, True)
    relay(0)
    relay(1)
    def attend_back(lo, m):
        for t in range(lo, lo + m):
            q, kk, v = (r["qkv"][t, :, j * WP : (j + 1) * WP] for j in range(3))
            qs, gs = stacked(q), stacked(r["da"][t])
            probs = r["probs"][t]
            dv = dot(probs.astype(BF16), gs, TN)
            dp_ = dot(gs, v, NT)
            ds = (probs * (dp_ - jnp.sum(probs * dp_, axis=-1, keepdims=True)) * SCALE).astype(BF16)
            dq = dot(side_by_side(ds), stacked(kk), NN)
            dk = dot(ds, qs, TN)
            for j, piece in enumerate((dq, dk, dv)):
                piece = piece.astype(BF16)
                r["dqkv"][t, :, j * WP : (j + 1) * WP] = piece
                r["dqc"][t, :, j * W : (j + 1) * W] = piece[:, :W]
        for n in range(3):
            cols = slice(n * 384, n * 384 + 384)
            total = dot(r["dqkv"][lo : lo + m].reshape(m * 128, D), r["win"][:, :, cols].reshape(D, 384), NN)
            r["p7"][lo : lo + m, :, cols] = total.astype(BF16).reshape(m, 128, 384)

    attend_back(0, 1)
    core_step(2)
    core_step(3)
    part_wait(5, r["ds"], r["da"], (3,))
    attend_back(3, 1)
    halved(*INPUT, 0).start()
    halved(*INPUT, 1).start()
    part_wait(5, r["ds"], r["da"], (1, 2))
    attend_back(1, 2)
    halved(*INPUT, 2).start()
    halved(*INPUT, 3).start()

    weight_grad(every("f"), lambda: r["dqc"][...].reshape(512, CI), CI, ("i", 0, 512), ("v", 512, 384))
    job_core(4, True)
    job_core(5, True)
    halved_relay(*INPUT)
    for m in (2, 3):
        halved(*RESULT, m).start()
    halved_relay(*RESULT)
    relay(2)
    relay(3)
    first_step(0)
    first_step(1)
    core_step(4)
    core_step(5)
    halved_wait(*INPUT)
    for h in range(2):
        rows = slice(64 * h, 64 * h + 64)
        normed, inverse = norm(halves(r["xs"], h))
        back = norm_back(normed, inverse, halved_sum("p7", "r7", h) * (1.0 + row(1)))
        out = r["mg"][rows, :] + back
        r["lo"][4 * h : 4 * h + 4] = out.astype(BF16).reshape(4, 2, 8, D)
    exchange_out(6, r["lo"], r["ll"])
    first_step(2)
    first_step(3)
    relay(4)
    relay(5)

    halved_wait(*RESULT)
    for h in range(2):
        rows = slice(64 * h, 64 * h + 64)
        out = r["mid"][rows, :] + row(5) * halved_sum("p8", "r8", h)
        r["ro"][4 * h : 4 * h + 4] = out.astype(BF16).reshape(4, 2, 8, D)
    exchange_out(5, r["ro"], r["rl"])


    for index, out in ((0, gu), (1, gd)):
        job_second(index, False)
        out[...] = job_second_sum(index).astype(BF16)
    job_second(2, False)
    job_second(3, False)
    both = jnp.concatenate([job_second_sum(2), job_second_sum(3)], axis=1)
    for k in range(4):
        r["oy"][k, :36, :W] = both[:, W * k : W * k + W].astype(BF16)
    for k in (3, 1, 2):
        part(8, r["oy"], r["or"], k).start()
    first_step(4)
    first_step(5)

    part_wait(8, r["oy"], r["or"])
    total = r["oy"][0, :36, :W].astype(F32)
    for k in (1, 2, 3):
        total = total + r["or"][k, :36, :W].astype(F32)
    go[...] = total.astype(BF16)
    exchange_out_wait(6, r["lo"], r["ll"])
    exchange_out_wait(5, r["ro"], r["rl"])
    done = [local(r["rl"], res, r["osem"].at[0]), local(r["ll"], lgr, r["osem"].at[1])]
    for c in done:
        c.start()
    job_second(4, False)
    job_second(5, False)
    both = jnp.concatenate([job_second_sum(4), job_second_sum(5)], axis=1)
    for j in range(3):
        gi[j] = both[:, W * j : W * j + W].astype(BF16)
    for row_, src, dst in (
        (0, lat, r["xs"]),
        (3, cot, r["cg"].at[0]),
        (1, r["cy"].at[1], r["cg"].at[1]),
        (2, r["cy"].at[2], r["cg"].at[2]),
        (4, r["cy"].at[3], r["cg"].at[3]),
    ):
        exchange_in_sent(row_, src, dst)
    gather_sent(1, r["cy"], PARTS_C, cot)
    gather_sent(0, r["f"], PARTS_T)
    gather_sent(3, r["s"], PARTS_T)
    share_sent()
    for m in range(6):
        halved(*RESULT, m).wait_send()
        halved(*INPUT, m).wait_send()
    for ph, src, dst in ((2, "as", "at"), (5, "ds", "da"), (4, "p5", "r5"), (8, "oy", "or")):
        part_send_wait(ph, r[src], r[dst])
    for c in done:
        c.wait()


def body(latents, modulation, in_weight, out_weight, up_weight, down_weight, cotangent):
    vmem = pl.BlockSpec(memory_space=pltpu.VMEM)
    anywhere = pl.BlockSpec(memory_space=pl.ANY)
    out = lambda *s: jax.ShapeDtypeStruct(s, BF16)
    shapes = (out(2, 8, 8, D), out(2, 8, 8, D), out(36, D), out(36, D), out(3, 36, W), out(36, W))
    found = pl.pallas_call(
        kernel,
        out_shape=shapes,
        in_specs=[anywhere] * 7,
        out_specs=(anywhere, anywhere, vmem, vmem, vmem, vmem),
        scratch_shapes=list(SPEC.values()),
        compiler_params=pltpu.CompilerParams(collective_id=0, has_side_effects=True, vmem_limit_bytes=67043328),
        name="block",
    )(
        latents.reshape(2, 8, 8, D),
        cotangent.reshape(2, 8, 8, D),
        jnp.transpose(modulation, (1, 0, 2)),
        jnp.transpose(in_weight, (1, 2, 0)),
        out_weight.reshape(36, 8, D),
        up_weight,
        down_weight,
    )
    res, lgr, gu, gd, gi, go = pl.pallas_call(
        hand_over,
        out_shape=shapes,
        in_specs=[anywhere] * 6,
        out_specs=(anywhere,) * 6,
        scratch_shapes=[pltpu.VMEM(v.shape, BF16) for v in shapes] + [pltpu.SemaphoreType.DMA((2, 6))],
        name="hand_over",
    )(*found)
    return (
        res.reshape(latents.shape),
        lgr.reshape(latents.shape),
        jnp.transpose(gi, (1, 0, 2)),
        go.T,
        gu,
        gd.T,
    )


def hand_over(*refs):
    given, outs, held, sems = refs[:6], refs[6:12], refs[12:18], refs[18]
    into = [pltpu.make_async_copy(a, b, sems.at[0, i]) for i, (a, b) in enumerate(zip(given, held))]
    back = [pltpu.make_async_copy(a, b, sems.at[1, i]) for i, (a, b) in enumerate(zip(held, outs))]
    for c in into:
        c.start()
    for c, d in zip(into, back):
        c.wait()
        d.start()
    for d in back:
        d.wait()


def solution(mesh):
    placed = (
        P("dp", "seq", "tensor", None),
        P("dp", None, None),
        P(None, None, "tensor"),
        P("tensor", None),
        P(None, "tensor"),
        P("tensor", None),
        P("dp", "seq", "tensor", None),
    )
    return jax.shard_map(
        body,
        mesh=mesh,
        in_specs=placed,
        out_specs=(
            P("dp", "seq", "tensor", None),
            P("dp", "seq", "tensor", None),
            P(("dp", "seq"), None, "tensor"),
            P("tensor", ("dp", "seq")),
            P(("dp", "seq"), "tensor"),
            P("tensor", ("dp", "seq")),
        ),
        check_vma=False,
    )
```
